32 devices in a mesh: lat: 8 (over y, x, core), depth: 4 (over z).
Axes of the slice: x: 2, y: 2, z: 4, core: 2. Of those that a mesh axis runs over, the one named last changes fastest.
Arguments:
- velocity_fine: float32 [3, 96, 64, 384], P(None, 'lat', 'depth'), may hold values from -6 to 6
- stress_fine: float32 [6, 96, 64, 384], P(None, 'lat', 'depth'), may hold values from -6 to 6
- memory_fine: float32 [6, 96, 64, 384], P(None, 'lat', 'depth'), may hold values from -1.8 to 1.8
- peak_fine: float32 [96, 64, 384], P('lat', 'depth'), may hold values from 0 to 12
- zone_fine: int32 [96, 64, 384], P('lat', 'depth'), may hold values from 0 to 7
- velocity_coarse: float32 [3, 32, 128, 128], P(None, 'lat', 'depth'), may hold values from -6 to 6
- stress_coarse: float32 [6, 32, 128, 128], P(None, 'lat', 'depth'), may hold values from -6 to 6
- memory_coarse: float32 [6, 32, 128, 128], P(None, 'lat', 'depth'), may hold values from -1.8 to 1.8
- peak_coarse: float32 [32, 128, 128], P('lat', 'depth'), may hold values from 0 to 12
- zone_coarse: int32 [32, 128, 128], P('lat', 'depth'), may hold values from 0 to 7
- zone_table: float32 [8, 5], replicated, may hold values from 0.05 to 1, as said below
- interp_weight: int32 [2, 3], replicated, may hold values from 0 to 8
- restrict_weight: int32 [2, 3], replicated, may hold values from 1 to 8
Outputs:
- fine_velocity: float32 [3, 96, 64, 384], P(None, 'lat', 'depth')
- fine_stress: float32 [6, 96, 64, 384], P(None, 'lat', 'depth')
- fine_memory: float32 [6, 96, 64, 384], P(None, 'lat', 'depth')
- fine_peak: float32 [96, 64, 384], P('lat', 'depth')
- coarse_velocity: float32 [3, 32, 128, 128], P(None, 'lat', 'depth')
- coarse_stress: float32 [6, 32, 128, 128], P(None, 'lat', 'depth')
- coarse_memory: float32 [6, 32, 128, 128], P(None, 'lat', 'depth')
- coarse_peak: float32 [32, 128, 128], P('lat', 'depth')
The draws below stay inside these ranges and needn't reach their ends.
Inputs may be any that keep to these rules, and one draw needn't show every extreme that they name: `zone_table`: column 0 lies in 0.5 to 1, columns 1 and 2 in 0.1 to 0.3, column 3 in 0.5 to 0.95, column 4 in 0.05 to 0.3.
All inputs are finite; a program needn't handle non-finite values.
Results may differ from the reference program's by a relative error of at most 0.0003.
Values sent between devices are 32-bit elements; how exact they have to be, the bound alone decides.
A program may use at most 128 MiB of HBM per device.

```python
import jax
import jax.numpy as jnp
from jax import lax

NYC = 128
ZONES = 8
STEPS = 2
NYF = 384
NXC = 32
NXF = 96
NZF = 64
NZC = 128


def draw_zone_table(key, part):
    lower_edge = jnp.array([0.5, 0.1, 0.1, 0.5, 0.05], jnp.float32)
    upper_edge = jnp.array([1.0, 0.3, 0.3, 0.95, 0.3], jnp.float32)
    unit = jax.random.uniform(jax.random.fold_in(key, 17), (ZONES, 5), jnp.float32)
    return lower_edge + (upper_edge - lower_edge) * unit


def with_ends(values, rng, least, largest):
    extent = values.shape
    spot = [jax.random.randint(jax.random.fold_in(rng, axis), (), 0, extent[axis]) for axis in range(len(extent))]
    values = values.at[tuple(spot)].set(least)
    longest = extent.index(max(extent))
    spot[longest] = (spot[longest] + 1) % extent[longest]
    return values.at[tuple(spot)].set(largest)


def levels(stream_key, shape, pieces, low, high):
    factor_of, own = 1.0, jax.random.fold_in(stream_key, 6)
    for dim, blocks in pieces:
        draws = jnp.exp(jax.random.uniform(jax.random.fold_in(own, dim), (blocks,), jnp.float32, low / len(pieces), high / len(pieces)))
        factor_of = factor_of * jnp.repeat(draws, shape[dim] // blocks).reshape([-1 if axis == dim else 1 for axis in range(len(shape))])
    return factor_of


def noise(key, dims, scale, limit, cuts=(), kind=jnp.bfloat16):
    drawn = jax.random.normal(key, dims, jnp.float32) * scale
    if len(cuts) > 0:
        drawn = levels(key, dims, cuts, -0.22, 0.18) * drawn
    return jnp.clip(drawn, min=-limit, max=limit).astype(kind)


def setup_inputs(seed: int = 0) -> dict:
    seeds = jax.random.split(jax.random.key(seed), 14)
    return {
        "velocity_fine": noise(seeds[0], (3, NXF, NZF, NYF), 1.0, 6.0, ((1, 8), (2, 4)), jnp.float32),
        "stress_fine": noise(seeds[1], (6, NXF, NZF, NYF), 1.0, 6.0, ((1, 8), (2, 4)), jnp.float32),
        "memory_fine": noise(seeds[2], (6, NXF, NZF, NYF), 0.3, 1.8, ((1, 8), (2, 4)), jnp.float32),
        "peak_fine": jnp.clip(12.0 * jax.random.uniform(seeds[3], (NXF, NZF, NYF), jnp.float32) ** levels(seeds[3], (NXF, NZF, NYF), ((0, 8), (1, 4)), -0.2, 0.2), 0.0, 12.0),
        "zone_fine": with_ends(jax.random.randint(seeds[4], (NXF, NZF, NYF), 0, ZONES), jax.random.fold_in(seeds[4], 1), 0, ZONES - 1).astype(jnp.int32),
        "velocity_coarse": noise(seeds[5], (3, NXC, NZC, NYC), 1.0, 6.0, ((1, 8), (2, 4)), jnp.float32),
        "stress_coarse": noise(seeds[6], (6, NXC, NZC, NYC), 1.0, 6.0, ((1, 8), (2, 4)), jnp.float32),
        "memory_coarse": noise(seeds[7], (6, NXC, NZC, NYC), 0.3, 1.8, ((1, 8), (2, 4)), jnp.float32),
        "peak_coarse": jnp.clip(12.0 * jax.random.uniform(seeds[8], (NXC, NZC, NYC), jnp.float32) ** levels(seeds[8], (NXC, NZC, NYC), ((0, 8), (1, 4)), -0.2, 0.2), 0.0, 12.0),
        "zone_coarse": with_ends(jax.random.randint(seeds[9], (NXC, NZC, NYC), 0, ZONES), jax.random.fold_in(seeds[9], 1), 0, ZONES - 1).astype(jnp.int32),
        "zone_table": draw_zone_table(jax.random.fold_in(seeds[13], 71), 0),
        "interp_weight": with_ends(jax.random.randint(seeds[11], (2, 3), 0, 9), jax.random.fold_in(seeds[11], 1), 0, 8).astype(jnp.int32),
        "restrict_weight": with_ends(jax.random.randint(seeds[12], (2, 3), 1, 9), jax.random.fold_in(seeds[12], 1), 1, 8).astype(jnp.int32),
    }


time_step = 0.4
near_coef = 9.0 / 8.0
far_coef = 1.0 / 24.0

def shifted(field, axis, offset):
    index = [slice(None), slice(2, -2), slice(2, -2), slice(2, -2)]
    index[axis] = slice(2 + offset, field.shape[axis] - 2 + offset)
    return field[tuple(index)]

def forward(field, axis):
    return near_coef * (shifted(field, axis, 1) - shifted(field, axis, 0)) - far_coef * (shifted(field, axis, 2) - shifted(field, axis, -1))

def backward(field, axis):
    return near_coef * (shifted(field, axis, 0) - shifted(field, axis, -1)) - far_coef * (shifted(field, axis, 1) - shifted(field, axis, -2))

def materials(zone, zone_table):
    columns = []
    for column in range(5):
        value = jnp.zeros(zone.shape, jnp.float32)
        for level in range(zone_table.shape[0]):
            value = jnp.where(zone == level, zone_table[level, column], value)
        columns.append(value)
    return columns

def velocity_update(padded, velocity, buoyancy, spacing):

    def part(index):
        return padded[index:index + 1]
    accel_x = forward(part(0), 1) + backward(part(3), 3) + backward(part(4), 2)
    accel_y = backward(part(3), 1) + forward(part(1), 3) + backward(part(5), 2)
    accel_z = backward(part(4), 1) + backward(part(5), 3) + forward(part(2), 2)
    accel = jnp.concatenate([accel_x, accel_y, accel_z], axis=0)
    return velocity + time_step / spacing * buoyancy[None] * accel

def stress_update(padded, stress, memory, props, spacing):
    lame, shear, decay, damping = (props[1][None], props[2][None], props[3][None], props[4][None])

    def part(index):
        return padded[index:index + 1]
    normal_x = backward(part(0), 1)
    normal_y = backward(part(1), 3)
    normal_z = backward(part(2), 2)
    shear_xy = 0.5 * (forward(part(0), 3) + forward(part(1), 1))
    shear_xz = 0.5 * (forward(part(0), 2) + forward(part(2), 1))
    shear_yz = 0.5 * (forward(part(1), 2) + forward(part(2), 3))
    volume = normal_x + normal_y + normal_z
    rate = jnp.concatenate([lame * volume + 2.0 * shear * normal_x, lame * volume + 2.0 * shear * normal_y, lame * volume + 2.0 * shear * normal_z, 2.0 * shear * shear_xy, 2.0 * shear * shear_xz, 2.0 * shear * shear_yz], axis=0) / spacing
    memory_next = decay * memory - damping * (1.0 - decay) * rate
    stress_next = stress + time_step * (rate + 0.5 * (memory + memory_next))
    return (stress_next, memory_next)

def entry_key(first, second):
    return (min(first, second), max(first, second))

def rotate(entries, first, second):
    other = 3 - first - second
    pivot = entries[first, second]
    gap = entries[second, second] - entries[first, first]
    denominator = jnp.abs(gap) + jnp.sqrt(gap * gap + 4.0 * pivot * pivot)
    direction = jnp.where(gap >= 0, 1.0, -1.0)
    usable = denominator > 0
    tangent = jnp.where(usable, 2.0 * pivot * direction / jnp.where(usable, denominator, 1.0), 0.0)
    cosine = 1.0 / jnp.sqrt(1.0 + tangent * tangent)
    sine = tangent * cosine
    low_entry = entries[entry_key(other, first)]
    high_entry = entries[entry_key(other, second)]
    result = dict(entries)
    result[first, first] = entries[first, first] - tangent * pivot
    result[second, second] = entries[second, second] + tangent * pivot
    result[first, second] = jnp.zeros_like(pivot)
    result[entry_key(other, first)] = cosine * low_entry - sine * high_entry
    result[entry_key(other, second)] = sine * low_entry + cosine * high_entry
    return result

def strain_peak(stress, props, peak):
    lame, shear = (props[1], props[2])
    trace = stress[0] + stress[1] + stress[2]
    isotropic = lame * trace / (3.0 * lame + 2.0 * shear)
    scale = 0.5 / shear
    entries = {(0, 0): (stress[0] - isotropic) * scale, (1, 1): (stress[1] - isotropic) * scale, (2, 2): (stress[2] - isotropic) * scale, (0, 1): stress[3] * scale, (0, 2): stress[4] * scale, (1, 2): stress[5] * scale}
    for sweep in range(3):
        entries = rotate(entries, 0, 1)
        entries = rotate(entries, 0, 2)
        entries = rotate(entries, 1, 2)
    principal = jnp.maximum(jnp.maximum(entries[0, 0], entries[1, 1]), entries[2, 2])
    return jnp.maximum(peak, principal)

def make_tables(interp_weight, restrict_weight, coarse_cells):
    x_share = interp_weight[0].astype(jnp.float32) / 8.0
    y_share = interp_weight[1].astype(jnp.float32) / 8.0
    x_weight = restrict_weight[0].astype(jnp.float32)
    y_weight = restrict_weight[1].astype(jnp.float32)
    coarse_index = lax.broadcasted_iota(jnp.int32, (coarse_cells, 3 * coarse_cells), 0)
    fine_index = lax.broadcasted_iota(jnp.int32, (coarse_cells, 3 * coarse_cells), 1)
    phase = fine_index % 3
    block = fine_index // 3
    y_interp = jnp.where(phase == 0, y_share[0], jnp.where(phase == 1, y_share[1], y_share[2]))
    y_restrict = jnp.where(phase == 0, y_weight[0], jnp.where(phase == 1, y_weight[1], y_weight[2]))
    y_spread = jnp.where(coarse_index == block, y_interp, 0.0) + jnp.where(coarse_index == block + 1, 1.0 - y_interp, 0.0)
    y_gather = jnp.where(coarse_index == block, y_restrict, 0.0).T
    normaliser = 3.0 * jnp.sum(x_weight) * jnp.sum(y_weight)
    return (x_share, y_spread, x_weight, y_gather, normaliser)

def interpolate(planes, tables):
    x_share, y_spread = (tables[0], tables[1])
    upper = planes[:, :, 0:1]
    lower = planes[:, :, 1:2]
    layered = jnp.concatenate([(2.0 * upper + lower) / 3.0, (upper + 2.0 * lower) / 3.0], axis=2)
    share = x_share[None, None, :, None, None]
    across = share * layered[:, :-1, None] + (1.0 - share) * layered[:, 1:, None]
    count, rows = (across.shape[0], across.shape[1])
    flat = across.reshape(count * rows * 6, -1)
    spread = jnp.dot(flat, y_spread, precision=lax.Precision.HIGHEST)
    return spread.reshape(count, rows * 3, 2, -1)

def restrict(block, tables):
    x_weight, y_gather, normaliser = (tables[2], tables[3], tables[4])
    count, rows = (block.shape[0], block.shape[1])
    layers = lax.optimization_barrier(jnp.sum(block.reshape(count, rows, 2, 3, -1), axis=3))
    grouped = layers.reshape(count, rows // 3, 3, 2, -1)
    across = lax.optimization_barrier(jnp.sum(x_weight[None, None, :, None, None] * grouped, axis=2))
    flat = across.reshape(count * (rows // 3) * 2, -1)
    gathered = jnp.dot(flat, y_gather, precision=lax.Precision.HIGHEST)
    return gathered.reshape(count, rows // 3, 2, -1) / normaliser

def pad_fine(fine, coarse, tables):
    planes = jnp.pad(coarse[:, :, 0:2], ((0, 0), (0, 1), (0, 0), (0, 0)))
    ghost = interpolate(planes, tables)
    column = jnp.concatenate([jnp.zeros_like(fine[:, :, 0:2]), fine, ghost], axis=2)
    return jnp.pad(column, ((0, 0), (2, 2), (0, 0), (2, 2)))

def pad_coarse(coarse, fine, tables):
    ghost = restrict(fine[:, :, -6:], tables)
    column = jnp.concatenate([ghost, coarse, jnp.zeros_like(coarse[:, :, 0:2])], axis=2)
    return jnp.pad(column, ((0, 0), (2, 2), (0, 0), (2, 2)))

def reference(velocity_fine, stress_fine, memory_fine, peak_fine, zone_fine, velocity_coarse, stress_coarse, memory_coarse, peak_coarse, zone_coarse, zone_table, interp_weight, restrict_weight):
    tables = make_tables(interp_weight, restrict_weight, stress_coarse.shape[3])
    props_fine = materials(zone_fine, zone_table)
    props_coarse = materials(zone_coarse, zone_table)
    for step in range(STEPS):
        padded_fine = pad_fine(stress_fine, stress_coarse, tables)
        padded_coarse = pad_coarse(stress_coarse, stress_fine, tables)
        velocity_fine = velocity_update(padded_fine, velocity_fine, props_fine[0], 1.0)
        velocity_coarse = velocity_update(padded_coarse, velocity_coarse, props_coarse[0], 3.0)
        padded_fine = pad_fine(velocity_fine, velocity_coarse, tables)
        padded_coarse = pad_coarse(velocity_coarse, velocity_fine, tables)
        stress_fine, memory_fine = stress_update(padded_fine, stress_fine, memory_fine, props_fine, 1.0)
        stress_coarse, memory_coarse = stress_update(padded_coarse, stress_coarse, memory_coarse, props_coarse, 3.0)
        peak_fine = strain_peak(stress_fine, props_fine, peak_fine)
        peak_coarse = strain_peak(stress_coarse, props_coarse, peak_coarse)
    return (velocity_fine, stress_fine, memory_fine, peak_fine, velocity_coarse, stress_coarse, memory_coarse, peak_coarse)
```

```python
import functools

import jax
import jax.numpy as jnp
from jax import lax
from jax.experimental import pallas as pl
from jax.experimental.pallas import tpu as pltpu
from jax.sharding import PartitionSpec as P

STEPS = 2
LANES = 128
ROWS = 8

TIME_STEP = 0.4
NEAR = 9.0 / 8.0
FAR = 1.0 / 27.0
TINY = 1e-18

FORWARD = (1, 2)
BACKWARD = (2, 1)
STRESS_X = ((0, FORWARD), (3, BACKWARD), (4, BACKWARD))
STRESS_Z = ((4, BACKWARD), (5, BACKWARD), (2, FORWARD))
VELOCITY_X = ((0, BACKWARD), (1, FORWARD), (2, FORWARD))
VELOCITY_Z = ((0, FORWARD), (1, FORWARD), (2, BACKWARD))

BUOYANCY, LAME, SHEAR, DECAY, DAMPING, VOLUMETRIC, SCALE = range(7)

MESH = pl.DeviceIdType.MESH
EXACT = lax.Precision.HIGHEST


def zone_columns(table_ref):
    lane = lax.broadcasted_iota(jnp.int32, (ROWS, LANES), 1)
    columns = []
    for column in range(table_ref.shape[1]):
        value = jnp.full((ROWS, LANES), table_ref[0, column], jnp.float32)
        for level in range(1, table_ref.shape[0]):
            value = jnp.where(lane == level, table_ref[level, column], value)
        columns.append(value)
    return columns


def strain_tables(columns):
    lame, shear = columns[1], columns[2]
    return [lame / (3.0 * lame + 2.0 * shear), 0.5 / shear]


def step_tables(columns, spacing):
    buoyancy, lame, shear, decay, damping = columns
    return [
        buoyancy * (TIME_STEP * NEAR / spacing),
        lame * (NEAR / spacing),
        shear * (2.0 * NEAR / spacing),
        decay,
        damping * (1.0 - decay),
    ]


def lookup(table, zone):
    parts = [
        jnp.take_along_axis(
            table, zone[begin : begin + ROWS], axis=1, mode="promise_in_bounds"
        )
        for begin in range(0, zone.shape[0], ROWS)
    ]
    return jnp.concatenate(parts, axis=0)


def rotation(low, high, pivot):
    half = 0.5 * (high - low)
    size = jnp.maximum(jnp.abs(half), TINY)
    square = size * size + pivot * pivot
    radius = square * lax.rsqrt(square)
    reach = size + radius
    weight = lax.rsqrt((radius + radius) * reach)
    sign = jnp.where(half >= 0, 1.0, -1.0)
    middle = low + half
    offset = sign * radius
    return reach * weight, sign * (pivot * weight), middle - offset, middle + offset


def largest(low, high, pivot):
    half = 0.5 * (high - low)
    size = jnp.maximum(jnp.abs(half), TINY)
    square = size * size + pivot * pivot
    return low + half + square * lax.rsqrt(square)


def principal(stress, volumetric, scale):
    a00, a11, a22, a01, a02, a12 = stress
    shift = volumetric * (a00 + a11 + a22)
    cosine, sine, a00, a11 = rotation(a00, a11, a01)
    a02, a12 = cosine * a02 - sine * a12, sine * a02 + cosine * a12
    for sweep in range(3):
        if sweep > 0:
            cosine, sine, a00, a11 = rotation(a00, a11, a01)
            a02, a12 = cosine * a02, sine * a02
        cosine, sine, a00, a22 = rotation(a00, a22, a02)
        a01, a12 = -(sine * a12), cosine * a12
        if sweep < 2:
            cosine, sine, a11, a22 = rotation(a11, a22, a12)
            a01, a02 = cosine * a01, sine * a01
    return (jnp.maximum(a00, largest(a11, a22, a12)) - shift) * scale


def shifted_y(tiles, offset):
    lane = lax.broadcasted_iota(jnp.int32, tiles[0].shape, 1)
    rolled = [pltpu.roll(tile, (-offset) % LANES, 1) for tile in tiles]
    zero = jnp.zeros_like(tiles[0])
    if offset > 0:
        outside, beside = lane >= LANES - offset, rolled[1:] + [zero]
    else:
        outside, beside = lane < -offset, [zero] + rolled[:-1]
    return [jnp.where(outside, other, own) for other, own in zip(beside, rolled)]


def difference_y(tiles, kind):
    if kind == FORWARD:
        near = [a - b for a, b in zip(shifted_y(tiles, 1), tiles)]
        far = [a - b for a, b in zip(shifted_y(tiles, 2), shifted_y(tiles, -1))]
    else:
        near = [a - b for a, b in zip(tiles, shifted_y(tiles, -1))]
        far = [a - b for a, b in zip(shifted_y(tiles, 1), shifted_y(tiles, -2))]
    return list(zip(near, far))


def difference(at, kind):
    if kind == FORWARD:
        return at(1) - at(0), at(2) - at(-1)
    return at(0) - at(-1), at(1) - at(-2)


def total(*pairs):
    near = sum(pair[0] for pair in pairs[1:]) + pairs[0][0]
    far = sum(pair[1] for pair in pairs[1:]) + pairs[0][1]
    return near - FAR * far


class Field:
    def __init__(self, spacing, refs):
        self.spacing = spacing
        (
            self.stress,
            self.velocity,
            self.memory,
            self.peak,
            self.zone,
            self.props,
            self.below_x,
            self.above_x,
            self.around_z,
        ) = refs
        self.tiles, self.rows, self.depth, _ = self.peak.shape

    def cells(self, ref, part, tile, row, dx=0, dz=0):
        return ref[part, tile, row + (2 + dx), pl.ds(ROWS + dz, self.depth), :]

    def along_x(self, ref, part, tile, row, kind):
        return difference(lambda d: self.cells(ref, part, tile, row, dx=d), kind)

    def along_z(self, ref, part, tile, row, kind):
        return difference(lambda d: self.cells(ref, part, tile, row, dz=d), kind)

    def along_y(self, ref, part, row, kind):
        tiles = [self.cells(ref, part, tile, row) for tile in range(self.tiles)]
        return difference_y(tiles, kind)

    def each_row(self, body, begin=0, end=None):
        def step(row, carry):
            body(row)
            return carry

        lax.fori_loop(begin, self.rows if end is None else end, step, 0)

    def clear(self):
        stress, velocity, depth = self.stress, self.velocity, self.depth
        tile_zero = jnp.zeros((ROWS, LANES), jnp.float32)
        zero = jnp.zeros((depth, LANES), jnp.float32)

        def body(row):
            for tile in range(self.tiles):
                for ref, parts in ((stress, (2, 4, 5)), (velocity, (0, 1, 2))):
                    for part in parts:
                        ref[part, tile, row + 2, 0:ROWS, :] = tile_zero
                        ref[part, tile, row + 2, pl.ds(ROWS + depth, ROWS), :] = tile_zero
                for turn in range(2 * STEPS):
                    for slot in range(3):
                        self.around_z[turn, slot, tile, row, pl.ds(ROWS, ROWS), :] = tile_zero

        self.each_row(body)
        for tile in range(self.tiles):
            for ref, parts in ((stress, (0, 3, 4)), (velocity, (0, 1, 2))):
                for part in parts:
                    for row in (0, 1, self.rows + 2, self.rows + 3):
                        ref[part, tile, row, pl.ds(ROWS, depth), :] = zero

    def clear_x(self, side):
        ref = self.below_x if side == 0 else self.above_x
        zero = jnp.zeros((self.depth, LANES), jnp.float32)

        def body(turn, carry):
            for slot in range(3):
                for tile in range(self.tiles):
                    for row in range(2):
                        ref[turn, slot, tile, row] = zero
            return carry

        lax.fori_loop(0, 2 * STEPS, body, 0)

    def clear_z(self, side):
        zero = jnp.zeros((ROWS, LANES), jnp.float32)

        def body(row):
            for turn in range(2 * STEPS):
                for slot in range(3):
                    for tile in range(self.tiles):
                        self.around_z[turn, slot, tile, row, pl.ds(2 * ROWS * side, ROWS), :] = zero

        self.each_row(body)

    def fill_props(self, columns):
        tables = step_tables(columns, self.spacing) + strain_tables(columns)

        def body(row):
            for tile in range(self.tiles):
                zone = self.zone[tile, row]
                for index, table in enumerate(tables):
                    self.props[index, tile, row] = lookup(table, zone)

        self.each_row(body)

    def velocity_inner(self, row):
        stress, velocity = self.stress, self.velocity
        across = [
            self.along_y(stress, 3, row, BACKWARD),
            self.along_y(stress, 1, row, FORWARD),
            self.along_y(stress, 5, row, BACKWARD),
        ]
        for part in range(3):
            for tile in range(self.tiles):
                (field_x, kind_x), (field_z, kind_z) = STRESS_X[part], STRESS_Z[part]
                accel = total(
                    self.along_x(stress, field_x, tile, row, kind_x),
                    across[part][tile],
                    self.along_z(stress, field_z, tile, row, kind_z),
                )
                old = self.cells(velocity, part, tile, row)
                buoyancy = self.props[BUOYANCY, tile, row]
                velocity[part, tile, row + 2, pl.ds(ROWS, self.depth), :] = old + buoyancy * accel

    def outer_rows(self, turn, slot, tile, kind):
        below, above = self.below_x.at[turn, slot, tile], self.above_x.at[turn, slot, tile]
        last = self.rows - 1
        if kind == FORWARD:
            return [
                (0, FAR * below[1]),
                (last, above[0] - FAR * above[1]),
                (last - 1, -FAR * above[0]),
            ]
        return [
            (0, FAR * below[0] - below[1]),
            (1, FAR * below[1]),
            (last, -FAR * above[0]),
        ]

    def outer_layers(self, turn, slot, tile, row, kind):
        at = self.around_z.at[turn, slot, tile, row]

        def lower(distance):
            return at[pl.ds(ROWS - distance, ROWS), :]

        def upper(distance):
            return at[pl.ds(ROWS + distance, ROWS), :]

        if kind == FORWARD:
            return FAR * lower(1), upper(1) - FAR * upper(2)
        return FAR * lower(2) - lower(1), -FAR * upper(1)

    def ends(self):
        return (0, self.depth - ROWS)

    def velocity_outer(self, turn):
        velocity, depth = self.velocity, self.depth
        for part in range(3):
            for tile in range(self.tiles):
                for row, term in self.outer_rows(turn, part, tile, STRESS_X[part][1]):
                    place = velocity.at[part, tile, row + 2, pl.ds(ROWS, depth), :]
                    place[...] = place[...] + self.props[BUOYANCY, tile, row] * term

        def body(row):
            for part in range(3):
                for tile in range(self.tiles):
                    terms = self.outer_layers(turn, part, tile, row, STRESS_Z[part][1])
                    for begin, term in zip(self.ends(), terms):
                        place = velocity.at[part, tile, row + 2, pl.ds(ROWS + begin, ROWS), :]
                        buoyancy = self.props[BUOYANCY, tile, row, pl.ds(begin, ROWS), :]
                        place[...] = place[...] + buoyancy * term

        self.each_row(body)

    def stress_inner(self, row):
        velocity, stress, memory = self.velocity, self.stress, self.memory
        across_y = self.along_y(velocity, 1, row, BACKWARD)
        across_x = self.along_y(velocity, 0, row, FORWARD)
        across_z = self.along_y(velocity, 2, row, FORWARD)
        for tile in range(self.tiles):
            lame, shear, decay, damping = (
                self.props[index, tile, row] for index in (LAME, SHEAR, DECAY, DAMPING)
            )
            normal_x = total(self.along_x(velocity, 0, tile, row, BACKWARD))
            normal_y = total(across_y[tile])
            normal_z = total(self.along_z(velocity, 2, tile, row, BACKWARD))
            shear_xy = total(across_x[tile], self.along_x(velocity, 1, tile, row, FORWARD))
            shear_xz = total(
                self.along_z(velocity, 0, tile, row, FORWARD),
                self.along_x(velocity, 2, tile, row, FORWARD),
            )
            shear_yz = total(across_z[tile], self.along_z(velocity, 1, tile, row, FORWARD))
            volume = lame * (normal_x + normal_y + normal_z)
            half = 0.5 * shear
            rates = [
                volume + shear * normal_x,
                volume + shear * normal_y,
                volume + shear * normal_z,
                half * shear_xy,
                half * shear_xz,
                half * shear_yz,
            ]
            kept = 0.5 * TIME_STEP * (1.0 + decay)
            gained = TIME_STEP - 0.5 * TIME_STEP * damping
            for part, rate in enumerate(rates):
                past = memory[part, tile, row]
                memory[part, tile, row] = decay * past - damping * rate
                old = self.cells(stress, part, tile, row)
                stress[part, tile, row + 2, pl.ds(ROWS, self.depth), :] = (
                    old + kept * past + gained * rate
                )

    def add_rates(self, rates, tile, row, begin, count):
        damping = self.props[DAMPING, tile, row, pl.ds(begin, count), :]
        gained = TIME_STEP - 0.5 * TIME_STEP * damping
        for part, rate in rates:
            place = self.memory.at[part, tile, row, pl.ds(begin, count), :]
            place[...] = place[...] - damping * rate
            place = self.stress.at[part, tile, row + 2, pl.ds(ROWS + begin, count), :]
            place[...] = place[...] + gained * rate

    def normal_rates(self, term, along, tile, row, begin, count):
        lame = self.props[LAME, tile, row, pl.ds(begin, count), :]
        shear = self.props[SHEAR, tile, row, pl.ds(begin, count), :]
        volume = lame * term
        return [(part, volume + shear * term if part == along else volume) for part in range(3)]

    def shear_rates(self, term, part, tile, row, begin, count):
        shear = self.props[SHEAR, tile, row, pl.ds(begin, count), :]
        return [(part, (0.5 * shear) * term)]

    def stress_outer(self, turn):
        depth = self.depth
        for tile in range(self.tiles):
            for row, term in self.outer_rows(turn, 0, tile, BACKWARD):
                rates = self.normal_rates(term, 0, tile, row, 0, depth)
                self.add_rates(rates, tile, row, 0, depth)
            for slot, part in ((1, 3), (2, 4)):
                for row, term in self.outer_rows(turn, slot, tile, FORWARD):
                    rates = self.shear_rates(term, part, tile, row, 0, depth)
                    self.add_rates(rates, tile, row, 0, depth)

        def body(row):
            for tile in range(self.tiles):
                normal = self.outer_layers(turn, 2, tile, row, BACKWARD)
                shear_xz = self.outer_layers(turn, 0, tile, row, FORWARD)
                shear_yz = self.outer_layers(turn, 1, tile, row, FORWARD)
                for end, begin in enumerate(self.ends()):
                    rates = (
                        self.normal_rates(normal[end], 2, tile, row, begin, ROWS)
                        + self.shear_rates(shear_xz[end], 4, tile, row, begin, ROWS)
                        + self.shear_rates(shear_yz[end], 5, tile, row, begin, ROWS)
                    )
                    self.add_rates(rates, tile, row, begin, ROWS)

        self.each_row(body)

    def raise_peak(self, row):
        for tile in range(self.tiles):
            strain = principal(
                [self.cells(self.stress, part, tile, row) for part in range(6)],
                self.props[VOLUMETRIC, tile, row],
                self.props[SCALE, tile, row],
            )
            self.peak[tile, row] = jnp.maximum(self.peak[tile, row], strain)


def spread_matrix(interp_ref, coarse_cells, fine_cells):
    coarse = lax.broadcasted_iota(jnp.int32, (coarse_cells, fine_cells), 0)
    fine = lax.broadcasted_iota(jnp.int32, (coarse_cells, fine_cells), 1)
    matrix = jnp.zeros((coarse_cells, fine_cells), jnp.float32)
    for phase in range(3):
        share = interp_ref[1, phase].astype(jnp.float32) / 8.0
        matrix = jnp.where(fine == 3 * coarse + phase, share, matrix)
        matrix = jnp.where(fine == 3 * coarse - 3 + phase, 1.0 - share, matrix)
    return matrix


def gather_matrix(restrict_ref, coarse_cells, fine_cells):
    fine = lax.broadcasted_iota(jnp.int32, (fine_cells, coarse_cells), 0)
    coarse = lax.broadcasted_iota(jnp.int32, (fine_cells, coarse_cells), 1)
    matrix = jnp.zeros((fine_cells, coarse_cells), jnp.float32)
    for phase in range(3):
        weight = restrict_ref[1, phase].astype(jnp.float32)
        matrix = jnp.where(fine == 3 * coarse + phase, weight, matrix)
    return matrix


def lift_matrix(interp_ref, fine_rows, rows):
    target = lax.broadcasted_iota(jnp.int32, (2 * fine_rows, 2 * rows), 0)
    source = lax.broadcasted_iota(jnp.int32, (2 * fine_rows, 2 * rows), 1)
    matrix = jnp.zeros((2 * fine_rows, 2 * rows), jnp.float32)
    for phase in range(3):
        share = interp_ref[0, phase].astype(jnp.float32) / 8.0
        for ghost in range(2):
            for layer in range(2):
                blend = (2.0 if ghost == layer else 1.0) / 3.0
                for ahead in range(2):
                    weight = (share if ahead == 0 else 1.0 - share) * blend
                    base = 6 * (source - layer * rows - ahead) + 2 * phase + ghost
                    inside = (source >= layer * rows + ahead) & (source < (layer + 1) * rows)
                    matrix = jnp.where((target == base) & inside, weight, matrix)
    return matrix


class Coupling:
    def __init__(self, fine, coarse, interp_ref, restrict_ref, refs):
        self.fine, self.coarse = fine, coarse
        self.interp_ref, self.restrict_ref = interp_ref, restrict_ref
        self.heads, self.lifted, self.layers, self.spread, self.gather = refs
        self.block = self.heads.shape[2] // 2

    def clear(self):
        coarse_cells, fine_cells = self.spread.shape
        self.spread[...] = spread_matrix(self.interp_ref, coarse_cells, fine_cells)
        self.gather[...] = gather_matrix(self.restrict_ref, coarse_cells, fine_cells)

    def restrict(self, turn, ref, along_z):
        fine, coarse = self.fine, self.coarse
        weight = [self.restrict_ref[0, phase].astype(jnp.float32) for phase in range(3)]
        weight_y = [self.restrict_ref[1, phase].astype(jnp.float32) for phase in range(3)]
        mass = 3.0 * (weight[0] + weight[1] + weight[2]) * (weight_y[0] + weight_y[1] + weight_y[2])
        for slot, (part, _) in enumerate(along_z):
            for row in range(coarse.rows):
                begin = (slot * coarse.rows + row) * ROWS
                for tile in range(fine.tiles):
                    block = sum(
                        weight[phase]
                        * ref[part, tile, 2 + 3 * row + phase, pl.ds(fine.depth, ROWS), :]
                        for phase in range(3)
                    )
                    self.layers[begin : begin + ROWS, tile * LANES : (tile + 1) * LANES] = block
        gathered = jnp.dot(
            self.layers[...], self.gather[...], precision=EXACT, preferred_element_type=jnp.float32
        )
        gathered = gathered / jnp.full(gathered.shape, mass, jnp.float32)
        for slot in range(3):
            for row in range(coarse.rows):
                begin = (slot * coarse.rows + row) * ROWS
                for tile in range(coarse.tiles):
                    block = gathered[begin : begin + ROWS, tile * LANES : (tile + 1) * LANES]
                    block = block + pltpu.roll(block, 1, 0) + pltpu.roll(block, 2, 0)
                    self.lifted[turn, slot, tile, row, 6:7, :] = block[4:5]
                    self.lifted[turn, slot, tile, row, 7:8, :] = block[7:8]

    def interpolate(self, turn):
        fine = self.fine
        lift = lift_matrix(self.interp_ref, fine.rows, self.block)
        lifted = [
            jnp.dot(lift, self.heads[turn, slot], precision=EXACT, preferred_element_type=jnp.float32)
            for slot in range(3)
        ]
        ghosts = jnp.dot(
            jnp.concatenate(lifted, axis=0),
            self.spread[...],
            precision=EXACT,
            preferred_element_type=jnp.float32,
        )
        for slot in range(3):
            for row in range(fine.rows):
                begin = 2 * (slot * fine.rows + row)
                for tile in range(fine.tiles):
                    fine.around_z[turn, slot, tile, row, 2 * ROWS : 2 * ROWS + 2, :] = ghosts[
                        begin : begin + 2, tile * LANES : (tile + 1) * LANES
                    ]


class Place:
    def __init__(self):
        self.lat, self.depth = lax.axis_index("lat"), lax.axis_index("depth")
        self.lats, self.depths = lax.axis_size("lat"), lax.axis_size("depth")
        lat, depth = self.lat, self.depth
        has_next, has_previous = lat < self.lats - 1, lat > 0
        has_lower, has_upper = depth < self.depths - 1, depth > 0
        top, bottom = depth == 0, depth == self.depths - 1
        self.routes = {
            "head": (lat, self.depths - 1, top, bottom),
            "corner": (lat - 1, self.depths - 1, top & has_previous, bottom & has_next),
            "lift": (lat, 0, bottom, top),
            "next": (lat + 1, depth, has_next, has_previous),
            "previous": (lat - 1, depth, has_previous, has_next),
            "down": (lat, depth + 1, has_lower, has_upper),
            "up": (lat, depth - 1, has_upper, has_lower),
        }
        self.top, self.bottom = top, bottom

    def target(self, route):
        lat, depth = self.routes[route][:2]
        return {"lat": lat, "depth": depth}

    def greet(self):
        barrier = pltpu.get_barrier_semaphore()
        lat, depth = self.lat, self.depth
        peers = [
            (lat + 1, depth, lat < self.lats - 1),
            (lat - 1, depth, lat > 0),
            (lat, depth + 1, depth < self.depths - 1),
            (lat, depth - 1, depth > 0),
            (lat, self.depths - 1, self.top),
            (lat, 0, self.bottom),
            (lat - 1, self.depths - 1, self.top & (lat > 0)),
            (lat + 1, 0, self.bottom & (lat < self.lats - 1)),
        ]
        for peer_lat, peer_depth, present in peers:

            @pl.when(present)
            def _():
                pl.semaphore_signal(
                    barrier,
                    inc=1,
                    device_id={"lat": peer_lat, "depth": peer_depth},
                    device_id_type=MESH,
                )

        return barrier, sum(present.astype(jnp.int32) for _, _, present in peers)


class Exchange:
    def __init__(self, turn, place, fine, coarse, coupling, velocity, sems):
        self.place = place
        along_x = VELOCITY_X if velocity else STRESS_X
        along_z = VELOCITY_Z if velocity else STRESS_Z
        self.messages = {route: [] for route in place.routes}
        self.send_sems, self.recv_sems, self.count, self.turn = sems[0], sems[1], 0, turn
        ref = coarse.velocity if velocity else coarse.stress
        block = coupling.block
        for slot, (part, (low, _)) in enumerate(along_z):
            for layer in range(2):
                for tile in range(coarse.tiles):
                    source = ref.at[part, tile, :, ROWS + layer, :]
                    lanes = pl.ds(tile * LANES, LANES)
                    begin = layer * block
                    self.add(
                        "head",
                        source.at[pl.ds(2, coarse.rows), :],
                        coupling.heads.at[turn, slot, pl.ds(begin, coarse.rows), lanes],
                    )
                    self.add(
                        "corner",
                        source.at[pl.ds(2, 1), :],
                        coupling.heads.at[turn, slot, pl.ds(begin + coarse.rows, 1), lanes],
                    )
            self.add(
                "lift",
                coupling.lifted.at[turn, slot, :, :, pl.ds(ROWS - low, low), :],
                coarse.around_z.at[turn, slot, :, :, pl.ds(ROWS - low, low), :],
            )
        for grid in (fine, coarse):
            ref = grid.velocity if velocity else grid.stress
            inner = pl.ds(ROWS, grid.depth)
            for slot, (part, (low, high)) in enumerate(along_x):
                self.add(
                    "next",
                    ref.at[part, :, pl.ds(2 + grid.rows - low, low), inner, :],
                    grid.below_x.at[turn, slot, :, pl.ds(2 - low, low), :, :],
                )
                self.add(
                    "previous",
                    ref.at[part, :, pl.ds(2, high), inner, :],
                    grid.above_x.at[turn, slot, :, pl.ds(0, high), :, :],
                )
            for slot, (part, (low, high)) in enumerate(along_z):
                rows = pl.ds(2, grid.rows)
                self.add(
                    "down",
                    ref.at[part, :, rows, pl.ds(ROWS + grid.depth - low, low), :],
                    grid.around_z.at[turn, slot, :, :, pl.ds(ROWS - low, low), :],
                )
                self.add(
                    "up",
                    ref.at[part, :, rows, pl.ds(ROWS, high), :],
                    grid.around_z.at[turn, slot, :, :, pl.ds(2 * ROWS, high), :],
                )

    def add(self, route, source, target):
        copy = pltpu.make_async_remote_copy(
            src_ref=source,
            dst_ref=target,
            send_sem=self.send_sems.at[self.turn, self.count],
            recv_sem=self.recv_sems.at[self.turn, self.count],
            device_id=self.place.target(route),
            device_id_type=MESH,
        )
        self.messages[route].append(copy)
        self.count += 1

    def send(self, *routes):
        for route in routes or self.messages:

            @pl.when(self.place.routes[route][2])
            def _():
                for copy in self.messages[route]:
                    copy.start()

    def receive(self, *routes):
        for route in routes or self.messages:

            @pl.when(self.place.routes[route][3])
            def _():
                for copy in self.messages[route]:
                    copy.wait_recv()

    def sent(self):
        for route in self.messages:

            @pl.when(self.place.routes[route][2])
            def _():
                for copy in self.messages[route]:
                    copy.wait_send()


MESSAGES = 64


def waves_kernel(counts, *refs):
    refs = list(refs)

    def take(count):
        taken = refs[:count]
        del refs[:count]
        return taken

    table_ref, interp_ref, restrict_ref = take(3)
    inputs = [take(5), take(5)]
    outputs = [take(4), take(4)]
    fine, coarse = Field(1.0, take(9)), Field(3.0, take(9))
    coupling = Coupling(fine, coarse, interp_ref, restrict_ref, take(5))
    load_sems, store_sems, send_sems, recv_sems = take(4)
    place = Place()
    grids = (fine, coarse)

    loads, stores = {}, {}
    for grid, (velocity, stress, memory, peak, zone) in zip(grids, inputs):
        inner_rows, inner = pl.ds(2, grid.rows), pl.ds(ROWS, grid.depth)
        pairs = [
            ("zone", zone, grid.zone, None),
            ("stress", stress, grid.stress, inner),
            ("velocity", velocity, grid.velocity, inner),
            ("memory", memory, grid.memory, None),
            ("peak", peak, grid.peak, None),
        ]
        for name, source, target, padded in pairs:
            for tile in range(grid.tiles):
                lanes = pl.ds(tile * LANES, LANES)
                if name in ("zone", "peak"):
                    source_part, target_part = source.at[:, :, lanes], target.at[tile]
                elif padded is None:
                    source_part, target_part = source.at[:, :, :, lanes], target.at[:, tile]
                else:
                    source_part = source.at[:, :, :, lanes]
                    target_part = target.at[:, tile, inner_rows, padded, :]
                index = sum(len(group) for group in loads.values())
                copy = pltpu.make_async_copy(source_part, target_part, load_sems.at[index])
                loads.setdefault(name, []).append(copy)
    for grid, (velocity, stress, memory, peak) in zip(grids, outputs):
        inner_rows, inner = pl.ds(2, grid.rows), pl.ds(ROWS, grid.depth)
        for tile in range(grid.tiles):
            lanes = pl.ds(tile * LANES, LANES)
            for name, source_part, target_part in (
                ("velocity", grid.velocity.at[:, tile, inner_rows, inner, :], velocity.at[:, :, :, lanes]),
                ("stress", grid.stress.at[:, tile, inner_rows, inner, :], stress.at[:, :, :, lanes]),
                ("memory", grid.memory.at[:, tile], memory.at[:, :, :, lanes]),
                ("peak", grid.peak.at[tile], peak.at[:, :, lanes]),
            ):
                index = sum(len(group) for group in stores.values())
                copy = pltpu.make_async_copy(source_part, target_part, store_sems.at[index])
                stores.setdefault(name, []).append(copy)

    def start(group):
        for copy in group:
            copy.start()

    def finish(group):
        for copy in group:
            copy.wait()

    for name in ("zone", "stress", "velocity", "memory", "peak"):
        start(loads[name])
    coupling.heads[...] = jnp.zeros(coupling.heads.shape, jnp.float32)
    barrier, peers = place.greet()

    for grid in grids:
        grid.clear()

    @pl.when(place.top)
    def _():
        fine.clear_z(0)

    @pl.when(place.bottom)
    def _():
        coarse.clear_z(1)

    for side, outside in ((0, place.lat == 0), (1, place.lat == place.lats - 1)):

        @pl.when(outside)
        def _():
            for grid in grids:
                grid.clear_x(side)

    coupling.clear()
    columns = zone_columns(table_ref)
    finish(loads["zone"])
    for grid in grids:
        grid.fill_props(columns)
    finish(loads["stress"])
    pl.semaphore_wait(barrier, peers)

    turns = [
        Exchange(turn, place, fine, coarse, coupling, turn % 2 == 1, (send_sems, recv_sems))
        for turn in range(2 * STEPS)
    ]

    def open_turn(turn):
        velocity = turn % 2 == 1
        turns[turn].send("head", "corner")

        @pl.when(place.bottom)
        def _():
            coupling.restrict(
                turn,
                fine.velocity if velocity else fine.stress,
                VELOCITY_Z if velocity else STRESS_Z,
            )

        turns[turn].send("lift", "next", "previous", "down", "up")

    def close_turn(turn):
        turns[turn].receive()

        @pl.when(place.bottom)
        def _():
            coupling.interpolate(turn)

        for grid in grids:
            if turn % 2 == 1:
                grid.stress_outer(turn)
            else:
                grid.velocity_outer(turn)

    for step in range(STEPS):
        turn = 2 * step
        open_turn(turn)
        if step == 0:
            finish(loads["velocity"])
        else:
            turns[turn - 1].sent()
        for grid in grids:
            grid.each_row(grid.velocity_inner)
        if step > 0:
            fine.each_row(fine.raise_peak, 0, fine.rows // 2)
        close_turn(turn)
        open_turn(turn + 1)
        if step == 0:
            finish(loads["memory"])
            finish(loads["peak"])
        else:
            fine.each_row(fine.raise_peak, fine.rows // 2)
            coarse.each_row(coarse.raise_peak)
        if step == STEPS - 1:
            start(stores["velocity"])
            start(stores["peak"])
        turns[turn].sent()
        for grid in grids:
            grid.each_row(grid.stress_inner)
        close_turn(turn + 1)
    turns[2 * STEPS - 1].sent()
    start(stores["stress"])
    start(stores["memory"])
    for name in ("velocity", "peak", "stress", "memory"):
        finish(stores[name])


def finish_kernel(table_ref, *refs):
    inputs, outputs = [refs[0:5], refs[5:10]], [refs[10:14], refs[14:18]]
    columns = zone_columns(table_ref)
    tables = strain_tables(columns)
    for (velocity, stress, memory, peak, zone), (new_velocity, new_stress, new_memory, new_peak) in zip(
        inputs, outputs
    ):
        new_velocity[...] = velocity[...]
        new_memory[...] = memory[...]
        rows, _, cells = zone.shape
        for row in range(rows):
            for begin in range(0, cells, LANES):
                lanes = slice(begin, begin + LANES)
                level = zone[row, :, lanes]
                parts = [stress[part, row, :, lanes] for part in range(6)]
                strain = principal(parts, lookup(tables[0], level), lookup(tables[1], level))
                new_peak[row, :, lanes] = jnp.maximum(peak[row, :, lanes], strain)
                for part in range(6):
                    new_stress[part, row, :, lanes] = parts[part]


def shapes_of(velocity, stress, memory, peak):
    return [jax.ShapeDtypeStruct(a.shape, a.dtype) for a in (velocity, stress, memory, peak)]


def scratch_of(peak):
    rows, depth, cells = peak.shape
    tiles, turns = cells // LANES, 2 * STEPS
    full = (tiles, rows + 4, depth + 2 * ROWS, LANES)
    plain = (tiles, rows, depth, LANES)

    def buffer(*shape):
        return pltpu.VMEM(shape, jnp.float32)

    return [
        buffer(6, *full),
        buffer(3, *full),
        buffer(6, *plain),
        buffer(*plain),
        pltpu.VMEM(plain, jnp.int32),
        buffer(7, *plain),
        buffer(turns, 3, tiles, 2, depth, LANES),
        buffer(turns, 3, tiles, 2, depth, LANES),
        buffer(turns, 3, tiles, rows, 3 * ROWS, LANES),
    ]


def on_device(
    velocity_fine,
    stress_fine,
    memory_fine,
    peak_fine,
    zone_fine,
    velocity_coarse,
    stress_coarse,
    memory_coarse,
    peak_coarse,
    zone_coarse,
    zone_table,
    interp_weight,
    restrict_weight,
):
    fine = (velocity_fine, stress_fine, memory_fine, peak_fine)
    coarse = (velocity_coarse, stress_coarse, memory_coarse, peak_coarse)
    fine_rows, _, fine_cells = peak_fine.shape
    coarse_rows, _, coarse_cells = peak_coarse.shape
    block = ROWS * ((coarse_rows + ROWS) // ROWS)
    turns = 2 * STEPS
    hbm = pl.BlockSpec(memory_space=pl.ANY)
    smem = pl.BlockSpec(memory_space=pltpu.SMEM)
    shapes = shapes_of(*fine) + shapes_of(*coarse)
    tiles = fine_cells // LANES + coarse_cells // LANES
    state = pl.pallas_call(
        functools.partial(waves_kernel, None),
        out_shape=shapes,
        in_specs=[smem] * 3 + [hbm] * 10,
        out_specs=[hbm] * 8,
        scratch_shapes=[
            *scratch_of(peak_fine),
            *scratch_of(peak_coarse),
            pltpu.VMEM((turns, 3, 2 * block, coarse_cells), jnp.float32),
            pltpu.VMEM((turns, 3, coarse_cells // LANES, coarse_rows, ROWS, LANES), jnp.float32),
            pltpu.VMEM((3 * coarse_rows * ROWS, fine_cells), jnp.float32),
            pltpu.VMEM((coarse_cells, fine_cells), jnp.float32),
            pltpu.VMEM((fine_cells, coarse_cells), jnp.float32),
            pltpu.SemaphoreType.DMA((5 * tiles,)),
            pltpu.SemaphoreType.DMA((4 * tiles,)),
            pltpu.SemaphoreType.DMA((turns, MESSAGES)),
            pltpu.SemaphoreType.DMA((turns, MESSAGES)),
        ],
        compiler_params=pltpu.CompilerParams(
            collective_id=0, has_side_effects=True, vmem_limit_bytes=60 * 1024 * 1024
        ),
        name="waves",
    )(
        zone_table,
        interp_weight,
        restrict_weight,
        *fine,
        zone_fine,
        *coarse,
        zone_coarse,
    )

    def spec(array, rows):
        lead = array.ndim - 3
        shape = (*array.shape[:lead], rows, *array.shape[lead + 1 :])
        return pl.BlockSpec(shape, lambda i: (*([0] * lead), i, 0, 0))

    steps = coarse_rows
    specs_in, specs_out = [], []
    for grid_shapes, zone, rows in (
        (shapes[:4], zone_fine, fine_rows // steps),
        (shapes[4:], zone_coarse, coarse_rows // steps),
    ):
        specs = [spec(array, rows) for array in grid_shapes]
        specs_in += [*specs, spec(zone, rows)]
        specs_out += specs
    return tuple(
        pl.pallas_call(
            finish_kernel,
            grid=(steps,),
            out_shape=shapes,
            in_specs=[smem, *specs_in],
            out_specs=specs_out,
            compiler_params=pltpu.CompilerParams(vmem_limit_bytes=40 * 1024 * 1024),
            name="finish",
        )(zone_table, *state[:4], zone_fine, *state[4:], zone_coarse)
    )


def solution(mesh):
    field, scalar, whole = P(None, "lat", "depth", None), P("lat", "depth", None), P()
    return jax.shard_map(
        on_device,
        mesh=mesh,
        in_specs=(field, field, field, scalar, scalar) * 2 + (whole,) * 3,
        out_specs=(field, field, field, scalar) * 2,
        check_vma=False,
    )
```

```python
import functools

import jax
import jax.numpy as jnp
from jax import lax
from jax.experimental import pallas as pl
from jax.experimental.pallas import tpu as pltpu
from jax.sharding import PartitionSpec as P

STEPS = 2
LANES = 128
ROWS = 8

TIME_STEP = 0.4
NEAR = 9.0 / 8.0
FAR = 1.0 / 27.0
TINY = 1e-18

FORWARD = (1, 2)
BACKWARD = (2, 1)
STRESS_X = ((0, FORWARD), (3, BACKWARD), (4, BACKWARD))
STRESS_Z = ((4, BACKWARD), (5, BACKWARD), (2, FORWARD))
VELOCITY_X = ((0, BACKWARD), (1, FORWARD), (2, FORWARD))
VELOCITY_Z = ((0, FORWARD), (1, FORWARD), (2, BACKWARD))

BUOYANCY, LAME, SHEAR, DECAY, DAMPING, VOLUMETRIC, SCALE = range(7)

MESH = pl.DeviceIdType.MESH
EXACT = lax.Precision.HIGHEST


def zone_columns(table_ref):
    lane = lax.broadcasted_iota(jnp.int32, (ROWS, LANES), 1)
    columns = []
    for column in range(table_ref.shape[1]):
        value = jnp.full((ROWS, LANES), table_ref[0, column], jnp.float32)
        for level in range(1, table_ref.shape[0]):
            value = jnp.where(lane == level, table_ref[level, column], value)
        columns.append(value)
    return columns


def strain_tables(columns):
    lame, shear = columns[1], columns[2]
    return [lame / (3.0 * lame + 2.0 * shear), 0.5 / shear]


def step_tables(columns, spacing):
    buoyancy, lame, shear, decay, damping = columns
    return [
        buoyancy * (TIME_STEP * NEAR / spacing),
        lame * (NEAR / spacing),
        shear * (2.0 * NEAR / spacing),
        decay,
        damping * (1.0 - decay),
    ]


def lookup(table, zone):
    parts = [
        jnp.take_along_axis(
            table, zone[begin : begin + ROWS], axis=1, mode="promise_in_bounds"
        )
        for begin in range(0, zone.shape[0], ROWS)
    ]
    return jnp.concatenate(parts, axis=0)


def rotation(low, high, pivot):
    half = 0.5 * (high - low)
    size = jnp.maximum(jnp.abs(half), TINY)
    square = size * size + pivot * pivot
    radius = square * lax.rsqrt(square)
    reach = size + radius
    weight = lax.rsqrt((radius + radius) * reach)
    sign = jnp.where(half >= 0, 1.0, -1.0)
    middle = low + half
    offset = sign * radius
    return reach * weight, sign * (pivot * weight), middle - offset, middle + offset


def largest(low, high, pivot):
    half = 0.5 * (high - low)
    size = jnp.maximum(jnp.abs(half), TINY)
    square = size * size + pivot * pivot
    return low + half + square * lax.rsqrt(square)


def principal(stress, volumetric, scale):
    a00, a11, a22, a01, a02, a12 = stress
    shift = volumetric * (a00 + a11 + a22)
    cosine, sine, a00, a11 = rotation(a00, a11, a01)
    a02, a12 = cosine * a02 - sine * a12, sine * a02 + cosine * a12
    for sweep in range(3):
        if sweep > 0:
            cosine, sine, a00, a11 = rotation(a00, a11, a01)
            a02, a12 = cosine * a02, sine * a02
        cosine, sine, a00, a22 = rotation(a00, a22, a02)
        a01, a12 = -(sine * a12), cosine * a12
        if sweep < 2:
            cosine, sine, a11, a22 = rotation(a11, a22, a12)
            a01, a02 = cosine * a01, sine * a01
    return (jnp.maximum(a00, largest(a11, a22, a12)) - shift) * scale


def shifted_y(tiles, offset):
    lane = lax.broadcasted_iota(jnp.int32, tiles[0].shape, 1)
    rolled = [pltpu.roll(tile, (-offset) % LANES, 1) for tile in tiles]
    zero = jnp.zeros_like(tiles[0])
    if offset > 0:
        outside, beside = lane >= LANES - offset, rolled[1:] + [zero]
    else:
        outside, beside = lane < -offset, [zero] + rolled[:-1]
    return [jnp.where(outside, other, own) for other, own in zip(beside, rolled)]


def difference_y(tiles, kind):
    if kind == FORWARD:
        near = [a - b for a, b in zip(shifted_y(tiles, 1), tiles)]
        far = [a - b for a, b in zip(shifted_y(tiles, 2), shifted_y(tiles, -1))]
    else:
        near = [a - b for a, b in zip(tiles, shifted_y(tiles, -1))]
        far = [a - b for a, b in zip(shifted_y(tiles, 1), shifted_y(tiles, -2))]
    return list(zip(near, far))


def difference(at, kind):
    if kind == FORWARD:
        return at(1) - at(0), at(2) - at(-1)
    return at(0) - at(-1), at(1) - at(-2)


def total(*pairs):
    near = sum(pair[0] for pair in pairs[1:]) + pairs[0][0]
    far = sum(pair[1] for pair in pairs[1:]) + pairs[0][1]
    return near - FAR * far


class Field:
    def __init__(self, spacing, refs):
        self.spacing = spacing
        (
            self.stress,
            self.velocity,
            self.memory,
            self.peak,
            self.props,
            self.zone,
            self.below_x,
            self.above_x,
            self.around_z,
        ) = refs
        self.tiles, self.rows, self.depth, _ = self.peak.shape

    def cells(self, ref, part, tile, row, dx=0, dz=0):
        return ref[part, tile, row + (2 + dx), pl.ds(ROWS + dz, self.depth), :]

    def along_x(self, ref, part, tile, row, kind):
        return difference(lambda d: self.cells(ref, part, tile, row, dx=d), kind)

    def along_z(self, ref, part, tile, row, kind):
        return difference(lambda d: self.cells(ref, part, tile, row, dz=d), kind)

    def along_y(self, ref, part, row, kind):
        tiles = [self.cells(ref, part, tile, row) for tile in range(self.tiles)]
        return difference_y(tiles, kind)

    def each_row(self, body, begin=0, end=None):
        def step(row, carry):
            body(row)
            return carry

        lax.fori_loop(begin, self.rows if end is None else end, step, 0)

    def clear(self):
        stress, velocity, depth = self.stress, self.velocity, self.depth
        tile_zero = jnp.zeros((ROWS, LANES), jnp.float32)
        zero = jnp.zeros((depth, LANES), jnp.float32)

        def body(row):
            for tile in range(self.tiles):
                for ref, parts in ((stress, (2, 4, 5)), (velocity, (0, 1, 2))):
                    for part in parts:
                        ref[part, tile, row + 2, 0:ROWS, :] = tile_zero
                        ref[part, tile, row + 2, pl.ds(ROWS + depth, ROWS), :] = tile_zero
                for turn in range(2 * STEPS):
                    for slot in range(3):
                        self.around_z[turn, slot, tile, row, pl.ds(ROWS, ROWS), :] = tile_zero

        self.each_row(body)
        for tile in range(self.tiles):
            for ref, parts in ((stress, (0, 3, 4)), (velocity, (0, 1, 2))):
                for part in parts:
                    for row in (0, 1, self.rows + 2, self.rows + 3):
                        ref[part, tile, row, pl.ds(ROWS, depth), :] = zero

    def clear_x(self, side):
        ref = self.below_x if side == 0 else self.above_x
        zero = jnp.zeros((self.depth, LANES), jnp.float32)

        def body(turn, carry):
            for slot in range(3):
                for tile in range(self.tiles):
                    for row in range(2):
                        ref[turn, slot, tile, row] = zero
            return carry

        lax.fori_loop(0, 2 * STEPS, body, 0)

    def clear_z(self, side):
        zero = jnp.zeros((ROWS, LANES), jnp.float32)

        def body(row):
            for turn in range(2 * STEPS):
                for slot in range(3):
                    for tile in range(self.tiles):
                        self.around_z[turn, slot, tile, row, pl.ds(2 * ROWS * side, ROWS), :] = zero

        self.each_row(body)

    def fill_props(self, columns):
        tables = step_tables(columns, self.spacing) + strain_tables(columns)

        def body(row):
            for tile in range(self.tiles):
                zone = self.zone[tile, row]
                for index, table in enumerate(tables):
                    self.props[index, tile, row] = lookup(table, zone)

        self.each_row(body)

    def velocity_inner(self, row):
        stress, velocity = self.stress, self.velocity
        across = [
            self.along_y(stress, 3, row, BACKWARD),
            self.along_y(stress, 1, row, FORWARD),
            self.along_y(stress, 5, row, BACKWARD),
        ]
        for part in range(3):
            for tile in range(self.tiles):
                (field_x, kind_x), (field_z, kind_z) = STRESS_X[part], STRESS_Z[part]
                accel = total(
                    self.along_x(stress, field_x, tile, row, kind_x),
                    across[part][tile],
                    self.along_z(stress, field_z, tile, row, kind_z),
                )
                old = self.cells(velocity, part, tile, row)
                buoyancy = self.props[BUOYANCY, tile, row]
                velocity[part, tile, row + 2, pl.ds(ROWS, self.depth), :] = old + buoyancy * accel

    def outer_rows(self, turn, slot, tile, kind):
        below, above = self.below_x.at[turn, slot, tile], self.above_x.at[turn, slot, tile]
        last = self.rows - 1
        if kind == FORWARD:
            return [
                (0, FAR * below[1]),
                (last, above[0] - FAR * above[1]),
                (last - 1, -FAR * above[0]),
            ]
        return [
            (0, FAR * below[0] - below[1]),
            (1, FAR * below[1]),
            (last, -FAR * above[0]),
        ]

    def outer_layers(self, turn, slot, tile, row, kind):
        at = self.around_z.at[turn, slot, tile, row]

        def lower(distance):
            return at[pl.ds(ROWS - distance, ROWS), :]

        def upper(distance):
            return at[pl.ds(ROWS + distance, ROWS), :]

        if kind == FORWARD:
            return FAR * lower(1), upper(1) - FAR * upper(2)
        return FAR * lower(2) - lower(1), -FAR * upper(1)

    def ends(self):
        return (0, self.depth - ROWS)

    def velocity_outer_x(self, turn):
        velocity, depth = self.velocity, self.depth
        for part in range(3):
            for tile in range(self.tiles):
                for row, term in self.outer_rows(turn, part, tile, STRESS_X[part][1]):
                    place = velocity.at[part, tile, row + 2, pl.ds(ROWS, depth), :]
                    place[...] = place[...] + self.props[BUOYANCY, tile, row] * term

    def velocity_outer_z(self, turn):
        velocity = self.velocity

        def body(row):
            for part in range(3):
                for tile in range(self.tiles):
                    terms = self.outer_layers(turn, part, tile, row, STRESS_Z[part][1])
                    for begin, term in zip(self.ends(), terms):
                        place = velocity.at[part, tile, row + 2, pl.ds(ROWS + begin, ROWS), :]
                        buoyancy = self.props[BUOYANCY, tile, row, pl.ds(begin, ROWS), :]
                        place[...] = place[...] + buoyancy * term

        self.each_row(body)

    def stress_inner(self, row):
        velocity, stress, memory = self.velocity, self.stress, self.memory
        across_y = self.along_y(velocity, 1, row, BACKWARD)
        across_x = self.along_y(velocity, 0, row, FORWARD)
        across_z = self.along_y(velocity, 2, row, FORWARD)
        for tile in range(self.tiles):
            lame, shear, decay, damping = (
                self.props[index, tile, row] for index in (LAME, SHEAR, DECAY, DAMPING)
            )
            normal_x = total(self.along_x(velocity, 0, tile, row, BACKWARD))
            normal_y = total(across_y[tile])
            normal_z = total(self.along_z(velocity, 2, tile, row, BACKWARD))
            shear_xy = total(across_x[tile], self.along_x(velocity, 1, tile, row, FORWARD))
            shear_xz = total(
                self.along_z(velocity, 0, tile, row, FORWARD),
                self.along_x(velocity, 2, tile, row, FORWARD),
            )
            shear_yz = total(across_z[tile], self.along_z(velocity, 1, tile, row, FORWARD))
            volume = lame * (normal_x + normal_y + normal_z)
            half = 0.5 * shear
            rates = [
                volume + shear * normal_x,
                volume + shear * normal_y,
                volume + shear * normal_z,
                half * shear_xy,
                half * shear_xz,
                half * shear_yz,
            ]
            kept = 0.5 * TIME_STEP * (1.0 + decay)
            gained = TIME_STEP - 0.5 * TIME_STEP * damping
            for part, rate in enumerate(rates):
                past = memory[part, tile, row]
                memory[part, tile, row] = decay * past - damping * rate
                old = self.cells(stress, part, tile, row)
                stress[part, tile, row + 2, pl.ds(ROWS, self.depth), :] = (
                    old + kept * past + gained * rate
                )

    def add_rates(self, rates, tile, row, begin, count):
        damping = self.props[DAMPING, tile, row, pl.ds(begin, count), :]
        gained = TIME_STEP - 0.5 * TIME_STEP * damping
        for part, rate in rates:
            place = self.memory.at[part, tile, row, pl.ds(begin, count), :]
            place[...] = place[...] - damping * rate
            place = self.stress.at[part, tile, row + 2, pl.ds(ROWS + begin, count), :]
            place[...] = place[...] + gained * rate

    def normal_rates(self, term, along, tile, row, begin, count):
        lame = self.props[LAME, tile, row, pl.ds(begin, count), :]
        shear = self.props[SHEAR, tile, row, pl.ds(begin, count), :]
        volume = lame * term
        return [(part, volume + shear * term if part == along else volume) for part in range(3)]

    def shear_rates(self, term, part, tile, row, begin, count):
        shear = self.props[SHEAR, tile, row, pl.ds(begin, count), :]
        return [(part, (0.5 * shear) * term)]

    def stress_outer_x(self, turn):
        depth = self.depth
        for tile in range(self.tiles):
            for row, term in self.outer_rows(turn, 0, tile, BACKWARD):
                rates = self.normal_rates(term, 0, tile, row, 0, depth)
                self.add_rates(rates, tile, row, 0, depth)
            for slot, part in ((1, 3), (2, 4)):
                for row, term in self.outer_rows(turn, slot, tile, FORWARD):
                    rates = self.shear_rates(term, part, tile, row, 0, depth)
                    self.add_rates(rates, tile, row, 0, depth)

    def stress_outer_z(self, turn):
        def body(row):
            for tile in range(self.tiles):
                normal = self.outer_layers(turn, 2, tile, row, BACKWARD)
                shear_xz = self.outer_layers(turn, 0, tile, row, FORWARD)
                shear_yz = self.outer_layers(turn, 1, tile, row, FORWARD)
                for end, begin in enumerate(self.ends()):
                    rates = (
                        self.normal_rates(normal[end], 2, tile, row, begin, ROWS)
                        + self.shear_rates(shear_xz[end], 4, tile, row, begin, ROWS)
                        + self.shear_rates(shear_yz[end], 5, tile, row, begin, ROWS)
                    )
                    self.add_rates(rates, tile, row, begin, ROWS)

        self.each_row(body)

    def raise_peak(self, row):
        for tile in range(self.tiles):
            strain = principal(
                [self.cells(self.stress, part, tile, row) for part in range(6)],
                self.props[VOLUMETRIC, tile, row],
                self.props[SCALE, tile, row],
            )
            self.peak[tile, row] = jnp.maximum(self.peak[tile, row], strain)


def spread_matrix(interp_ref, coarse_cells, fine_cells):
    coarse = lax.broadcasted_iota(jnp.int32, (coarse_cells, fine_cells), 0)
    fine = lax.broadcasted_iota(jnp.int32, (coarse_cells, fine_cells), 1)
    matrix = jnp.zeros((coarse_cells, fine_cells), jnp.float32)
    for phase in range(3):
        share = interp_ref[1, phase].astype(jnp.float32) / 8.0
        matrix = jnp.where(fine == 3 * coarse + phase, share, matrix)
        matrix = jnp.where(fine == 3 * coarse - 3 + phase, 1.0 - share, matrix)
    return matrix


def gather_matrix(restrict_ref, coarse_cells, fine_cells):
    fine = lax.broadcasted_iota(jnp.int32, (fine_cells, coarse_cells), 0)
    coarse = lax.broadcasted_iota(jnp.int32, (fine_cells, coarse_cells), 1)
    matrix = jnp.zeros((fine_cells, coarse_cells), jnp.float32)
    for phase in range(3):
        weight = restrict_ref[1, phase].astype(jnp.float32)
        matrix = jnp.where(fine == 3 * coarse + phase, weight, matrix)
    return matrix


def lift_matrix(interp_ref, fine_rows, rows):
    target = lax.broadcasted_iota(jnp.int32, (2 * fine_rows, 2 * rows), 0)
    source = lax.broadcasted_iota(jnp.int32, (2 * fine_rows, 2 * rows), 1)
    matrix = jnp.zeros((2 * fine_rows, 2 * rows), jnp.float32)
    for phase in range(3):
        share = interp_ref[0, phase].astype(jnp.float32) / 8.0
        for ghost in range(2):
            for layer in range(2):
                blend = (2.0 if ghost == layer else 1.0) / 3.0
                for ahead in range(2):
                    weight = (share if ahead == 0 else 1.0 - share) * blend
                    base = 6 * (source - layer * rows - ahead) + 2 * phase + ghost
                    inside = (source >= layer * rows + ahead) & (source < (layer + 1) * rows)
                    matrix = jnp.where((target == base) & inside, weight, matrix)
    return matrix


class Coupling:
    def __init__(self, fine, coarse, interp_ref, restrict_ref, refs):
        self.fine, self.coarse = fine, coarse
        self.interp_ref, self.restrict_ref = interp_ref, restrict_ref
        self.heads, self.lifted, self.layers, self.spread, self.gather = refs
        self.block = self.heads.shape[2] // 2

    def clear(self):
        coarse_cells, fine_cells = self.spread.shape
        self.spread[...] = spread_matrix(self.interp_ref, coarse_cells, fine_cells)
        self.gather[...] = gather_matrix(self.restrict_ref, coarse_cells, fine_cells)

    def restrict(self, turn, ref, along_z):
        fine, coarse = self.fine, self.coarse
        weight = [self.restrict_ref[0, phase].astype(jnp.float32) for phase in range(3)]
        weight_y = [self.restrict_ref[1, phase].astype(jnp.float32) for phase in range(3)]
        mass = 3.0 * (weight[0] + weight[1] + weight[2]) * (weight_y[0] + weight_y[1] + weight_y[2])
        for slot, (part, _) in enumerate(along_z):
            for row in range(coarse.rows):
                begin = (slot * coarse.rows + row) * ROWS
                for tile in range(fine.tiles):
                    block = sum(
                        weight[phase]
                        * ref[part, tile, 2 + 3 * row + phase, pl.ds(fine.depth, ROWS), :]
                        for phase in range(3)
                    )
                    self.layers[begin : begin + ROWS, tile * LANES : (tile + 1) * LANES] = block
        gathered = jnp.dot(
            self.layers[...], self.gather[...], precision=EXACT, preferred_element_type=jnp.float32
        )
        gathered = gathered / jnp.full(gathered.shape, mass, jnp.float32)
        for slot in range(3):
            for row in range(coarse.rows):
                begin = (slot * coarse.rows + row) * ROWS
                for tile in range(coarse.tiles):
                    block = gathered[begin : begin + ROWS, tile * LANES : (tile + 1) * LANES]
                    block = block + pltpu.roll(block, 1, 0) + pltpu.roll(block, 2, 0)
                    self.lifted[turn, slot, tile, row, 6:7, :] = block[4:5]
                    self.lifted[turn, slot, tile, row, 7:8, :] = block[7:8]

    def interpolate(self, turn):
        fine = self.fine
        lift = lift_matrix(self.interp_ref, fine.rows, self.block)
        lifted = [
            jnp.dot(lift, self.heads[turn, slot], precision=EXACT, preferred_element_type=jnp.float32)
            for slot in range(3)
        ]
        ghosts = jnp.dot(
            jnp.concatenate(lifted, axis=0),
            self.spread[...],
            precision=EXACT,
            preferred_element_type=jnp.float32,
        )
        for slot in range(3):
            for row in range(fine.rows):
                begin = 2 * (slot * fine.rows + row)
                for tile in range(fine.tiles):
                    fine.around_z[turn, slot, tile, row, 2 * ROWS : 2 * ROWS + 2, :] = ghosts[
                        begin : begin + 2, tile * LANES : (tile + 1) * LANES
                    ]


class Place:
    def __init__(self):
        self.lat, self.depth = lax.axis_index("lat"), lax.axis_index("depth")
        self.lats, self.depths = lax.axis_size("lat"), lax.axis_size("depth")
        lat, depth = self.lat, self.depth
        has_next, has_previous = lat < self.lats - 1, lat > 0
        has_lower, has_upper = depth < self.depths - 1, depth > 0
        top, bottom = depth == 0, depth == self.depths - 1
        self.routes = {
            "head": (lat, self.depths - 1, top, bottom),
            "corner": (lat - 1, self.depths - 1, top & has_previous, bottom & has_next),
            "lift": (lat, 0, bottom, top),
            "next": (lat + 1, depth, has_next, has_previous),
            "previous": (lat - 1, depth, has_previous, has_next),
            "down": (lat, depth + 1, has_lower, has_upper),
            "up": (lat, depth - 1, has_upper, has_lower),
        }
        self.top, self.bottom = top, bottom

    def target(self, route):
        lat, depth = self.routes[route][:2]
        return {"lat": lat, "depth": depth}

    def greet(self):
        barrier = pltpu.get_barrier_semaphore()
        lat, depth = self.lat, self.depth
        peers = [
            (lat + 1, depth, lat < self.lats - 1),
            (lat - 1, depth, lat > 0),
            (lat, depth + 1, depth < self.depths - 1),
            (lat, depth - 1, depth > 0),
            (lat, self.depths - 1, self.top),
            (lat, 0, self.bottom),
            (lat - 1, self.depths - 1, self.top & (lat > 0)),
            (lat + 1, 0, self.bottom & (lat < self.lats - 1)),
        ]
        for peer_lat, peer_depth, present in peers:

            @pl.when(present)
            def _():
                pl.semaphore_signal(
                    barrier,
                    inc=1,
                    device_id={"lat": peer_lat, "depth": peer_depth},
                    device_id_type=MESH,
                )

        return barrier, sum(present.astype(jnp.int32) for _, _, present in peers)


class Exchange:
    def __init__(self, turn, place, fine, coarse, coupling, velocity, sems):
        self.place = place
        along_x = VELOCITY_X if velocity else STRESS_X
        along_z = VELOCITY_Z if velocity else STRESS_Z
        self.messages = {route: [] for route in place.routes}
        self.send_sems, self.recv_sems, self.count, self.turn = sems[0], sems[1], 0, turn
        ref = coarse.velocity if velocity else coarse.stress
        block = coupling.block
        for slot, (part, (low, _)) in enumerate(along_z):
            for layer in range(2):
                for tile in range(coarse.tiles):
                    source = ref.at[part, tile, :, ROWS + layer, :]
                    lanes = pl.ds(tile * LANES, LANES)
                    begin = layer * block
                    self.add(
                        "head",
                        source.at[pl.ds(2, coarse.rows), :],
                        coupling.heads.at[turn, slot, pl.ds(begin, coarse.rows), lanes],
                    )
                    self.add(
                        "corner",
                        source.at[pl.ds(2, 1), :],
                        coupling.heads.at[turn, slot, pl.ds(begin + coarse.rows, 1), lanes],
                    )
            self.add(
                "lift",
                coupling.lifted.at[turn, slot, :, :, pl.ds(ROWS - low, low), :],
                coarse.around_z.at[turn, slot, :, :, pl.ds(ROWS - low, low), :],
            )
        for grid in (fine, coarse):
            ref = grid.velocity if velocity else grid.stress
            inner = pl.ds(ROWS, grid.depth)
            for slot, (part, (low, high)) in enumerate(along_x):
                self.add(
                    "next",
                    ref.at[part, :, pl.ds(2 + grid.rows - low, low), inner, :],
                    grid.below_x.at[turn, slot, :, pl.ds(2 - low, low), :, :],
                )
                self.add(
                    "previous",
                    ref.at[part, :, pl.ds(2, high), inner, :],
                    grid.above_x.at[turn, slot, :, pl.ds(0, high), :, :],
                )
            for slot, (part, (low, high)) in enumerate(along_z):
                rows = pl.ds(2, grid.rows)
                self.add(
                    "down",
                    ref.at[part, :, rows, pl.ds(ROWS + grid.depth - low, low), :],
                    grid.around_z.at[turn, slot, :, :, pl.ds(ROWS - low, low), :],
                )
                self.add(
                    "up",
                    ref.at[part, :, rows, pl.ds(ROWS, high), :],
                    grid.around_z.at[turn, slot, :, :, pl.ds(2 * ROWS, high), :],
                )

    def add(self, route, source, target):
        copy = pltpu.make_async_remote_copy(
            src_ref=source,
            dst_ref=target,
            send_sem=self.send_sems.at[self.turn, self.count],
            recv_sem=self.recv_sems.at[self.turn, self.count],
            device_id=self.place.target(route),
            device_id_type=MESH,
        )
        self.messages[route].append(copy)
        self.count += 1

    def send(self, *routes):
        for route in routes or self.messages:

            @pl.when(self.place.routes[route][2])
            def _():
                for copy in self.messages[route]:
                    copy.start()

    def receive(self, *routes):
        for route in routes or self.messages:

            @pl.when(self.place.routes[route][3])
            def _():
                for copy in self.messages[route]:
                    copy.wait_recv()

    def sent(self):
        for route in self.messages:

            @pl.when(self.place.routes[route][2])
            def _():
                for copy in self.messages[route]:
                    copy.wait_send()


MESSAGES = 64
KERNEL_BYTES = 32 * 1024 * 1024


def waves_kernel(*refs):
    refs = list(refs)

    def take(count):
        taken = refs[:count]
        del refs[:count]
        return taken

    table_ref, interp_ref, restrict_ref = take(3)
    inputs = [take(5), take(5)]
    states = [take(5), take(5)]
    fine = Field(1.0, states[0] + take(4))
    coarse = Field(3.0, states[1] + take(4))
    coupling = Coupling(fine, coarse, interp_ref, restrict_ref, take(5))
    load_sems, send_sems, recv_sems = take(3)
    place = Place()
    grids = (fine, coarse)

    loads, count = {}, 0
    for grid, (velocity, stress, memory, peak, zone) in zip(grids, inputs):
        rows, inner = pl.ds(2, grid.rows), pl.ds(ROWS, grid.depth)
        for tile in range(grid.tiles):
            lanes = pl.ds(tile * LANES, LANES)
            for name, source, target in (
                ("zone", zone.at[:, :, lanes], grid.zone.at[tile]),
                ("stress", stress.at[:, :, :, lanes], grid.stress.at[:, tile, rows, inner, :]),
                ("velocity", velocity.at[:, :, :, lanes], grid.velocity.at[:, tile, rows, inner, :]),
                ("memory", memory.at[:, :, :, lanes], grid.memory.at[:, tile]),
                ("peak", peak.at[:, :, lanes], grid.peak.at[tile]),
            ):
                copy = pltpu.make_async_copy(source, target, load_sems.at[count])
                loads.setdefault(name, []).append(copy)
                count += 1

    def start(name):
        for copy in loads[name]:
            copy.start()

    def finish(name):
        for copy in loads[name]:
            copy.wait()

    start("stress")
    coupling.heads[...] = jnp.zeros(coupling.heads.shape, jnp.float32)
    barrier, peers = place.greet()
    for name in ("zone", "velocity", "memory", "peak"):
        start(name)

    turns = [
        Exchange(turn, place, fine, coarse, coupling, turn % 2 == 1, (send_sems, recv_sems))
        for turn in range(2 * STEPS)
    ]

    def restrict(turn):
        velocity = turn % 2 == 1

        @pl.when(place.bottom)
        def _():
            coupling.restrict(
                turn,
                fine.velocity if velocity else fine.stress,
                VELOCITY_Z if velocity else STRESS_Z,
            )

        turns[turn].send("lift")

    def open_turn(turn):
        turns[turn].send("head", "corner", "next", "previous", "down", "up")

    def close_turn(turn):
        turns[turn].receive("head", "corner")

        @pl.when(place.bottom)
        def _():
            coupling.interpolate(turn)

        turns[turn].receive("down", "up", "lift")
        for grid in grids:
            if turn % 2 == 1:
                grid.stress_outer_z(turn)
            else:
                grid.velocity_outer_z(turn)
        turns[turn].receive("next", "previous")
        for grid in grids:
            if turn % 2 == 1:
                grid.stress_outer_x(turn)
            else:
                grid.velocity_outer_x(turn)

    finish("stress")
    pl.semaphore_wait(barrier, peers)
    open_turn(0)
    coupling.clear()
    restrict(0)

    for grid in grids:
        grid.clear()

    @pl.when(place.top)
    def _():
        fine.clear_z(0)

    @pl.when(place.bottom)
    def _():
        coarse.clear_z(1)

    for side, outside in ((0, place.lat == 0), (1, place.lat == place.lats - 1)):

        @pl.when(outside)
        def _():
            for grid in grids:
                grid.clear_x(side)

    columns = zone_columns(table_ref)
    finish("zone")
    for grid in grids:
        grid.fill_props(columns)

    for step in range(STEPS):
        turn = 2 * step
        if step == 0:
            finish("velocity")
        else:
            turns[turn - 1].sent()
        for grid in grids:
            grid.each_row(grid.velocity_inner)
        if step > 0:
            fine.each_row(fine.raise_peak, 0, fine.rows // 2)
        close_turn(turn)
        open_turn(turn + 1)
        restrict(turn + 1)
        if step == 0:
            finish("memory")
            finish("peak")
        else:
            fine.each_row(fine.raise_peak, fine.rows // 2)
            coarse.each_row(coarse.raise_peak)
        turns[turn].sent()
        for grid in grids:
            grid.each_row(grid.stress_inner)
        close_turn(turn + 1)
        if step < STEPS - 1:
            open_turn(turn + 2)
            restrict(turn + 2)
    turns[2 * STEPS - 1].sent()


def finish_kernel(*refs):
    states, outputs = [refs[0:5], refs[5:10]], [refs[10:14], refs[14:18]]
    peaks, sems = refs[18:20], refs[20]
    copies, count = [], 0

    def move(source, target):
        nonlocal count
        copy = pltpu.make_async_copy(source, target, sems.at[count])
        copy.start()
        copies.append(copy)
        count += 1

    for (stress, velocity, memory, peak, _), (new_velocity, new_stress, new_memory, _) in zip(
        states, outputs
    ):
        tiles, rows, depth, _ = peak.shape
        inner_rows, inner = pl.ds(2, rows), pl.ds(ROWS, depth)
        for tile in range(tiles):
            lanes = pl.ds(tile * LANES, LANES)
            move(stress.at[:, tile, inner_rows, inner, :], new_stress.at[:, :, :, lanes])
            move(memory.at[:, tile], new_memory.at[:, :, :, lanes])
            move(velocity.at[:, tile, inner_rows, inner, :], new_velocity.at[:, :, :, lanes])
    for (stress, _, _, peak, props), (_, _, _, new_peak), raised in zip(states, outputs, peaks):
        tiles, rows, depth, _ = peak.shape
        half = rows // 2

        def body(row, carry):
            for tile in range(tiles):
                strain = principal(
                    [stress[part, tile, row + 2, pl.ds(ROWS, depth), :] for part in range(6)],
                    props[VOLUMETRIC, tile, row],
                    props[SCALE, tile, row],
                )
                raised[tile, row] = jnp.maximum(peak[tile, row], strain)
            return carry

        for begin, end in ((0, half), (half, rows)):
            lax.fori_loop(begin, end, body, 0)
            span = pl.ds(begin, end - begin)
            for tile in range(tiles):
                move(raised.at[tile, span], new_peak.at[span, :, pl.ds(tile * LANES, LANES)])
    for copy in copies:
        copy.wait()


def sizes_of(peak):
    rows, depth, cells = peak.shape
    tiles = cells // LANES
    return tiles, (tiles, rows + 4, depth + 2 * ROWS, LANES), (tiles, rows, depth, LANES)


def state_of(peak):
    _, full, plain = sizes_of(peak)
    shapes = [(6, *full), (3, *full), (6, *plain), plain, (7, *plain)]
    return [pltpu.VMEM(shape, jnp.float32) for shape in shapes]


def scratch_of(peak):
    tiles, _, plain = sizes_of(peak)
    _, rows, depth, _ = plain
    side = pltpu.VMEM((2 * STEPS, 3, tiles, 2, depth, LANES), jnp.float32)
    around = pltpu.VMEM((2 * STEPS, 3, tiles, rows, 3 * ROWS, LANES), jnp.float32)
    return [pltpu.VMEM(plain, jnp.int32), side, side, around]


def on_device(
    velocity_fine,
    stress_fine,
    memory_fine,
    peak_fine,
    zone_fine,
    velocity_coarse,
    stress_coarse,
    memory_coarse,
    peak_coarse,
    zone_coarse,
    zone_table,
    interp_weight,
    restrict_weight,
):
    fine = (velocity_fine, stress_fine, memory_fine, peak_fine)
    coarse = (velocity_coarse, stress_coarse, memory_coarse, peak_coarse)
    fine_rows, _, fine_cells = peak_fine.shape
    coarse_rows, _, coarse_cells = peak_coarse.shape
    block = ROWS * ((coarse_rows + ROWS) // ROWS)
    turns = 2 * STEPS
    hbm = pl.BlockSpec(memory_space=pl.ANY)
    smem = pl.BlockSpec(memory_space=pltpu.SMEM)
    vmem = pl.BlockSpec(memory_space=pltpu.VMEM)
    tiles = fine_cells // LANES + coarse_cells // LANES
    state = pl.pallas_call(
        waves_kernel,
        out_shape=state_of(peak_fine) + state_of(peak_coarse),
        in_specs=[smem] * 3 + [hbm] * 10,
        out_specs=[vmem] * 10,
        scratch_shapes=[
            *scratch_of(peak_fine),
            *scratch_of(peak_coarse),
            pltpu.VMEM((turns, 3, 2 * block, coarse_cells), jnp.float32),
            pltpu.VMEM((turns, 3, coarse_cells // LANES, coarse_rows, ROWS, LANES), jnp.float32),
            pltpu.VMEM((3 * coarse_rows * ROWS, fine_cells), jnp.float32),
            pltpu.VMEM((coarse_cells, fine_cells), jnp.float32),
            pltpu.VMEM((fine_cells, coarse_cells), jnp.float32),
            pltpu.SemaphoreType.DMA((5 * tiles,)),
            pltpu.SemaphoreType.DMA((turns, MESSAGES)),
            pltpu.SemaphoreType.DMA((turns, MESSAGES)),
        ],
        compiler_params=pltpu.CompilerParams(
            collective_id=0, has_side_effects=True, vmem_limit_bytes=KERNEL_BYTES
        ),
        name="waves",
    )(
        *(
            pltpu.with_memory_space_constraint(array, pltpu.HBM)
            for array in (
                zone_table,
                interp_weight,
                restrict_weight,
                *fine,
                zone_fine,
                *coarse,
                zone_coarse,
            )
        )
    )
    outputs = (*fine, *coarse)
    return tuple(
        pl.pallas_call(
            finish_kernel,
            out_shape=[jax.ShapeDtypeStruct(array.shape, array.dtype) for array in outputs],
            in_specs=[vmem] * 10,
            out_specs=[hbm] * 8,
            scratch_shapes=[
                pltpu.VMEM(sizes_of(peak_fine)[2], jnp.float32),
                pltpu.VMEM(sizes_of(peak_coarse)[2], jnp.float32),
                pltpu.SemaphoreType.DMA((5 * tiles,)),
            ],
            compiler_params=pltpu.CompilerParams(vmem_limit_bytes=KERNEL_BYTES),
            name="finish",
        )(*state)
    )


def solution(mesh):
    field, scalar, whole = P(None, "lat", "depth", None), P("lat", "depth", None), P()
    return jax.shard_map(
        on_device,
        mesh=mesh,
        in_specs=(field, field, field, scalar, scalar) * 2 + (whole,) * 3,
        out_specs=(field, field, field, scalar) * 2,
        check_vma=False,
    )
```

```python
import math

import jax
import jax.numpy as jnp
from jax import lax
from jax.experimental import pallas as pl
from jax.experimental.pallas import tpu as pltpu
from jax.sharding import PartitionSpec as P

STEPS = 2
LANES = 128
ROWS = 8

TIME_STEP = 0.4
NEAR = 9.0 / 8.0
FAR = 1.0 / 27.0
TINY = 1e-18

FORWARD = (1, 2)
BACKWARD = (2, 1)
STRESS_X = ((0, FORWARD), (3, BACKWARD), (4, BACKWARD))
STRESS_Z = ((4, BACKWARD), (5, BACKWARD), (2, FORWARD))
VELOCITY_X = ((0, BACKWARD), (1, FORWARD), (2, FORWARD))
VELOCITY_Z = ((0, FORWARD), (1, FORWARD), (2, BACKWARD))

BUOYANCY, LAME, SHEAR, DECAY, DAMPING, VOLUMETRIC, SCALE = range(7)

MESH = pl.DeviceIdType.MESH
EXACT = lax.Precision.HIGHEST


def property_tables(table_ref, spacing):
    def fill(column, level):
        return jnp.full((ROWS, LANES), table_ref[level, column], jnp.float32)

    tables = []
    for level in range(table_ref.shape[0]):
        buoyancy, lame, shear, decay, damping = (fill(column, level) for column in range(5))
        tables.append(
            [
                buoyancy * (TIME_STEP * NEAR / spacing),
                lame * (NEAR / spacing),
                shear * (2.0 * NEAR / spacing),
                decay,
                damping * (1.0 - decay),
                lame / (3.0 * lame + 2.0 * shear),
                0.5 / shear,
            ]
        )
    return tables


def select(masks, values):
    for mask in masks:
        pairs = [values[i : i + 2] for i in range(0, len(values), 2)]
        values = [jnp.where(mask, pair[-1], pair[0]) for pair in pairs]
    return values[0]


def rotation(low, high, pivot):
    half = 0.5 * (high - low)
    size = jnp.maximum(jnp.abs(half), TINY)
    square = size * size + pivot * pivot
    radius = square * lax.rsqrt(square)
    reach = size + radius
    weight = lax.rsqrt((radius + radius) * reach)
    sign = jnp.where(half >= 0, 1.0, -1.0)
    middle = low + half
    offset = sign * radius
    return reach * weight, sign * (pivot * weight), middle - offset, middle + offset


def largest(low, high, pivot):
    half = 0.5 * (high - low)
    size = jnp.maximum(jnp.abs(half), TINY)
    square = size * size + pivot * pivot
    return low + half + square * lax.rsqrt(square)


def principal(stress, volumetric, scale):
    a00, a11, a22, a01, a02, a12 = stress
    shift = volumetric * (a00 + a11 + a22)
    cosine, sine, a00, a11 = rotation(a00, a11, a01)
    a02, a12 = cosine * a02 - sine * a12, sine * a02 + cosine * a12
    for sweep in range(3):
        if sweep > 0:
            cosine, sine, a00, a11 = rotation(a00, a11, a01)
            a02, a12 = cosine * a02, sine * a02
        cosine, sine, a00, a22 = rotation(a00, a22, a02)
        a01, a12 = -(sine * a12), cosine * a12
        if sweep < 2:
            cosine, sine, a11, a22 = rotation(a11, a22, a12)
            a01, a02 = cosine * a01, sine * a01
    return (jnp.maximum(a00, largest(a11, a22, a12)) - shift) * scale


def shifted_y(tiles, offset):
    lane = lax.broadcasted_iota(jnp.int32, tiles[0].shape, 1)
    rolled = [pltpu.roll(tile, (-offset) % LANES, 1) for tile in tiles]
    zero = jnp.zeros_like(tiles[0])
    if offset > 0:
        outside, beside = lane >= LANES - offset, rolled[1:] + [zero]
    else:
        outside, beside = lane < -offset, [zero] + rolled[:-1]
    return [jnp.where(outside, other, own) for other, own in zip(beside, rolled)]


def difference_y(tiles, kind):
    if kind == FORWARD:
        near = [a - b for a, b in zip(shifted_y(tiles, 1), tiles)]
        far = [a - b for a, b in zip(shifted_y(tiles, 2), shifted_y(tiles, -1))]
    else:
        near = [a - b for a, b in zip(tiles, shifted_y(tiles, -1))]
        far = [a - b for a, b in zip(shifted_y(tiles, 1), shifted_y(tiles, -2))]
    return list(zip(near, far))


def difference(at, kind):
    if kind == FORWARD:
        return at(1) - at(0), at(2) - at(-1)
    return at(0) - at(-1), at(1) - at(-2)


def total(*pairs):
    near = sum(pair[0] for pair in pairs[1:]) + pairs[0][0]
    far = sum(pair[1] for pair in pairs[1:]) + pairs[0][1]
    return near - FAR * far


class Field:
    def __init__(self, spacing, refs):
        self.spacing = spacing
        (
            self.stress,
            self.velocity,
            self.memory,
            self.peak,
            self.props,
            self.zone,
            self.below_x,
            self.above_x,
            self.around_z,
        ) = refs
        self.tiles, self.rows, self.depth, _ = self.peak.shape

    def cells(self, ref, part, tile, row, dx=0, dz=0):
        return ref[part, tile, row + (2 + dx), pl.ds(ROWS + dz, self.depth), :]

    def along_x(self, ref, part, tile, row, kind):
        return difference(lambda d: self.cells(ref, part, tile, row, dx=d), kind)

    def along_z(self, ref, part, tile, row, kind):
        return difference(lambda d: self.cells(ref, part, tile, row, dz=d), kind)

    def along_y(self, ref, part, row, kind):
        tiles = [self.cells(ref, part, tile, row) for tile in range(self.tiles)]
        return difference_y(tiles, kind)

    def each_row(self, body, begin=0, end=None):
        def step(row, carry):
            body(row)
            return carry

        lax.fori_loop(begin, self.rows if end is None else end, step, 0)

    def clear(self):
        stress, velocity, depth = self.stress, self.velocity, self.depth
        tile_zero = jnp.zeros((ROWS, LANES), jnp.float32)
        zero = jnp.zeros((depth, LANES), jnp.float32)

        def body(row):
            for tile in range(self.tiles):
                for ref, parts in ((stress, (2, 4, 5)), (velocity, (0, 1, 2))):
                    for part in parts:
                        ref[part, tile, row + 2, 0:ROWS, :] = tile_zero
                        ref[part, tile, row + 2, pl.ds(ROWS + depth, ROWS), :] = tile_zero
                for turn in range(2 * STEPS):
                    for slot in range(3):
                        self.around_z[turn, slot, tile, row, pl.ds(ROWS, ROWS), :] = tile_zero

        self.each_row(body)
        for tile in range(self.tiles):
            for ref, parts in ((stress, (0, 3, 4)), (velocity, (0, 1, 2))):
                for part in parts:
                    for row in (0, 1, self.rows + 2, self.rows + 3):
                        ref[part, tile, row, pl.ds(ROWS, depth), :] = zero

    def clear_x(self, side):
        ref = self.below_x if side == 0 else self.above_x
        zero = jnp.zeros((self.depth, LANES), jnp.float32)

        def body(turn, carry):
            for slot in range(3):
                for tile in range(self.tiles):
                    for row in range(2):
                        ref[turn, slot, tile, row] = zero
            return carry

        lax.fori_loop(0, 2 * STEPS, body, 0)

    def clear_z(self, side):
        zero = jnp.zeros((ROWS, LANES), jnp.float32)

        def body(row):
            for turn in range(2 * STEPS):
                for slot in range(3):
                    for tile in range(self.tiles):
                        self.around_z[turn, slot, tile, row, pl.ds(2 * ROWS * side, ROWS), :] = zero

        self.each_row(body)

    def fill_props(self, table_ref, filled):
        zones = table_ref.shape[0]
        for level, values in enumerate(property_tables(table_ref, self.spacing)):
            for index, value in enumerate(values):
                filled[index, level] = value

        def body(row):
            for tile in range(self.tiles):
                for begin in range(0, self.depth, ROWS):
                    zone = self.zone[tile, row, begin : begin + ROWS, :]
                    masks = [
                        jnp.bitwise_and(zone, 1 << bit) != 0 for bit in range((zones - 1).bit_length())
                    ]
                    for index in range(filled.shape[0]):
                        values = [filled[index, level] for level in range(zones)]
                        self.props[index, tile, row, begin : begin + ROWS, :] = select(masks, values)

        self.each_row(body)

    def velocity_inner(self, row):
        stress, velocity = self.stress, self.velocity
        across = [
            self.along_y(stress, 3, row, BACKWARD),
            self.along_y(stress, 1, row, FORWARD),
            self.along_y(stress, 5, row, BACKWARD),
        ]
        for part in range(3):
            for tile in range(self.tiles):
                (field_x, kind_x), (field_z, kind_z) = STRESS_X[part], STRESS_Z[part]
                accel = total(
                    self.along_x(stress, field_x, tile, row, kind_x),
                    across[part][tile],
                    self.along_z(stress, field_z, tile, row, kind_z),
                )
                old = self.cells(velocity, part, tile, row)
                buoyancy = self.props[BUOYANCY, tile, row]
                velocity[part, tile, row + 2, pl.ds(ROWS, self.depth), :] = old + buoyancy * accel

    def outer_rows(self, turn, slot, tile, kind):
        below, above = self.below_x.at[turn, slot, tile], self.above_x.at[turn, slot, tile]
        last = self.rows - 1
        if kind == FORWARD:
            return [
                (0, FAR * below[1]),
                (last, above[0] - FAR * above[1]),
                (last - 1, -FAR * above[0]),
            ]
        return [
            (0, FAR * below[0] - below[1]),
            (1, FAR * below[1]),
            (last, -FAR * above[0]),
        ]

    def outer_layers(self, turn, slot, tile, row, kind):
        at = self.around_z.at[turn, slot, tile, row]

        def lower(distance):
            return at[pl.ds(ROWS - distance, ROWS), :]

        def upper(distance):
            return at[pl.ds(ROWS + distance, ROWS), :]

        if kind == FORWARD:
            return FAR * lower(1), upper(1) - FAR * upper(2)
        return FAR * lower(2) - lower(1), -FAR * upper(1)

    def ends(self):
        return (0, self.depth - ROWS)

    def velocity_outer_x(self, turn):
        velocity, depth = self.velocity, self.depth
        for part in range(3):
            for tile in range(self.tiles):
                for row, term in self.outer_rows(turn, part, tile, STRESS_X[part][1]):
                    place = velocity.at[part, tile, row + 2, pl.ds(ROWS, depth), :]
                    place[...] = place[...] + self.props[BUOYANCY, tile, row] * term

    def velocity_outer_z(self, turn):
        velocity = self.velocity

        def body(row):
            for part in range(3):
                for tile in range(self.tiles):
                    terms = self.outer_layers(turn, part, tile, row, STRESS_Z[part][1])
                    for begin, term in zip(self.ends(), terms):
                        place = velocity.at[part, tile, row + 2, pl.ds(ROWS + begin, ROWS), :]
                        buoyancy = self.props[BUOYANCY, tile, row, pl.ds(begin, ROWS), :]
                        place[...] = place[...] + buoyancy * term

        self.each_row(body)

    def stress_inner(self, row):
        velocity, stress, memory = self.velocity, self.stress, self.memory
        across_y = self.along_y(velocity, 1, row, BACKWARD)
        across_x = self.along_y(velocity, 0, row, FORWARD)
        across_z = self.along_y(velocity, 2, row, FORWARD)
        for tile in range(self.tiles):
            lame, shear, decay, damping = (
                self.props[index, tile, row] for index in (LAME, SHEAR, DECAY, DAMPING)
            )
            normal_x = total(self.along_x(velocity, 0, tile, row, BACKWARD))
            normal_y = total(across_y[tile])
            normal_z = total(self.along_z(velocity, 2, tile, row, BACKWARD))
            shear_xy = total(across_x[tile], self.along_x(velocity, 1, tile, row, FORWARD))
            shear_xz = total(
                self.along_z(velocity, 0, tile, row, FORWARD),
                self.along_x(velocity, 2, tile, row, FORWARD),
            )
            shear_yz = total(across_z[tile], self.along_z(velocity, 1, tile, row, FORWARD))
            volume = lame * (normal_x + normal_y + normal_z)
            half = 0.5 * shear
            rates = [
                volume + shear * normal_x,
                volume + shear * normal_y,
                volume + shear * normal_z,
                half * shear_xy,
                half * shear_xz,
                half * shear_yz,
            ]
            kept = 0.5 * TIME_STEP * (1.0 + decay)
            gained = TIME_STEP - 0.5 * TIME_STEP * damping
            for part, rate in enumerate(rates):
                past = memory[part, tile, row]
                memory[part, tile, row] = decay * past - damping * rate
                old = self.cells(stress, part, tile, row)
                stress[part, tile, row + 2, pl.ds(ROWS, self.depth), :] = (
                    old + kept * past + gained * rate
                )

    def add_rates(self, rates, tile, row, begin, count):
        damping = self.props[DAMPING, tile, row, pl.ds(begin, count), :]
        gained = TIME_STEP - 0.5 * TIME_STEP * damping
        for part, rate in rates:
            place = self.memory.at[part, tile, row, pl.ds(begin, count), :]
            place[...] = place[...] - damping * rate
            place = self.stress.at[part, tile, row + 2, pl.ds(ROWS + begin, count), :]
            place[...] = place[...] + gained * rate

    def normal_rates(self, term, along, tile, row, begin, count):
        lame = self.props[LAME, tile, row, pl.ds(begin, count), :]
        shear = self.props[SHEAR, tile, row, pl.ds(begin, count), :]
        volume = lame * term
        return [(part, volume + shear * term if part == along else volume) for part in range(3)]

    def shear_rates(self, term, part, tile, row, begin, count):
        shear = self.props[SHEAR, tile, row, pl.ds(begin, count), :]
        return [(part, (0.5 * shear) * term)]

    def stress_outer_x(self, turn):
        depth = self.depth
        for tile in range(self.tiles):
            for row, term in self.outer_rows(turn, 0, tile, BACKWARD):
                rates = self.normal_rates(term, 0, tile, row, 0, depth)
                self.add_rates(rates, tile, row, 0, depth)
            for slot, part in ((1, 3), (2, 4)):
                for row, term in self.outer_rows(turn, slot, tile, FORWARD):
                    rates = self.shear_rates(term, part, tile, row, 0, depth)
                    self.add_rates(rates, tile, row, 0, depth)

    def stress_outer_z(self, turn):
        def body(row):
            for tile in range(self.tiles):
                normal = self.outer_layers(turn, 2, tile, row, BACKWARD)
                shear_xz = self.outer_layers(turn, 0, tile, row, FORWARD)
                shear_yz = self.outer_layers(turn, 1, tile, row, FORWARD)
                for end, begin in enumerate(self.ends()):
                    rates = (
                        self.normal_rates(normal[end], 2, tile, row, begin, ROWS)
                        + self.shear_rates(shear_xz[end], 4, tile, row, begin, ROWS)
                        + self.shear_rates(shear_yz[end], 5, tile, row, begin, ROWS)
                    )
                    self.add_rates(rates, tile, row, begin, ROWS)

        self.each_row(body)

    def raise_peak(self, row):
        for tile in range(self.tiles):
            strain = principal(
                [self.cells(self.stress, part, tile, row) for part in range(6)],
                self.props[VOLUMETRIC, tile, row],
                self.props[SCALE, tile, row],
            )
            self.peak[tile, row] = jnp.maximum(self.peak[tile, row], strain)


def spread_matrix(interp_ref, coarse_cells, fine_cells):
    coarse = lax.broadcasted_iota(jnp.int32, (coarse_cells, fine_cells), 0)
    fine = lax.broadcasted_iota(jnp.int32, (coarse_cells, fine_cells), 1)
    matrix = jnp.zeros((coarse_cells, fine_cells), jnp.float32)
    for phase in range(3):
        share = interp_ref[1, phase].astype(jnp.float32) / 8.0
        matrix = jnp.where(fine == 3 * coarse + phase, share, matrix)
        matrix = jnp.where(fine == 3 * coarse - 3 + phase, 1.0 - share, matrix)
    return matrix


def gather_matrix(restrict_ref, coarse_cells, fine_cells):
    fine = lax.broadcasted_iota(jnp.int32, (fine_cells, coarse_cells), 0)
    coarse = lax.broadcasted_iota(jnp.int32, (fine_cells, coarse_cells), 1)
    matrix = jnp.zeros((fine_cells, coarse_cells), jnp.float32)
    for phase in range(3):
        weight = restrict_ref[1, phase].astype(jnp.float32)
        matrix = jnp.where(fine == 3 * coarse + phase, weight, matrix)
    return matrix


def lift_matrix(interp_ref, fine_rows, rows):
    target = lax.broadcasted_iota(jnp.int32, (2 * fine_rows, 2 * rows), 0)
    source = lax.broadcasted_iota(jnp.int32, (2 * fine_rows, 2 * rows), 1)
    matrix = jnp.zeros((2 * fine_rows, 2 * rows), jnp.float32)
    for phase in range(3):
        share = interp_ref[0, phase].astype(jnp.float32) / 8.0
        for ghost in range(2):
            for layer in range(2):
                blend = (2.0 if ghost == layer else 1.0) / 3.0
                for ahead in range(2):
                    weight = (share if ahead == 0 else 1.0 - share) * blend
                    base = 6 * (source - layer * rows - ahead) + 2 * phase + ghost
                    inside = (source >= layer * rows + ahead) & (source < (layer + 1) * rows)
                    matrix = jnp.where((target == base) & inside, weight, matrix)
    return matrix


class Coupling:
    def __init__(self, fine, coarse, interp_ref, restrict_ref, refs):
        self.fine, self.coarse = fine, coarse
        self.interp_ref, self.restrict_ref = interp_ref, restrict_ref
        self.heads, self.lifted, self.layers, self.spread, self.gather = refs
        self.block = self.heads.shape[2] // 2

    def clear(self):
        coarse_cells, fine_cells = self.spread.shape
        self.spread[...] = spread_matrix(self.interp_ref, coarse_cells, fine_cells)
        self.gather[...] = gather_matrix(self.restrict_ref, coarse_cells, fine_cells)

    def restrict(self, turn, ref, along_z):
        fine, coarse = self.fine, self.coarse
        weight = [self.restrict_ref[0, phase].astype(jnp.float32) for phase in range(3)]
        weight_y = [self.restrict_ref[1, phase].astype(jnp.float32) for phase in range(3)]
        mass = 3.0 * (weight[0] + weight[1] + weight[2]) * (weight_y[0] + weight_y[1] + weight_y[2])
        for slot, (part, _) in enumerate(along_z):
            for row in range(coarse.rows):
                begin = (slot * coarse.rows + row) * ROWS
                for tile in range(fine.tiles):
                    block = sum(
                        weight[phase]
                        * ref[part, tile, 2 + 3 * row + phase, pl.ds(fine.depth, ROWS), :]
                        for phase in range(3)
                    )
                    self.layers[begin : begin + ROWS, tile * LANES : (tile + 1) * LANES] = block
        gathered = jnp.dot(
            self.layers[...], self.gather[...], precision=EXACT, preferred_element_type=jnp.float32
        )
        gathered = gathered / jnp.full(gathered.shape, mass, jnp.float32)
        for slot in range(3):
            for row in range(coarse.rows):
                begin = (slot * coarse.rows + row) * ROWS
                for tile in range(coarse.tiles):
                    block = gathered[begin : begin + ROWS, tile * LANES : (tile + 1) * LANES]
                    block = block + pltpu.roll(block, 1, 0) + pltpu.roll(block, 2, 0)
                    self.lifted[turn, slot, tile, row, 6:7, :] = block[4:5]
                    self.lifted[turn, slot, tile, row, 7:8, :] = block[7:8]

    def interpolate(self, turn):
        fine = self.fine
        lift = lift_matrix(self.interp_ref, fine.rows, self.block)
        lifted = [
            jnp.dot(lift, self.heads[turn, slot], precision=EXACT, preferred_element_type=jnp.float32)
            for slot in range(3)
        ]
        ghosts = jnp.dot(
            jnp.concatenate(lifted, axis=0),
            self.spread[...],
            precision=EXACT,
            preferred_element_type=jnp.float32,
        )
        for slot in range(3):
            for row in range(fine.rows):
                begin = 2 * (slot * fine.rows + row)
                for tile in range(fine.tiles):
                    fine.around_z[turn, slot, tile, row, 2 * ROWS : 2 * ROWS + 2, :] = ghosts[
                        begin : begin + 2, tile * LANES : (tile + 1) * LANES
                    ]


class Place:
    def __init__(self):
        self.lat, self.depth = lax.axis_index("lat"), lax.axis_index("depth")
        self.lats, self.depths = lax.axis_size("lat"), lax.axis_size("depth")
        lat, depth = self.lat, self.depth
        has_next, has_previous = lat < self.lats - 1, lat > 0
        has_lower, has_upper = depth < self.depths - 1, depth > 0
        top, bottom = depth == 0, depth == self.depths - 1
        self.routes = {
            "head": (lat, self.depths - 1, top, bottom),
            "corner": (lat - 1, self.depths - 1, top & has_previous, bottom & has_next),
            "lift": (lat, 0, bottom, top),
            "next": (lat + 1, depth, has_next, has_previous),
            "previous": (lat - 1, depth, has_previous, has_next),
            "down": (lat, depth + 1, has_lower, has_upper),
            "up": (lat, depth - 1, has_upper, has_lower),
        }
        self.top, self.bottom = top, bottom

    def target(self, route):
        lat, depth = self.routes[route][:2]
        return {"lat": lat, "depth": depth}

    def greet(self):
        barrier = pltpu.get_barrier_semaphore()
        lat, depth = self.lat, self.depth
        peers = [
            (lat + 1, depth, lat < self.lats - 1),
            (lat - 1, depth, lat > 0),
            (lat, depth + 1, depth < self.depths - 1),
            (lat, depth - 1, depth > 0),
            (lat, self.depths - 1, self.top),
            (lat, 0, self.bottom),
            (lat - 1, self.depths - 1, self.top & (lat > 0)),
            (lat + 1, 0, self.bottom & (lat < self.lats - 1)),
        ]
        for peer_lat, peer_depth, present in peers:

            @pl.when(present)
            def _():
                pl.semaphore_signal(
                    barrier,
                    inc=1,
                    device_id={"lat": peer_lat, "depth": peer_depth},
                    device_id_type=MESH,
                )

        return barrier, sum(present.astype(jnp.int32) for _, _, present in peers)


class Exchange:
    def __init__(self, turn, place, fine, coarse, coupling, velocity, sems):
        self.place = place
        along_x = VELOCITY_X if velocity else STRESS_X
        along_z = VELOCITY_Z if velocity else STRESS_Z
        self.messages = {route: [] for route in place.routes}
        self.numbers = {route: number for number, route in enumerate(place.routes)}
        self.length = dict.fromkeys(place.routes, 0)
        self.send_sems, self.recv_sems, self.token = (sems[0].at[turn], sems[1].at[turn], sems[2])
        ref = coarse.velocity if velocity else coarse.stress
        block = coupling.block
        for slot, (part, (low, _)) in enumerate(along_z):
            for layer in range(2):
                for tile in range(coarse.tiles):
                    source = ref.at[part, tile, :, ROWS + layer, :]
                    lanes = pl.ds(tile * LANES, LANES)
                    begin = layer * block
                    self.add(
                        "head",
                        source.at[pl.ds(2, coarse.rows), :],
                        coupling.heads.at[turn, slot, pl.ds(begin, coarse.rows), lanes],
                    )
                    self.add(
                        "corner",
                        source.at[pl.ds(2, 1), :],
                        coupling.heads.at[turn, slot, pl.ds(begin + coarse.rows, 1), lanes],
                    )
            self.add(
                "lift",
                coupling.lifted.at[turn, slot, :, :, pl.ds(ROWS - low, low), :],
                coarse.around_z.at[turn, slot, :, :, pl.ds(ROWS - low, low), :],
            )
        for grid in (fine, coarse):
            ref = grid.velocity if velocity else grid.stress
            inner = pl.ds(ROWS, grid.depth)
            for slot, (part, (low, high)) in enumerate(along_x):
                self.add(
                    "next",
                    ref.at[part, :, pl.ds(2 + grid.rows - low, low), inner, :],
                    grid.below_x.at[turn, slot, :, pl.ds(2 - low, low), :, :],
                )
                self.add(
                    "previous",
                    ref.at[part, :, pl.ds(2, high), inner, :],
                    grid.above_x.at[turn, slot, :, pl.ds(0, high), :, :],
                )
            for slot, (part, (low, high)) in enumerate(along_z):
                rows = pl.ds(2, grid.rows)
                self.add(
                    "down",
                    ref.at[part, :, rows, pl.ds(ROWS + grid.depth - low, low), :],
                    grid.around_z.at[turn, slot, :, :, pl.ds(ROWS - low, low), :],
                )
                self.add(
                    "up",
                    ref.at[part, :, rows, pl.ds(ROWS, high), :],
                    grid.around_z.at[turn, slot, :, :, pl.ds(2 * ROWS, high), :],
                )

    def add(self, route, source, target):
        number = self.numbers[route]
        copy = pltpu.make_async_remote_copy(
            src_ref=source,
            dst_ref=target,
            send_sem=self.send_sems.at[number],
            recv_sem=self.recv_sems.at[number],
            device_id=self.place.target(route),
            device_id_type=MESH,
        )
        self.messages[route].append(copy)
        self.length[route] += math.prod(target.shape) // LANES

    def settle(self, route, sem):
        whole = self.token.at[pl.ds(0, self.length[route]), :]
        pltpu.make_async_copy(whole, whole, sem).wait()

    def send(self, *routes):
        for route in routes:

            @pl.when(self.place.routes[route][2])
            def _():
                for copy in self.messages[route]:
                    copy.start()

    def receive(self, *routes):
        for route in routes:

            @pl.when(self.place.routes[route][3])
            def _():
                self.settle(route, self.recv_sems.at[self.numbers[route]])

    def sent(self):
        for route in self.messages:

            @pl.when(self.place.routes[route][2])
            def _():
                self.settle(route, self.send_sems.at[self.numbers[route]])


ROUTES = 7
KERNEL_BYTES = 32 * 1024 * 1024


def waves_kernel(*refs):
    refs = list(refs)

    def take(count):
        taken = refs[:count]
        del refs[:count]
        return taken

    table_ref, interp_ref, restrict_ref = take(3)
    inputs = [take(5), take(5)]
    states = [take(5), take(5)]
    fine = Field(1.0, states[0] + take(4))
    coarse = Field(3.0, states[1] + take(4))
    coupling = Coupling(fine, coarse, interp_ref, restrict_ref, take(5))
    filled, token = take(2)
    load_sems, send_sems, recv_sems = take(3)
    place = Place()
    grids = (fine, coarse)

    loads = {}
    for grid, arrays, sems in zip(grids, inputs, (load_sems.at[0], load_sems.at[1])):
        velocity, stress, memory, peak, zone = arrays
        rows, inner = pl.ds(2, grid.rows), pl.ds(ROWS, grid.depth)
        wholes = (zone, stress, velocity, memory, peak)
        for index, name in enumerate(("zone", "stress", "velocity", "memory", "peak")):
            copies = []
            for tile in range(grid.tiles):
                lanes = pl.ds(tile * LANES, LANES)
                source, target = {
                    "zone": (zone.at[:, :, lanes], grid.zone.at[tile]),
                    "stress": (stress.at[:, :, :, lanes], grid.stress.at[:, tile, rows, inner, :]),
                    "velocity": (
                        velocity.at[:, :, :, lanes],
                        grid.velocity.at[:, tile, rows, inner, :],
                    ),
                    "memory": (memory.at[:, :, :, lanes], grid.memory.at[:, tile]),
                    "peak": (peak.at[:, :, lanes], grid.peak.at[tile]),
                }[name]
                copies.append(pltpu.make_async_copy(source, target, sems.at[index]))
            whole = pltpu.make_async_copy(wholes[index], wholes[index], sems.at[index])
            loads.setdefault(name, []).append((copies, whole))

    def start(name):
        for copies, _ in loads[name]:
            for copy in copies:
                copy.start()

    def finish(name):
        for _, whole in loads[name]:
            whole.wait()

    start("stress")
    coupling.heads[...] = jnp.zeros(coupling.heads.shape, jnp.float32)
    barrier, peers = place.greet()
    for name in ("zone", "velocity", "memory", "peak"):
        start(name)

    turns = [
        Exchange(turn, place, fine, coarse, coupling, turn % 2 == 1, (send_sems, recv_sems, token))
        for turn in range(2 * STEPS)
    ]

    def restrict(turn):
        velocity = turn % 2 == 1

        @pl.when(place.bottom)
        def _():
            coupling.restrict(
                turn,
                fine.velocity if velocity else fine.stress,
                VELOCITY_Z if velocity else STRESS_Z,
            )

        turns[turn].send("lift")

    def open_turn(turn):
        turns[turn].send("head", "corner", "next", "previous", "down", "up")

    def close_turn(turn):
        turns[turn].receive("head", "corner")

        @pl.when(place.bottom)
        def _():
            coupling.interpolate(turn)

        turns[turn].receive("down", "up", "lift")
        for grid in grids:
            if turn % 2 == 1:
                grid.stress_outer_z(turn)
            else:
                grid.velocity_outer_z(turn)
        turns[turn].receive("next", "previous")
        for grid in grids:
            if turn % 2 == 1:
                grid.stress_outer_x(turn)
            else:
                grid.velocity_outer_x(turn)

    finish("stress")
    pl.semaphore_wait(barrier, peers)
    open_turn(0)
    coupling.clear()
    restrict(0)

    for grid in grids:
        grid.clear()

    @pl.when(place.top)
    def _():
        fine.clear_z(0)

    @pl.when(place.bottom)
    def _():
        coarse.clear_z(1)

    for side, outside in ((0, place.lat == 0), (1, place.lat == place.lats - 1)):

        @pl.when(outside)
        def _():
            for grid in grids:
                grid.clear_x(side)

    finish("zone")
    for grid in grids:
        grid.fill_props(table_ref, filled)

    for step in range(STEPS):
        turn = 2 * step
        if step == 0:
            finish("velocity")
        else:
            turns[turn - 1].sent()
        for grid in grids:
            grid.each_row(grid.velocity_inner)
        if step > 0:
            fine.each_row(fine.raise_peak, 0, fine.rows // 2)
        close_turn(turn)
        open_turn(turn + 1)
        restrict(turn + 1)
        if step == 0:
            finish("memory")
            finish("peak")
        else:
            fine.each_row(fine.raise_peak, fine.rows // 2)
            coarse.each_row(coarse.raise_peak)
        turns[turn].sent()
        for grid in grids:
            grid.each_row(grid.stress_inner)
        close_turn(turn + 1)
        if step < STEPS - 1:
            open_turn(turn + 2)
            restrict(turn + 2)
    turns[2 * STEPS - 1].sent()


def finish_kernel(*refs):
    states, outputs = [refs[0:5], refs[5:10]], [refs[10:14], refs[14:18]]
    peaks, sems = refs[18:20], refs[20]
    wholes = []
    for grid, ((stress, velocity, memory, peak, _), arrays) in enumerate(zip(states, outputs)):
        new_velocity, new_stress, new_memory, _ = arrays
        tiles, rows, depth, _ = peak.shape
        inner_rows, inner = pl.ds(2, rows), pl.ds(ROWS, depth)
        for tile in range(tiles):
            lanes = pl.ds(tile * LANES, LANES)
            for index, (source, target) in enumerate(
                (
                    (velocity.at[:, tile, inner_rows, inner, :], new_velocity),
                    (stress.at[:, tile, inner_rows, inner, :], new_stress),
                    (memory.at[:, tile], new_memory),
                )
            ):
                place = target.at[:, :, :, lanes]
                pltpu.make_async_copy(source, place, sems.at[grid, index]).start()
        wholes += [(array, sems.at[grid, index]) for index, array in enumerate(arrays)]
    for grid, ((stress, _, _, peak, props), (_, _, _, new_peak), raised) in enumerate(
        zip(states, outputs, peaks)
    ):
        tiles, rows, depth, _ = peak.shape
        half = rows // 2

        def body(row, carry):
            for tile in range(tiles):
                strain = principal(
                    [stress[part, tile, row + 2, pl.ds(ROWS, depth), :] for part in range(6)],
                    props[VOLUMETRIC, tile, row],
                    props[SCALE, tile, row],
                )
                raised[tile, row] = jnp.maximum(peak[tile, row], strain)
            return carry

        for begin, end in ((0, half), (half, rows)):
            lax.fori_loop(begin, end, body, 0)
            span = pl.ds(begin, end - begin)
            for tile in range(tiles):
                place = new_peak.at[span, :, pl.ds(tile * LANES, LANES)]
                pltpu.make_async_copy(raised.at[tile, span], place, sems.at[grid, 3]).start()
    for array, sem in wholes:
        pltpu.make_async_copy(array, array, sem).wait()


def sizes_of(peak):
    rows, depth, cells = peak.shape
    tiles = cells // LANES
    return tiles, (tiles, rows + 4, depth + 2 * ROWS, LANES), (tiles, rows, depth, LANES)


def state_of(peak):
    _, full, plain = sizes_of(peak)
    shapes = [(6, *full), (3, *full), (6, *plain), plain, (7, *plain)]
    return [pltpu.VMEM(shape, jnp.float32) for shape in shapes]


def scratch_of(peak):
    tiles, _, plain = sizes_of(peak)
    _, rows, depth, _ = plain
    side = pltpu.VMEM((2 * STEPS, 3, tiles, 2, depth, LANES), jnp.float32)
    around = pltpu.VMEM((2 * STEPS, 3, tiles, rows, 3 * ROWS, LANES), jnp.float32)
    return [pltpu.VMEM(plain, jnp.int32), side, side, around]


def on_device(
    velocity_fine,
    stress_fine,
    memory_fine,
    peak_fine,
    zone_fine,
    velocity_coarse,
    stress_coarse,
    memory_coarse,
    peak_coarse,
    zone_coarse,
    zone_table,
    interp_weight,
    restrict_weight,
):
    fine = (velocity_fine, stress_fine, memory_fine, peak_fine)
    coarse = (velocity_coarse, stress_coarse, memory_coarse, peak_coarse)
    fine_rows, _, fine_cells = peak_fine.shape
    coarse_rows, _, coarse_cells = peak_coarse.shape
    block = ROWS * ((coarse_rows + ROWS) // ROWS)
    turns = 2 * STEPS
    hbm = pl.BlockSpec(memory_space=pl.ANY)
    smem = pl.BlockSpec(memory_space=pltpu.SMEM)
    vmem = pl.BlockSpec(memory_space=pltpu.VMEM)
    token_rows = sum(
        5 * (peak.size // LANES) // min(peak.shape[:2]) for peak in (peak_fine, peak_coarse)
    )
    state = pl.pallas_call(
        waves_kernel,
        out_shape=state_of(peak_fine) + state_of(peak_coarse),
        in_specs=[smem] * 3 + [hbm] * 10,
        out_specs=[vmem] * 10,
        scratch_shapes=[
            *scratch_of(peak_fine),
            *scratch_of(peak_coarse),
            pltpu.VMEM((turns, 3, 2 * block, coarse_cells), jnp.float32),
            pltpu.VMEM((turns, 3, coarse_cells // LANES, coarse_rows, ROWS, LANES), jnp.float32),
            pltpu.VMEM((3 * coarse_rows * ROWS, fine_cells), jnp.float32),
            pltpu.VMEM((coarse_cells, fine_cells), jnp.float32),
            pltpu.VMEM((fine_cells, coarse_cells), jnp.float32),
            pltpu.VMEM((7, zone_table.shape[0], ROWS, LANES), jnp.float32),
            pltpu.VMEM((token_rows, LANES), jnp.float32),
            pltpu.SemaphoreType.DMA((2, 5)),
            pltpu.SemaphoreType.DMA((turns, ROUTES)),
            pltpu.SemaphoreType.DMA((turns, ROUTES)),
        ],
        compiler_params=pltpu.CompilerParams(
            collective_id=0, has_side_effects=True, vmem_limit_bytes=KERNEL_BYTES
        ),
        name="waves",
    )(
        *(
            pltpu.with_memory_space_constraint(array, pltpu.HBM)
            for array in (
                zone_table,
                interp_weight,
                restrict_weight,
                *fine,
                zone_fine,
                *coarse,
                zone_coarse,
            )
        )
    )
    outputs = (*fine, *coarse)
    return tuple(
        pl.pallas_call(
            finish_kernel,
            out_shape=[jax.ShapeDtypeStruct(array.shape, array.dtype) for array in outputs],
            in_specs=[vmem] * 10,
            out_specs=[hbm] * 8,
            scratch_shapes=[
                pltpu.VMEM(sizes_of(peak_fine)[2], jnp.float32),
                pltpu.VMEM(sizes_of(peak_coarse)[2], jnp.float32),
                pltpu.SemaphoreType.DMA((2, 4)),
            ],
            compiler_params=pltpu.CompilerParams(vmem_limit_bytes=KERNEL_BYTES),
            name="finish",
        )(*state)
    )


def solution(mesh):
    field, scalar, whole = P(None, "lat", "depth", None), P("lat", "depth", None), P()
    return jax.shard_map(
        on_device,
        mesh=mesh,
        in_specs=(field, field, field, scalar, scalar) * 2 + (whole,) * 3,
        out_specs=(field, field, field, scalar) * 2,
        check_vma=False,
    )
```

```python
import math

import jax
import jax.numpy as jnp
from jax import lax
from jax.experimental import pallas as pl
from jax.experimental.pallas import tpu as pltpu
from jax.sharding import PartitionSpec as P

STEPS = 2
LANES = 128
ROWS = 8

TIME_STEP = 0.4
NEAR = 9.0 / 8.0
FAR = 1.0 / 27.0
TINY = 1e-18

FORWARD = (1, 2)
BACKWARD = (2, 1)
STRESS_X = ((0, FORWARD), (3, BACKWARD), (4, BACKWARD))
STRESS_Z = ((4, BACKWARD), (5, BACKWARD), (2, FORWARD))
VELOCITY_X = ((0, BACKWARD), (1, FORWARD), (2, FORWARD))
VELOCITY_Z = ((0, FORWARD), (1, FORWARD), (2, BACKWARD))

BUOYANCY, LAME, SHEAR, DECAY, DAMPING, VOLUMETRIC, SCALE = range(7)

MESH = pl.DeviceIdType.MESH


def property_tables(table_ref, spacing):
    def fill(column, level):
        return jnp.full((ROWS, LANES), table_ref[level, column], jnp.float32)

    tables = []
    for level in range(table_ref.shape[0]):
        buoyancy, lame, shear, decay, damping = (fill(column, level) for column in range(5))
        tables.append(
            [
                buoyancy * (TIME_STEP * NEAR / spacing),
                lame * (NEAR / spacing),
                shear * (2.0 * NEAR / spacing),
                decay,
                damping * (1.0 - decay),
                lame / (3.0 * lame + 2.0 * shear),
                0.5 / shear,
            ]
        )
    return tables


def select(masks, values):
    for mask in masks:
        pairs = [values[i : i + 2] for i in range(0, len(values), 2)]
        values = [jnp.where(mask, pair[-1], pair[0]) for pair in pairs]
    return values[0]


def rotation(low, high, pivot):
    half = 0.5 * (high - low)
    size = jnp.maximum(jnp.abs(half), TINY)
    square = size * size + pivot * pivot
    radius = square * lax.rsqrt(square)
    reach = size + radius
    weight = lax.rsqrt((radius + radius) * reach)
    sign = jnp.where(half >= 0, 1.0, -1.0)
    middle = low + half
    offset = sign * radius
    return reach * weight, sign * (pivot * weight), middle - offset, middle + offset


def largest(low, high, pivot):
    half = 0.5 * (high - low)
    size = jnp.maximum(jnp.abs(half), TINY)
    square = size * size + pivot * pivot
    return low + half + square * lax.rsqrt(square)


def principal(stress, volumetric, scale):
    a00, a11, a22, a01, a02, a12 = stress
    shift = volumetric * (a00 + a11 + a22)
    cosine, sine, a00, a11 = rotation(a00, a11, a01)
    a02, a12 = cosine * a02 - sine * a12, sine * a02 + cosine * a12
    for sweep in range(3):
        if sweep > 0:
            cosine, sine, a00, a11 = rotation(a00, a11, a01)
            a02, a12 = cosine * a02, sine * a02
        cosine, sine, a00, a22 = rotation(a00, a22, a02)
        a01, a12 = -(sine * a12), cosine * a12
        if sweep < 2:
            cosine, sine, a11, a22 = rotation(a11, a22, a12)
            a01, a02 = cosine * a01, sine * a01
    return (jnp.maximum(a00, largest(a11, a22, a12)) - shift) * scale


def shifted_y(tiles, offset):
    lane = lax.broadcasted_iota(jnp.int32, tiles[0].shape, 1)
    rolled = [pltpu.roll(tile, (-offset) % LANES, 1) for tile in tiles]
    zero = jnp.zeros_like(tiles[0])
    if offset > 0:
        outside, beside = lane >= LANES - offset, rolled[1:] + [zero]
    else:
        outside, beside = lane < -offset, [zero] + rolled[:-1]
    return [jnp.where(outside, other, own) for other, own in zip(beside, rolled)]


def difference_y(tiles, kind):
    if kind == FORWARD:
        near = [a - b for a, b in zip(shifted_y(tiles, 1), tiles)]
        far = [a - b for a, b in zip(shifted_y(tiles, 2), shifted_y(tiles, -1))]
    else:
        near = [a - b for a, b in zip(tiles, shifted_y(tiles, -1))]
        far = [a - b for a, b in zip(shifted_y(tiles, 1), shifted_y(tiles, -2))]
    return list(zip(near, far))


def difference(at, kind):
    if kind == FORWARD:
        return at(1) - at(0), at(2) - at(-1)
    return at(0) - at(-1), at(1) - at(-2)


def total(*pairs):
    near = sum(pair[0] for pair in pairs[1:]) + pairs[0][0]
    far = sum(pair[1] for pair in pairs[1:]) + pairs[0][1]
    return near - FAR * far


class Field:
    def __init__(self, spacing, refs):
        self.spacing = spacing
        (
            self.stress,
            self.velocity,
            self.memory,
            self.peak,
            self.props,
            self.zone,
            self.below_x,
            self.above_x,
            self.around_z,
        ) = refs
        self.tiles, self.rows, self.depth, _ = self.peak.shape

    def cells(self, ref, part, tile, row, dx=0, dz=0):
        return ref[part, tile, row + (2 + dx), pl.ds(ROWS + dz, self.depth), :]

    def along_x(self, ref, part, tile, row, kind):
        return difference(lambda d: self.cells(ref, part, tile, row, dx=d), kind)

    def along_z(self, ref, part, tile, row, kind):
        return difference(lambda d: self.cells(ref, part, tile, row, dz=d), kind)

    def along_y(self, ref, part, row, kind):
        tiles = [self.cells(ref, part, tile, row) for tile in range(self.tiles)]
        return difference_y(tiles, kind)

    def each_row(self, body, begin=0, end=None):
        def step(row, carry):
            body(row)
            return carry

        lax.fori_loop(begin, self.rows if end is None else end, step, 0)

    def clear(self):
        stress, velocity, depth = self.stress, self.velocity, self.depth
        tile_zero = jnp.zeros((ROWS, LANES), jnp.float32)
        zero = jnp.zeros((depth, LANES), jnp.float32)

        def body(row):
            for tile in range(self.tiles):
                for ref, parts in ((stress, (2, 4, 5)), (velocity, (0, 1, 2))):
                    for part in parts:
                        ref[part, tile, row + 2, 0:ROWS, :] = tile_zero
                        ref[part, tile, row + 2, pl.ds(ROWS + depth, ROWS), :] = tile_zero
                for turn in range(2 * STEPS):
                    for slot in range(3):
                        self.around_z[turn, slot, tile, row, pl.ds(ROWS, ROWS), :] = tile_zero

        self.each_row(body)
        for tile in range(self.tiles):
            for ref, parts in ((stress, (0, 3, 4)), (velocity, (0, 1, 2))):
                for part in parts:
                    for row in (0, 1, self.rows + 2, self.rows + 3):
                        ref[part, tile, row, pl.ds(ROWS, depth), :] = zero

    def clear_x(self, side):
        ref = self.below_x if side == 0 else self.above_x
        zero = jnp.zeros((self.depth, LANES), jnp.float32)

        def body(turn, carry):
            for slot in range(3):
                for tile in range(self.tiles):
                    for row in range(2):
                        ref[turn, slot, tile, row] = zero
            return carry

        lax.fori_loop(0, 2 * STEPS, body, 0)

    def clear_z(self, side):
        zero = jnp.zeros((ROWS, LANES), jnp.float32)

        def body(row):
            for turn in range(2 * STEPS):
                for slot in range(3):
                    for tile in range(self.tiles):
                        self.around_z[turn, slot, tile, row, pl.ds(2 * ROWS * side, ROWS), :] = zero

        self.each_row(body)

    def fill_props(self, table_ref, filled):
        zones = table_ref.shape[0]
        for level, values in enumerate(property_tables(table_ref, self.spacing)):
            for index, value in enumerate(values):
                filled[index, level] = value

        def body(row):
            for tile in range(self.tiles):
                for begin in range(0, self.depth, ROWS):
                    zone = self.zone[tile, row, begin : begin + ROWS, :]
                    masks = [
                        jnp.bitwise_and(zone, 1 << bit) != 0 for bit in range((zones - 1).bit_length())
                    ]
                    for index in range(filled.shape[0]):
                        values = [filled[index, level] for level in range(zones)]
                        self.props[index, tile, row, begin : begin + ROWS, :] = select(masks, values)

        self.each_row(body)

    def velocity_inner(self, row):
        stress, velocity = self.stress, self.velocity
        across = [
            self.along_y(stress, 3, row, BACKWARD),
            self.along_y(stress, 1, row, FORWARD),
            self.along_y(stress, 5, row, BACKWARD),
        ]
        for part in range(3):
            for tile in range(self.tiles):
                (field_x, kind_x), (field_z, kind_z) = STRESS_X[part], STRESS_Z[part]
                accel = total(
                    self.along_x(stress, field_x, tile, row, kind_x),
                    across[part][tile],
                    self.along_z(stress, field_z, tile, row, kind_z),
                )
                old = self.cells(velocity, part, tile, row)
                buoyancy = self.props[BUOYANCY, tile, row]
                velocity[part, tile, row + 2, pl.ds(ROWS, self.depth), :] = old + buoyancy * accel

    def outer_rows(self, turn, slot, tile, kind):
        below, above = self.below_x.at[turn, slot, tile], self.above_x.at[turn, slot, tile]
        last = self.rows - 1
        if kind == FORWARD:
            return [
                (0, FAR * below[1]),
                (last, above[0] - FAR * above[1]),
                (last - 1, -FAR * above[0]),
            ]
        return [
            (0, FAR * below[0] - below[1]),
            (1, FAR * below[1]),
            (last, -FAR * above[0]),
        ]

    def outer_layers(self, turn, slot, tile, row, kind):
        at = self.around_z.at[turn, slot, tile, row]

        def lower(distance):
            return at[pl.ds(ROWS - distance, ROWS), :]

        def upper(distance):
            return at[pl.ds(ROWS + distance, ROWS), :]

        if kind == FORWARD:
            return FAR * lower(1), upper(1) - FAR * upper(2)
        return FAR * lower(2) - lower(1), -FAR * upper(1)

    def ends(self):
        return (0, self.depth - ROWS)

    def velocity_outer_x(self, turn):
        velocity, depth = self.velocity, self.depth
        for part in range(3):
            for tile in range(self.tiles):
                for row, term in self.outer_rows(turn, part, tile, STRESS_X[part][1]):
                    place = velocity.at[part, tile, row + 2, pl.ds(ROWS, depth), :]
                    place[...] = place[...] + self.props[BUOYANCY, tile, row] * term

    def velocity_outer_z(self, turn):
        velocity = self.velocity

        def body(row):
            for part in range(3):
                for tile in range(self.tiles):
                    terms = self.outer_layers(turn, part, tile, row, STRESS_Z[part][1])
                    for begin, term in zip(self.ends(), terms):
                        place = velocity.at[part, tile, row + 2, pl.ds(ROWS + begin, ROWS), :]
                        buoyancy = self.props[BUOYANCY, tile, row, pl.ds(begin, ROWS), :]
                        place[...] = place[...] + buoyancy * term

        self.each_row(body)

    def stress_inner(self, row):
        velocity, stress, memory = self.velocity, self.stress, self.memory
        across_y = self.along_y(velocity, 1, row, BACKWARD)
        across_x = self.along_y(velocity, 0, row, FORWARD)
        across_z = self.along_y(velocity, 2, row, FORWARD)
        for tile in range(self.tiles):
            lame, shear, decay, damping = (
                self.props[index, tile, row] for index in (LAME, SHEAR, DECAY, DAMPING)
            )
            normal_x = total(self.along_x(velocity, 0, tile, row, BACKWARD))
            normal_y = total(across_y[tile])
            normal_z = total(self.along_z(velocity, 2, tile, row, BACKWARD))
            shear_xy = total(across_x[tile], self.along_x(velocity, 1, tile, row, FORWARD))
            shear_xz = total(
                self.along_z(velocity, 0, tile, row, FORWARD),
                self.along_x(velocity, 2, tile, row, FORWARD),
            )
            shear_yz = total(across_z[tile], self.along_z(velocity, 1, tile, row, FORWARD))
            volume = lame * (normal_x + normal_y + normal_z)
            half = 0.5 * shear
            rates = [
                volume + shear * normal_x,
                volume + shear * normal_y,
                volume + shear * normal_z,
                half * shear_xy,
                half * shear_xz,
                half * shear_yz,
            ]
            kept = 0.5 * TIME_STEP * (1.0 + decay)
            gained = TIME_STEP - 0.5 * TIME_STEP * damping
            for part, rate in enumerate(rates):
                past = memory[part, tile, row]
                memory[part, tile, row] = decay * past - damping * rate
                old = self.cells(stress, part, tile, row)
                stress[part, tile, row + 2, pl.ds(ROWS, self.depth), :] = (
                    old + kept * past + gained * rate
                )

    def add_rates(self, rates, tile, row, begin, count):
        damping = self.props[DAMPING, tile, row, pl.ds(begin, count), :]
        gained = TIME_STEP - 0.5 * TIME_STEP * damping
        for part, rate in rates:
            place = self.memory.at[part, tile, row, pl.ds(begin, count), :]
            place[...] = place[...] - damping * rate
            place = self.stress.at[part, tile, row + 2, pl.ds(ROWS + begin, count), :]
            place[...] = place[...] + gained * rate

    def normal_rates(self, term, along, tile, row, begin, count):
        lame = self.props[LAME, tile, row, pl.ds(begin, count), :]
        shear = self.props[SHEAR, tile, row, pl.ds(begin, count), :]
        volume = lame * term
        return [(part, volume + shear * term if part == along else volume) for part in range(3)]

    def shear_rates(self, term, part, tile, row, begin, count):
        shear = self.props[SHEAR, tile, row, pl.ds(begin, count), :]
        return [(part, (0.5 * shear) * term)]

    def stress_outer_x(self, turn):
        depth = self.depth
        for tile in range(self.tiles):
            for row, term in self.outer_rows(turn, 0, tile, BACKWARD):
                rates = self.normal_rates(term, 0, tile, row, 0, depth)
                self.add_rates(rates, tile, row, 0, depth)
            for slot, part in ((1, 3), (2, 4)):
                for row, term in self.outer_rows(turn, slot, tile, FORWARD):
                    rates = self.shear_rates(term, part, tile, row, 0, depth)
                    self.add_rates(rates, tile, row, 0, depth)

    def stress_outer_z(self, turn):
        def body(row):
            for tile in range(self.tiles):
                normal = self.outer_layers(turn, 2, tile, row, BACKWARD)
                shear_xz = self.outer_layers(turn, 0, tile, row, FORWARD)
                shear_yz = self.outer_layers(turn, 1, tile, row, FORWARD)
                for end, begin in enumerate(self.ends()):
                    rates = (
                        self.normal_rates(normal[end], 2, tile, row, begin, ROWS)
                        + self.shear_rates(shear_xz[end], 4, tile, row, begin, ROWS)
                        + self.shear_rates(shear_yz[end], 5, tile, row, begin, ROWS)
                    )
                    self.add_rates(rates, tile, row, begin, ROWS)

        self.each_row(body)

    def raise_peak(self, row):
        for tile in range(self.tiles):
            strain = principal(
                [self.cells(self.stress, part, tile, row) for part in range(6)],
                self.props[VOLUMETRIC, tile, row],
                self.props[SCALE, tile, row],
            )
            self.peak[tile, row] = jnp.maximum(self.peak[tile, row], strain)


def spread_matrix(interp_ref, coarse_cells, fine_cells):
    coarse = lax.broadcasted_iota(jnp.int32, (coarse_cells, fine_cells), 0)
    fine = lax.broadcasted_iota(jnp.int32, (coarse_cells, fine_cells), 1)
    matrix = jnp.zeros((coarse_cells, fine_cells), jnp.float32)
    for phase in range(3):
        share = interp_ref[1, phase].astype(jnp.float32) / 8.0
        matrix = jnp.where(fine == 3 * coarse + phase, share, matrix)
        matrix = jnp.where(fine == 3 * coarse - 3 + phase, 1.0 - share, matrix)
    return matrix.astype(jnp.bfloat16)


def gather_matrix(restrict_ref, coarse_cells, fine_cells):
    fine = lax.broadcasted_iota(jnp.int32, (fine_cells, coarse_cells), 0)
    coarse = lax.broadcasted_iota(jnp.int32, (fine_cells, coarse_cells), 1)
    matrix = jnp.zeros((fine_cells, coarse_cells), jnp.float32)
    for phase in range(3):
        weight = restrict_ref[1, phase].astype(jnp.float32)
        matrix = jnp.where(fine == 3 * coarse + phase, weight, matrix)
    return matrix.astype(jnp.bfloat16)


def lift_matrix(interp_ref, fine_rows, rows):
    shape = (2 * fine_rows, 6 * rows)
    target = lax.broadcasted_iota(jnp.int32, shape, 0)
    source = lax.broadcasted_iota(jnp.int32, shape, 1)
    matrix = jnp.zeros(shape, jnp.float32)
    for phase in range(3):
        share = interp_ref[0, phase].astype(jnp.float32) / 8.0
        for begin in range(0, 6 * rows, rows):
            ghost = begin // rows % 2
            for ahead in range(2):
                base = 6 * (source - begin - ahead) + 2 * phase + ghost
                inside = (source >= begin + ahead) & (source < begin + rows)
                weight = share if ahead == 0 else 1.0 - share
                matrix = jnp.where((target == base) & inside, weight, matrix)
    return matrix.astype(jnp.bfloat16)


def three_parts(value):
    parts = []
    for _ in range(3):
        part = value.astype(jnp.bfloat16)
        value = value - part.astype(jnp.float32)
        parts.append(part)
    return jnp.concatenate(parts, axis=0)


def exact_dot(left, right):
    count = left.shape[0]
    product = jnp.dot(three_parts(left), right, preferred_element_type=jnp.float32)
    return product[:count] + (product[count : 2 * count] + product[2 * count :])


class Coupling:
    def __init__(self, fine, coarse, interp_ref, restrict_ref, refs):
        self.fine, self.coarse = fine, coarse
        self.interp_ref, self.restrict_ref = interp_ref, restrict_ref
        self.heads, self.lifted, self.layers, self.spread, self.gather, self.lift = refs
        self.block = self.heads.shape[2] // 2

    def clear(self):
        coarse_cells, fine_cells = self.spread.shape
        self.spread[...] = spread_matrix(self.interp_ref, coarse_cells, fine_cells)
        self.gather[...] = gather_matrix(self.restrict_ref, coarse_cells, fine_cells)
        self.lift[...] = lift_matrix(self.interp_ref, self.fine.rows, self.block)

    def restrict(self, turn, ref, along_z):
        fine, coarse = self.fine, self.coarse
        weight = [self.restrict_ref[0, phase].astype(jnp.float32) for phase in range(3)]
        weight_y = [self.restrict_ref[1, phase].astype(jnp.float32) for phase in range(3)]
        mass = 3.0 * (weight[0] + weight[1] + weight[2]) * (weight_y[0] + weight_y[1] + weight_y[2])
        for slot, (part, _) in enumerate(along_z):
            for row in range(coarse.rows):
                begin = (slot * coarse.rows + row) * ROWS
                for tile in range(fine.tiles):
                    block = sum(
                        weight[phase]
                        * ref[part, tile, 2 + 3 * row + phase, pl.ds(fine.depth, ROWS), :]
                        for phase in range(3)
                    )
                    self.layers[begin : begin + ROWS, tile * LANES : (tile + 1) * LANES] = block
        gathered = exact_dot(self.layers[...], self.gather[...])
        gathered = gathered / jnp.full(gathered.shape, mass, jnp.float32)
        for slot in range(3):
            for row in range(coarse.rows):
                begin = (slot * coarse.rows + row) * ROWS
                for tile in range(coarse.tiles):
                    block = gathered[begin : begin + ROWS, tile * LANES : (tile + 1) * LANES]
                    block = block + pltpu.roll(block, 1, 0) + pltpu.roll(block, 2, 0)
                    self.lifted[turn, slot, tile, row, 6:7, :] = block[4:5]
                    self.lifted[turn, slot, tile, row, 7:8, :] = block[7:8]

    def interpolate(self, turn):
        fine = self.fine
        lifted = []
        for slot in range(3):
            first = self.heads[turn, slot, 0 : self.block, :]
            second = self.heads[turn, slot, self.block : 2 * self.block, :]
            layers = [(2.0 * first + second) / 3.0, (first + 2.0 * second) / 3.0]
            parts = three_parts(jnp.concatenate(layers, axis=0))
            lifted.append(jnp.dot(self.lift[...], parts, preferred_element_type=jnp.float32))
        ghosts = exact_dot(jnp.concatenate(lifted, axis=0), self.spread[...])
        for slot in range(3):
            for row in range(fine.rows):
                begin = 2 * (slot * fine.rows + row)
                for tile in range(fine.tiles):
                    fine.around_z[turn, slot, tile, row, 2 * ROWS : 2 * ROWS + 2, :] = ghosts[
                        begin : begin + 2, tile * LANES : (tile + 1) * LANES
                    ]


class Place:
    def __init__(self):
        self.lat, self.depth = lax.axis_index("lat"), lax.axis_index("depth")
        self.lats, self.depths = lax.axis_size("lat"), lax.axis_size("depth")
        lat, depth = self.lat, self.depth
        has_next, has_previous = lat < self.lats - 1, lat > 0
        has_lower, has_upper = depth < self.depths - 1, depth > 0
        top, bottom = depth == 0, depth == self.depths - 1
        self.routes = {
            "head": (lat, self.depths - 1, top, bottom),
            "corner": (lat - 1, self.depths - 1, top & has_previous, bottom & has_next),
            "lift": (lat, 0, bottom, top),
        }
        for grid in ("fine", "coarse"):
            self.routes[f"next {grid}"] = (lat + 1, depth, has_next, has_previous)
            self.routes[f"previous {grid}"] = (lat - 1, depth, has_previous, has_next)
            self.routes[f"down {grid}"] = (lat, depth + 1, has_lower, has_upper)
            self.routes[f"up {grid}"] = (lat, depth - 1, has_upper, has_lower)
        self.top, self.bottom = top, bottom

    def target(self, route):
        lat, depth = self.routes[route][:2]
        return {"lat": lat, "depth": depth}

    def greet(self):
        barrier = pltpu.get_barrier_semaphore()
        lat, depth = self.lat, self.depth
        peers = [
            (lat + 1, depth, lat < self.lats - 1),
            (lat - 1, depth, lat > 0),
            (lat, depth + 1, depth < self.depths - 1),
            (lat, depth - 1, depth > 0),
            (lat, self.depths - 1, self.top),
            (lat, 0, self.bottom),
            (lat - 1, self.depths - 1, self.top & (lat > 0)),
            (lat + 1, 0, self.bottom & (lat < self.lats - 1)),
        ]
        for peer_lat, peer_depth, present in peers:

            @pl.when(present)
            def _():
                pl.semaphore_signal(
                    barrier,
                    inc=1,
                    device_id={"lat": peer_lat, "depth": peer_depth},
                    device_id_type=MESH,
                )

        return barrier, sum(present.astype(jnp.int32) for _, _, present in peers)


class Exchange:
    def __init__(self, turn, place, fine, coarse, coupling, velocity, sems):
        self.place = place
        along_x = VELOCITY_X if velocity else STRESS_X
        along_z = VELOCITY_Z if velocity else STRESS_Z
        self.messages = {route: [] for route in place.routes}
        self.numbers = {route: number for number, route in enumerate(place.routes)}
        self.length = dict.fromkeys(place.routes, 0)
        self.send_sems, self.recv_sems, self.token = (sems[0].at[turn], sems[1].at[turn], sems[2])
        ref = coarse.velocity if velocity else coarse.stress
        block = coupling.block
        for slot, (part, (low, _)) in enumerate(along_z):
            for layer in range(2):
                for tile in range(coarse.tiles):
                    source = ref.at[part, tile, :, ROWS + layer, :]
                    lanes = pl.ds(tile * LANES, LANES)
                    begin = layer * block
                    self.add(
                        "head",
                        source.at[pl.ds(2, coarse.rows), :],
                        coupling.heads.at[turn, slot, pl.ds(begin, coarse.rows), lanes],
                    )
                    self.add(
                        "corner",
                        source.at[pl.ds(2, 1), :],
                        coupling.heads.at[turn, slot, pl.ds(begin + coarse.rows, 1), lanes],
                    )
            self.add(
                "lift",
                coupling.lifted.at[turn, slot, :, :, pl.ds(ROWS - low, low), :],
                coarse.around_z.at[turn, slot, :, :, pl.ds(ROWS - low, low), :],
            )
        for name, grid in (("fine", fine), ("coarse", coarse)):
            ref = grid.velocity if velocity else grid.stress
            inner = pl.ds(ROWS, grid.depth)
            for slot, (part, (low, high)) in enumerate(along_x):
                self.add(
                    f"next {name}",
                    ref.at[part, :, pl.ds(2 + grid.rows - low, low), inner, :],
                    grid.below_x.at[turn, slot, :, pl.ds(2 - low, low), :, :],
                )
                self.add(
                    f"previous {name}",
                    ref.at[part, :, pl.ds(2, high), inner, :],
                    grid.above_x.at[turn, slot, :, pl.ds(0, high), :, :],
                )
            for slot, (part, (low, high)) in enumerate(along_z):
                rows = pl.ds(2, grid.rows)
                self.add(
                    f"down {name}",
                    ref.at[part, :, rows, pl.ds(ROWS + grid.depth - low, low), :],
                    grid.around_z.at[turn, slot, :, :, pl.ds(ROWS - low, low), :],
                )
                self.add(
                    f"up {name}",
                    ref.at[part, :, rows, pl.ds(ROWS, high), :],
                    grid.around_z.at[turn, slot, :, :, pl.ds(2 * ROWS, high), :],
                )

    def add(self, route, source, target):
        number = self.numbers[route]
        copy = pltpu.make_async_remote_copy(
            src_ref=source,
            dst_ref=target,
            send_sem=self.send_sems.at[number],
            recv_sem=self.recv_sems.at[number],
            device_id=self.place.target(route),
            device_id_type=MESH,
        )
        self.messages[route].append(copy)
        self.length[route] += math.prod(target.shape) // LANES

    def settle(self, route, sem):
        whole = self.token.at[pl.ds(0, self.length[route]), :]
        pltpu.make_async_copy(whole, whole, sem).wait()

    def send(self, *routes):
        for route in routes:

            @pl.when(self.place.routes[route][2])
            def _():
                for copy in self.messages[route]:
                    copy.start()

    def receive(self, *routes):
        for route in routes:

            @pl.when(self.place.routes[route][3])
            def _():
                self.settle(route, self.recv_sems.at[self.numbers[route]])

    def sent(self):
        for route in self.messages:

            @pl.when(self.place.routes[route][2])
            def _():
                self.settle(route, self.send_sems.at[self.numbers[route]])


ROUTES = 11
EDGE = 2
KERNEL_BYTES = 32 * 1024 * 1024


def waves_kernel(*refs):
    refs = list(refs)

    def take(count):
        taken = refs[:count]
        del refs[:count]
        return taken

    table_ref, interp_ref, restrict_ref = take(3)
    inputs = [take(5), take(5)]
    states = [take(5), take(5)]
    fine = Field(1.0, states[0] + take(4))
    coarse = Field(3.0, states[1] + take(4))
    coupling = Coupling(fine, coarse, interp_ref, restrict_ref, take(6))
    filled, token = take(2)
    load_sems, send_sems, recv_sems = take(3)
    place = Place()
    grids = (fine, coarse)

    loads = {}
    for grid, arrays, sems in zip(grids, inputs, (load_sems.at[0], load_sems.at[1])):
        velocity, stress, memory, peak, zone = arrays
        rows, inner = pl.ds(2, grid.rows), pl.ds(ROWS, grid.depth)
        wholes = (zone, stress, velocity, memory, peak)
        for index, name in enumerate(("zone", "stress", "velocity", "memory", "peak")):
            copies = []
            for tile in range(grid.tiles):
                lanes = pl.ds(tile * LANES, LANES)
                source, target = {
                    "zone": (zone.at[:, :, lanes], grid.zone.at[tile]),
                    "stress": (stress.at[:, :, :, lanes], grid.stress.at[:, tile, rows, inner, :]),
                    "velocity": (
                        velocity.at[:, :, :, lanes],
                        grid.velocity.at[:, tile, rows, inner, :],
                    ),
                    "memory": (memory.at[:, :, :, lanes], grid.memory.at[:, tile]),
                    "peak": (peak.at[:, :, lanes], grid.peak.at[tile]),
                }[name]
                copies.append(pltpu.make_async_copy(source, target, sems.at[index]))
            whole = pltpu.make_async_copy(wholes[index], wholes[index], sems.at[index])
            loads.setdefault(name, []).append((copies, whole))

    def start(name):
        for copies, _ in loads[name]:
            for copy in copies:
                copy.start()

    def finish(name):
        for _, whole in loads[name]:
            whole.wait()

    start("stress")
    coupling.heads[...] = jnp.zeros(coupling.heads.shape, jnp.float32)
    barrier, peers = place.greet()
    for name in ("zone", "velocity", "memory", "peak"):
        start(name)

    turns = [
        Exchange(turn, place, fine, coarse, coupling, turn % 2 == 1, (send_sems, recv_sems, token))
        for turn in range(2 * STEPS)
    ]

    def restrict(turn):
        velocity = turn % 2 == 1

        @pl.when(place.bottom)
        def _():
            coupling.restrict(
                turn,
                fine.velocity if velocity else fine.stress,
                VELOCITY_Z if velocity else STRESS_Z,
            )

        turns[turn].send("lift")

    def open_coarse(turn):
        turns[turn].send(
            "head", "corner", "next coarse", "previous coarse", "down coarse", "up coarse"
        )

    def open_fine(turn):
        turns[turn].send("next fine", "previous fine", "down fine", "up fine")

    def outer_z(grid, turn):
        if turn % 2 == 1:
            grid.stress_outer_z(turn)
        else:
            grid.velocity_outer_z(turn)

    def outer_x(grid, turn):
        if turn % 2 == 1:
            grid.stress_outer_x(turn)
        else:
            grid.velocity_outer_x(turn)

    def close_turn(turn):
        last = turn == 2 * STEPS - 1
        turns[turn].receive("down coarse", "up coarse", "lift")
        outer_z(coarse, turn)
        turns[turn].receive("next coarse", "previous coarse")
        outer_x(coarse, turn)
        if last:
            coarse.each_row(coarse.raise_peak)
        else:
            open_coarse(turn + 1)
        turns[turn].receive("head", "corner")

        @pl.when(place.bottom)
        def _():
            coupling.interpolate(turn)

        turns[turn].receive("down fine", "up fine")
        outer_z(fine, turn)
        if last:
            fine.each_row(fine.raise_peak, EDGE, fine.rows - EDGE)
        turns[turn].receive("next fine", "previous fine")
        outer_x(fine, turn)
        if not last:
            open_fine(turn + 1)
            restrict(turn + 1)

    finish("stress")
    pl.semaphore_wait(barrier, peers)
    open_coarse(0)
    open_fine(0)

    @pl.when(place.bottom)
    def _():
        coupling.clear()

    restrict(0)

    for grid in grids:
        grid.clear()

    @pl.when(place.top)
    def _():
        fine.clear_z(0)

    @pl.when(place.bottom)
    def _():
        coarse.clear_z(1)

    for side, outside in ((0, place.lat == 0), (1, place.lat == place.lats - 1)):

        @pl.when(outside)
        def _():
            for grid in grids:
                grid.clear_x(side)

    finish("zone")
    for grid in grids:
        grid.fill_props(table_ref, filled)

    early = 2 * fine.rows // 3
    for step in range(STEPS):
        turn = 2 * step
        if step == 0:
            finish("velocity")
        else:
            turns[turn - 1].sent()
        for grid in grids:
            grid.each_row(grid.velocity_inner)
        if step > 0:
            fine.each_row(fine.raise_peak, 0, early)
        close_turn(turn)
        if step == 0:
            finish("memory")
            finish("peak")
        else:
            fine.each_row(fine.raise_peak, early)
            coarse.each_row(coarse.raise_peak)
        turns[turn].sent()
        for grid in grids:
            grid.each_row(grid.stress_inner)
        close_turn(turn + 1)
    turns[2 * STEPS - 1].sent()


def finish_kernel(*refs):
    states, outputs = [refs[0:5], refs[5:10]], [refs[10:14], refs[14:18]]
    raised_fine, sems = refs[18:20]
    wholes = []
    for grid, ((stress, velocity, memory, peak, _), arrays) in enumerate(zip(states, outputs)):
        new_velocity, new_stress, new_memory, _ = arrays
        tiles, rows, depth, _ = peak.shape
        inner_rows, inner = pl.ds(2, rows), pl.ds(ROWS, depth)
        for tile in range(tiles):
            lanes = pl.ds(tile * LANES, LANES)
            for index, (source, target) in enumerate(
                (
                    (velocity.at[:, tile, inner_rows, inner, :], new_velocity),
                    (stress.at[:, tile, inner_rows, inner, :], new_stress),
                    (memory.at[:, tile], new_memory),
                )
            ):
                place = target.at[:, :, :, lanes]
                pltpu.make_async_copy(source, place, sems.at[grid, index]).start()
        wholes += [(array, sems.at[grid, index]) for index, array in enumerate(arrays)]
    for grid, ((stress, _, _, peak, props), (_, _, _, new_peak), raised) in enumerate(
        zip(states, outputs, (raised_fine, None))
    ):
        tiles, rows, depth, _ = peak.shape

        def emit(source, begin, end, new_peak=new_peak, grid=grid, tiles=tiles):
            span = pl.ds(begin, end - begin)
            for tile in range(tiles):
                place = new_peak.at[span, :, pl.ds(tile * LANES, LANES)]
                pltpu.make_async_copy(source.at[tile, span], place, sems.at[grid, 3]).start()

        if raised is None:
            emit(peak, 0, rows)
            continue
        emit(peak, EDGE, rows - EDGE)

        def body(row, carry):
            for tile in range(tiles):
                strain = principal(
                    [stress[part, tile, row + 2, pl.ds(ROWS, depth), :] for part in range(6)],
                    props[VOLUMETRIC, tile, row],
                    props[SCALE, tile, row],
                )
                raised[tile, row] = jnp.maximum(peak[tile, row], strain)
            return carry

        for begin, end in ((0, EDGE), (rows - EDGE, rows)):
            lax.fori_loop(begin, end, body, 0)
            emit(raised, begin, end)
    for array, sem in wholes:
        pltpu.make_async_copy(array, array, sem).wait()


def sizes_of(peak):
    rows, depth, cells = peak.shape
    tiles = cells // LANES
    return tiles, (tiles, rows + 4, depth + 2 * ROWS, LANES), (tiles, rows, depth, LANES)


def state_of(peak):
    _, full, plain = sizes_of(peak)
    shapes = [(6, *full), (3, *full), (6, *plain), plain, (7, *plain)]
    return [pltpu.VMEM(shape, jnp.float32) for shape in shapes]


def scratch_of(peak):
    tiles, _, plain = sizes_of(peak)
    _, rows, depth, _ = plain
    side = pltpu.VMEM((2 * STEPS, 3, tiles, 2, depth, LANES), jnp.float32)
    around = pltpu.VMEM((2 * STEPS, 3, tiles, rows, 3 * ROWS, LANES), jnp.float32)
    return [pltpu.VMEM(plain, jnp.int32), side, side, around]


def on_device(
    velocity_fine,
    stress_fine,
    memory_fine,
    peak_fine,
    zone_fine,
    velocity_coarse,
    stress_coarse,
    memory_coarse,
    peak_coarse,
    zone_coarse,
    zone_table,
    interp_weight,
    restrict_weight,
):
    fine = (velocity_fine, stress_fine, memory_fine, peak_fine)
    coarse = (velocity_coarse, stress_coarse, memory_coarse, peak_coarse)
    fine_rows, _, fine_cells = peak_fine.shape
    coarse_rows, _, coarse_cells = peak_coarse.shape
    block = ROWS * ((coarse_rows + ROWS) // ROWS)
    turns = 2 * STEPS
    hbm = pl.BlockSpec(memory_space=pl.ANY)
    smem = pl.BlockSpec(memory_space=pltpu.SMEM)
    vmem = pl.BlockSpec(memory_space=pltpu.VMEM)
    token_rows = sum(
        5 * (peak.size // LANES) // min(peak.shape[:2]) for peak in (peak_fine, peak_coarse)
    )
    state = pl.pallas_call(
        waves_kernel,
        out_shape=state_of(peak_fine) + state_of(peak_coarse),
        in_specs=[smem] * 3 + [hbm] * 10,
        out_specs=[vmem] * 10,
        scratch_shapes=[
            *scratch_of(peak_fine),
            *scratch_of(peak_coarse),
            pltpu.VMEM((turns, 3, 2 * block, coarse_cells), jnp.float32),
            pltpu.VMEM((turns, 3, coarse_cells // LANES, coarse_rows, ROWS, LANES), jnp.float32),
            pltpu.VMEM((3 * coarse_rows * ROWS, fine_cells), jnp.float32),
            pltpu.VMEM((coarse_cells, fine_cells), jnp.bfloat16),
            pltpu.VMEM((fine_cells, coarse_cells), jnp.bfloat16),
            pltpu.VMEM((2 * fine_rows, 6 * block), jnp.bfloat16),
            pltpu.VMEM((7, zone_table.shape[0], ROWS, LANES), jnp.float32),
            pltpu.VMEM((token_rows, LANES), jnp.float32),
            pltpu.SemaphoreType.DMA((2, 5)),
            pltpu.SemaphoreType.DMA((turns, ROUTES)),
            pltpu.SemaphoreType.DMA((turns, ROUTES)),
        ],
        compiler_params=pltpu.CompilerParams(
            collective_id=0, has_side_effects=True, vmem_limit_bytes=KERNEL_BYTES
        ),
        name="waves",
    )(
        *(
            pltpu.with_memory_space_constraint(array, pltpu.HBM)
            for array in (
                zone_table,
                interp_weight,
                restrict_weight,
                *fine,
                zone_fine,
                *coarse,
                zone_coarse,
            )
        )
    )
    outputs = (*fine, *coarse)
    return tuple(
        pl.pallas_call(
            finish_kernel,
            out_shape=[jax.ShapeDtypeStruct(array.shape, array.dtype) for array in outputs],
            in_specs=[vmem] * 10,
            out_specs=[hbm] * 8,
            scratch_shapes=[
                pltpu.VMEM(sizes_of(peak_fine)[2], jnp.float32),
                pltpu.SemaphoreType.DMA((2, 4)),
            ],
            compiler_params=pltpu.CompilerParams(vmem_limit_bytes=KERNEL_BYTES),
            name="finish",
        )(*state)
    )


def solution(mesh):
    field, scalar, whole = P(None, "lat", "depth", None), P("lat", "depth", None), P()
    return jax.shard_map(
        on_device,
        mesh=mesh,
        in_specs=(field, field, field, scalar, scalar) * 2 + (whole,) * 3,
        out_specs=(field, field, field, scalar) * 2,
        check_vma=False,
    )
```

```python
import math

import jax
import jax.numpy as jnp
from jax import lax
from jax.experimental import pallas as pl
from jax.experimental.pallas import tpu as pltpu
from jax.sharding import PartitionSpec as P

STEPS = 2
LANES = 128
ROWS = 8

TIME_STEP = 0.4
NEAR = 9.0 / 8.0
FAR = 1.0 / 27.0
TINY = 1e-18

FORWARD = (1, 2)
BACKWARD = (2, 1)
STRESS_X = ((0, FORWARD), (3, BACKWARD), (4, BACKWARD))
STRESS_Z = ((4, BACKWARD), (5, BACKWARD), (2, FORWARD))
VELOCITY_X = ((0, BACKWARD), (1, FORWARD), (2, FORWARD))
VELOCITY_Z = ((0, FORWARD), (1, FORWARD), (2, BACKWARD))

BUOYANCY, LAME, SHEAR, DECAY, DAMPING, VOLUMETRIC, SCALE = range(7)

MESH = pl.DeviceIdType.MESH


def property_tables(table_ref, spacing):
    def fill(column, level):
        return jnp.full((ROWS, LANES), table_ref[level, column], jnp.float32)

    tables = []
    for level in range(table_ref.shape[0]):
        buoyancy, lame, shear, decay, damping = (fill(column, level) for column in range(5))
        tables.append(
            [
                buoyancy * (TIME_STEP * NEAR / spacing),
                lame * (NEAR / spacing),
                shear * (2.0 * NEAR / spacing),
                decay,
                damping * (1.0 - decay),
                lame / (3.0 * lame + 2.0 * shear),
                0.5 / shear,
            ]
        )
    return tables


def select(masks, values):
    for mask in masks:
        pairs = [values[i : i + 2] for i in range(0, len(values), 2)]
        values = [jnp.where(mask, pair[-1], pair[0]) for pair in pairs]
    return values[0]


def rotation(low, high, pivot):
    half = 0.5 * (high - low)
    size = jnp.maximum(jnp.abs(half), TINY)
    square = size * size + pivot * pivot
    radius = square * lax.rsqrt(square)
    reach = size + radius
    weight = lax.rsqrt((radius + radius) * reach)
    sign = jnp.where(half >= 0, 1.0, -1.0)
    middle = low + half
    offset = sign * radius
    return reach * weight, sign * (pivot * weight), middle - offset, middle + offset


def largest(low, high, pivot):
    half = 0.5 * (high - low)
    size = jnp.maximum(jnp.abs(half), TINY)
    square = size * size + pivot * pivot
    return low + half + square * lax.rsqrt(square)


def principal(stress, volumetric, scale):
    a00, a11, a22, a01, a02, a12 = stress
    shift = volumetric * (a00 + a11 + a22)
    cosine, sine, a00, a11 = rotation(a00, a11, a01)
    a02, a12 = cosine * a02 - sine * a12, sine * a02 + cosine * a12
    for sweep in range(3):
        if sweep > 0:
            cosine, sine, a00, a11 = rotation(a00, a11, a01)
            a02, a12 = cosine * a02, sine * a02
        cosine, sine, a00, a22 = rotation(a00, a22, a02)
        a01, a12 = -(sine * a12), cosine * a12
        if sweep < 2:
            cosine, sine, a11, a22 = rotation(a11, a22, a12)
            a01, a02 = cosine * a01, sine * a01
    return (jnp.maximum(a00, largest(a11, a22, a12)) - shift) * scale


def shifted_y(tiles, offset):
    lane = lax.broadcasted_iota(jnp.int32, tiles[0].shape, 1)
    rolled = [pltpu.roll(tile, (-offset) % LANES, 1) for tile in tiles]
    zero = jnp.zeros_like(tiles[0])
    if offset > 0:
        outside, beside = lane >= LANES - offset, rolled[1:] + [zero]
    else:
        outside, beside = lane < -offset, [zero] + rolled[:-1]
    return [jnp.where(outside, other, own) for other, own in zip(beside, rolled)]


def difference_y(tiles, kind):
    if kind == FORWARD:
        near = [a - b for a, b in zip(shifted_y(tiles, 1), tiles)]
        far = [a - b for a, b in zip(shifted_y(tiles, 2), shifted_y(tiles, -1))]
    else:
        near = [a - b for a, b in zip(tiles, shifted_y(tiles, -1))]
        far = [a - b for a, b in zip(shifted_y(tiles, 1), shifted_y(tiles, -2))]
    return list(zip(near, far))


def difference(at, kind):
    if kind == FORWARD:
        return at(1) - at(0), at(2) - at(-1)
    return at(0) - at(-1), at(1) - at(-2)


def total(*pairs):
    near = sum(pair[0] for pair in pairs[1:]) + pairs[0][0]
    far = sum(pair[1] for pair in pairs[1:]) + pairs[0][1]
    return near - FAR * far


class Field:
    def __init__(self, spacing, refs):
        self.spacing = spacing
        (
            self.stress,
            self.velocity,
            self.memory,
            self.peak,
            self.props,
            self.zone,
            self.below_x,
            self.above_x,
            self.around_z,
        ) = refs
        self.tiles, self.rows, self.depth, _ = self.peak.shape

    def cells(self, ref, part, tile, row, dx=0, dz=0):
        return ref[part, tile, row + (2 + dx), pl.ds(ROWS + dz, self.depth), :]

    def along_x(self, ref, part, tile, row, kind):
        return difference(lambda d: self.cells(ref, part, tile, row, dx=d), kind)

    def along_z(self, ref, part, tile, row, kind):
        return difference(lambda d: self.cells(ref, part, tile, row, dz=d), kind)

    def along_y(self, ref, part, row, kind):
        tiles = [self.cells(ref, part, tile, row) for tile in range(self.tiles)]
        return difference_y(tiles, kind)

    def each_pair(self, body):
        def step(pair, carry):
            body(2 * pair)
            body(2 * pair + 1)
            return carry

        lax.fori_loop(0, self.rows // 2, step, 0)
        if self.rows % 2 == 1:
            body(self.rows - 1)

    def each_row(self, body, begin=0, end=None):
        def step(row, carry):
            body(row)
            return carry

        lax.fori_loop(begin, self.rows if end is None else end, step, 0)

    def clear(self):
        stress, velocity, depth = self.stress, self.velocity, self.depth
        tile_zero = jnp.zeros((ROWS, LANES), jnp.float32)
        zero = jnp.zeros((depth, LANES), jnp.float32)

        def body(row):
            for tile in range(self.tiles):
                for ref, parts in ((stress, (2, 4, 5)), (velocity, (0, 1, 2))):
                    for part in parts:
                        ref[part, tile, row + 2, 0:ROWS, :] = tile_zero
                        ref[part, tile, row + 2, pl.ds(ROWS + depth, ROWS), :] = tile_zero
                for turn in range(2 * STEPS):
                    for slot in range(3):
                        self.around_z[turn, slot, tile, row, pl.ds(ROWS, ROWS), :] = tile_zero

        self.each_row(body)
        for tile in range(self.tiles):
            for ref, parts in ((stress, (0, 3, 4)), (velocity, (0, 1, 2))):
                for part in parts:
                    for row in (0, 1, self.rows + 2, self.rows + 3):
                        ref[part, tile, row, pl.ds(ROWS, depth), :] = zero

    def clear_x(self, side):
        ref = self.below_x if side == 0 else self.above_x
        zero = jnp.zeros((self.depth, LANES), jnp.float32)

        def body(turn, carry):
            for slot in range(3):
                for tile in range(self.tiles):
                    for row in range(2):
                        ref[turn, slot, tile, row] = zero
            return carry

        lax.fori_loop(0, 2 * STEPS, body, 0)

    def clear_z(self, side):
        zero = jnp.zeros((ROWS, LANES), jnp.float32)

        def body(row):
            for turn in range(2 * STEPS):
                for slot in range(3):
                    for tile in range(self.tiles):
                        self.around_z[turn, slot, tile, row, pl.ds(2 * ROWS * side, ROWS), :] = zero

        self.each_row(body)

    def fill_props(self, table_ref, filled):
        zones = table_ref.shape[0]
        for level, values in enumerate(property_tables(table_ref, self.spacing)):
            for index, value in enumerate(values):
                filled[index, level] = value

        def body(row):
            for tile in range(self.tiles):
                for begin in range(0, self.depth, ROWS):
                    zone = self.zone[tile, row, begin : begin + ROWS, :]
                    masks = [
                        jnp.bitwise_and(zone, 1 << bit) != 0 for bit in range((zones - 1).bit_length())
                    ]
                    for index in range(filled.shape[0]):
                        values = [filled[index, level] for level in range(zones)]
                        self.props[index, tile, row, begin : begin + ROWS, :] = select(masks, values)

        self.each_row(body)

    def velocity_inner(self, row):
        stress, velocity = self.stress, self.velocity
        across = [
            self.along_y(stress, 3, row, BACKWARD),
            self.along_y(stress, 1, row, FORWARD),
            self.along_y(stress, 5, row, BACKWARD),
        ]
        for part in range(3):
            for tile in range(self.tiles):
                (field_x, kind_x), (field_z, kind_z) = STRESS_X[part], STRESS_Z[part]
                accel = total(
                    self.along_x(stress, field_x, tile, row, kind_x),
                    across[part][tile],
                    self.along_z(stress, field_z, tile, row, kind_z),
                )
                old = self.cells(velocity, part, tile, row)
                buoyancy = self.props[BUOYANCY, tile, row]
                velocity[part, tile, row + 2, pl.ds(ROWS, self.depth), :] = old + buoyancy * accel

    def outer_rows(self, turn, slot, tile, kind):
        below, above = self.below_x.at[turn, slot, tile], self.above_x.at[turn, slot, tile]
        last = self.rows - 1
        if kind == FORWARD:
            return [
                (0, FAR * below[1]),
                (last, above[0] - FAR * above[1]),
                (last - 1, -FAR * above[0]),
            ]
        return [
            (0, FAR * below[0] - below[1]),
            (1, FAR * below[1]),
            (last, -FAR * above[0]),
        ]

    def outer_layers(self, turn, slot, tile, row, kind):
        at = self.around_z.at[turn, slot, tile, row]

        def lower(distance):
            return at[pl.ds(ROWS - distance, ROWS), :]

        def upper(distance):
            return at[pl.ds(ROWS + distance, ROWS), :]

        if kind == FORWARD:
            return FAR * lower(1), upper(1) - FAR * upper(2)
        return FAR * lower(2) - lower(1), -FAR * upper(1)

    def ends(self):
        return (0, self.depth - ROWS)

    def velocity_outer_x(self, turn):
        velocity, depth = self.velocity, self.depth
        for part in range(3):
            for tile in range(self.tiles):
                for row, term in self.outer_rows(turn, part, tile, STRESS_X[part][1]):
                    place = velocity.at[part, tile, row + 2, pl.ds(ROWS, depth), :]
                    place[...] = place[...] + self.props[BUOYANCY, tile, row] * term

    def velocity_outer_z(self, turn):
        velocity = self.velocity

        def body(row):
            for part in range(3):
                for tile in range(self.tiles):
                    terms = self.outer_layers(turn, part, tile, row, STRESS_Z[part][1])
                    for begin, term in zip(self.ends(), terms):
                        place = velocity.at[part, tile, row + 2, pl.ds(ROWS + begin, ROWS), :]
                        buoyancy = self.props[BUOYANCY, tile, row, pl.ds(begin, ROWS), :]
                        place[...] = place[...] + buoyancy * term

        self.each_pair(body)

    def stress_inner(self, row):
        velocity, stress, memory = self.velocity, self.stress, self.memory
        across_y = self.along_y(velocity, 1, row, BACKWARD)
        across_x = self.along_y(velocity, 0, row, FORWARD)
        across_z = self.along_y(velocity, 2, row, FORWARD)
        for tile in range(self.tiles):
            lame, shear, decay, damping = (
                self.props[index, tile, row] for index in (LAME, SHEAR, DECAY, DAMPING)
            )
            normal_x = total(self.along_x(velocity, 0, tile, row, BACKWARD))
            normal_y = total(across_y[tile])
            normal_z = total(self.along_z(velocity, 2, tile, row, BACKWARD))
            shear_xy = total(across_x[tile], self.along_x(velocity, 1, tile, row, FORWARD))
            shear_xz = total(
                self.along_z(velocity, 0, tile, row, FORWARD),
                self.along_x(velocity, 2, tile, row, FORWARD),
            )
            shear_yz = total(across_z[tile], self.along_z(velocity, 1, tile, row, FORWARD))
            volume = lame * (normal_x + normal_y + normal_z)
            half = 0.5 * shear
            rates = [
                volume + shear * normal_x,
                volume + shear * normal_y,
                volume + shear * normal_z,
                half * shear_xy,
                half * shear_xz,
                half * shear_yz,
            ]
            kept = 0.5 * TIME_STEP * (1.0 + decay)
            gained = TIME_STEP - 0.5 * TIME_STEP * damping
            for part, rate in enumerate(rates):
                past = memory[part, tile, row]
                memory[part, tile, row] = decay * past - damping * rate
                old = self.cells(stress, part, tile, row)
                stress[part, tile, row + 2, pl.ds(ROWS, self.depth), :] = (
                    old + kept * past + gained * rate
                )

    def add_rates(self, rates, tile, row, begin, count):
        damping = self.props[DAMPING, tile, row, pl.ds(begin, count), :]
        gained = TIME_STEP - 0.5 * TIME_STEP * damping
        for part, rate in rates:
            place = self.memory.at[part, tile, row, pl.ds(begin, count), :]
            place[...] = place[...] - damping * rate
            place = self.stress.at[part, tile, row + 2, pl.ds(ROWS + begin, count), :]
            place[...] = place[...] + gained * rate

    def normal_rates(self, term, along, tile, row, begin, count):
        lame = self.props[LAME, tile, row, pl.ds(begin, count), :]
        shear = self.props[SHEAR, tile, row, pl.ds(begin, count), :]
        volume = lame * term
        return [(part, volume + shear * term if part == along else volume) for part in range(3)]

    def shear_rates(self, term, part, tile, row, begin, count):
        shear = self.props[SHEAR, tile, row, pl.ds(begin, count), :]
        return [(part, (0.5 * shear) * term)]

    def stress_outer_x(self, turn):
        depth = self.depth
        for tile in range(self.tiles):
            for row, term in self.outer_rows(turn, 0, tile, BACKWARD):
                rates = self.normal_rates(term, 0, tile, row, 0, depth)
                self.add_rates(rates, tile, row, 0, depth)
            for slot, part in ((1, 3), (2, 4)):
                for row, term in self.outer_rows(turn, slot, tile, FORWARD):
                    rates = self.shear_rates(term, part, tile, row, 0, depth)
                    self.add_rates(rates, tile, row, 0, depth)

    def stress_outer_z(self, turn):
        def body(row):
            for tile in range(self.tiles):
                normal = self.outer_layers(turn, 2, tile, row, BACKWARD)
                shear_xz = self.outer_layers(turn, 0, tile, row, FORWARD)
                shear_yz = self.outer_layers(turn, 1, tile, row, FORWARD)
                for end, begin in enumerate(self.ends()):
                    rates = (
                        self.normal_rates(normal[end], 2, tile, row, begin, ROWS)
                        + self.shear_rates(shear_xz[end], 4, tile, row, begin, ROWS)
                        + self.shear_rates(shear_yz[end], 5, tile, row, begin, ROWS)
                    )
                    self.add_rates(rates, tile, row, begin, ROWS)

        self.each_pair(body)

    def raise_peak(self, row):
        for tile in range(self.tiles):
            strain = principal(
                [self.cells(self.stress, part, tile, row) for part in range(6)],
                self.props[VOLUMETRIC, tile, row],
                self.props[SCALE, tile, row],
            )
            self.peak[tile, row] = jnp.maximum(self.peak[tile, row], strain)


def spread_matrix(interp_ref, coarse_cells, fine_cells):
    coarse = lax.broadcasted_iota(jnp.int32, (coarse_cells, fine_cells), 0)
    fine = lax.broadcasted_iota(jnp.int32, (coarse_cells, fine_cells), 1)
    matrix = jnp.zeros((coarse_cells, fine_cells), jnp.float32)
    for phase in range(3):
        share = interp_ref[1, phase].astype(jnp.float32) / 8.0
        matrix = jnp.where(fine == 3 * coarse + phase, share, matrix)
        matrix = jnp.where(fine == 3 * coarse - 3 + phase, 1.0 - share, matrix)
    return matrix.astype(jnp.bfloat16)


def gather_matrix(restrict_ref, coarse_cells, fine_cells):
    fine = lax.broadcasted_iota(jnp.int32, (fine_cells, coarse_cells), 0)
    coarse = lax.broadcasted_iota(jnp.int32, (fine_cells, coarse_cells), 1)
    matrix = jnp.zeros((fine_cells, coarse_cells), jnp.float32)
    for phase in range(3):
        weight = restrict_ref[1, phase].astype(jnp.float32)
        matrix = jnp.where(fine == 3 * coarse + phase, weight, matrix)
    return matrix.astype(jnp.bfloat16)


def lift_matrix(interp_ref, fine_rows, rows):
    shape = (2 * fine_rows, 6 * rows)
    target = lax.broadcasted_iota(jnp.int32, shape, 0)
    source = lax.broadcasted_iota(jnp.int32, shape, 1)
    matrix = jnp.zeros(shape, jnp.float32)
    for phase in range(3):
        share = interp_ref[0, phase].astype(jnp.float32) / 8.0
        for begin in range(0, 6 * rows, rows):
            ghost = begin // rows % 2
            for ahead in range(2):
                base = 6 * (source - begin - ahead) + 2 * phase + ghost
                inside = (source >= begin + ahead) & (source < begin + rows)
                weight = share if ahead == 0 else 1.0 - share
                matrix = jnp.where((target == base) & inside, weight, matrix)
    return matrix.astype(jnp.bfloat16)


def three_parts(value):
    parts = []
    for _ in range(3):
        part = value.astype(jnp.bfloat16)
        value = value - part.astype(jnp.float32)
        parts.append(part)
    return jnp.concatenate(parts, axis=0)


def exact_dot(left, right):
    count = left.shape[0]
    product = jnp.dot(three_parts(left), right, preferred_element_type=jnp.float32)
    return product[:count] + (product[count : 2 * count] + product[2 * count :])


class Coupling:
    def __init__(self, fine, coarse, interp_ref, restrict_ref, refs):
        self.fine, self.coarse = fine, coarse
        self.interp_ref, self.restrict_ref = interp_ref, restrict_ref
        self.heads, self.lifted, self.layers, self.spread, self.gather, self.lift = refs
        self.block = self.heads.shape[2] // 2

    def clear(self):
        coarse_cells, fine_cells = self.spread.shape
        self.spread[...] = spread_matrix(self.interp_ref, coarse_cells, fine_cells)
        self.gather[...] = gather_matrix(self.restrict_ref, coarse_cells, fine_cells)
        self.lift[...] = lift_matrix(self.interp_ref, self.fine.rows, self.block)

    def restrict(self, turn, ref, along_z):
        fine, coarse = self.fine, self.coarse
        weight = [self.restrict_ref[0, phase].astype(jnp.float32) for phase in range(3)]
        weight_y = [self.restrict_ref[1, phase].astype(jnp.float32) for phase in range(3)]
        mass = 3.0 * (weight[0] + weight[1] + weight[2]) * (weight_y[0] + weight_y[1] + weight_y[2])
        for slot, (part, _) in enumerate(along_z):
            for row in range(coarse.rows):
                begin = (slot * coarse.rows + row) * ROWS
                for tile in range(fine.tiles):
                    block = sum(
                        weight[phase]
                        * ref[part, tile, 2 + 3 * row + phase, pl.ds(fine.depth, ROWS), :]
                        for phase in range(3)
                    )
                    self.layers[begin : begin + ROWS, tile * LANES : (tile + 1) * LANES] = block
        gathered = exact_dot(self.layers[...], self.gather[...])
        gathered = gathered / jnp.full(gathered.shape, mass, jnp.float32)
        for slot in range(3):
            for row in range(coarse.rows):
                begin = (slot * coarse.rows + row) * ROWS
                for tile in range(coarse.tiles):
                    block = gathered[begin : begin + ROWS, tile * LANES : (tile + 1) * LANES]
                    block = block + pltpu.roll(block, 1, 0) + pltpu.roll(block, 2, 0)
                    self.lifted[turn, slot, tile, row, 6:7, :] = block[4:5]
                    self.lifted[turn, slot, tile, row, 7:8, :] = block[7:8]

    def interpolate(self, turn):
        fine = self.fine
        lifted = []
        for slot in range(3):
            first = self.heads[turn, slot, 0 : self.block, :]
            second = self.heads[turn, slot, self.block : 2 * self.block, :]
            layers = [(2.0 * first + second) / 3.0, (first + 2.0 * second) / 3.0]
            parts = three_parts(jnp.concatenate(layers, axis=0))
            lifted.append(jnp.dot(self.lift[...], parts, preferred_element_type=jnp.float32))
        ghosts = exact_dot(jnp.concatenate(lifted, axis=0), self.spread[...])
        for slot in range(3):
            for row in range(fine.rows):
                begin = 2 * (slot * fine.rows + row)
                for tile in range(fine.tiles):
                    fine.around_z[turn, slot, tile, row, 2 * ROWS : 2 * ROWS + 2, :] = ghosts[
                        begin : begin + 2, tile * LANES : (tile + 1) * LANES
                    ]


class Place:
    def __init__(self):
        self.lat, self.depth = lax.axis_index("lat"), lax.axis_index("depth")
        self.lats, self.depths = lax.axis_size("lat"), lax.axis_size("depth")
        lat, depth = self.lat, self.depth
        has_next, has_previous = lat < self.lats - 1, lat > 0
        has_lower, has_upper = depth < self.depths - 1, depth > 0
        top, bottom = depth == 0, depth == self.depths - 1
        self.routes = {
            "head": (lat, self.depths - 1, top, bottom),
            "corner": (lat - 1, self.depths - 1, top & has_previous, bottom & has_next),
            "lift": (lat, 0, bottom, top),
        }
        for grid in ("fine", "coarse"):
            self.routes[f"next {grid}"] = (lat + 1, depth, has_next, has_previous)
            self.routes[f"previous {grid}"] = (lat - 1, depth, has_previous, has_next)
            self.routes[f"down {grid}"] = (lat, depth + 1, has_lower, has_upper)
            self.routes[f"up {grid}"] = (lat, depth - 1, has_upper, has_lower)
        self.top, self.bottom = top, bottom

    def target(self, route):
        lat, depth = self.routes[route][:2]
        return {"lat": lat, "depth": depth}

    def greet(self):
        barrier = pltpu.get_barrier_semaphore()
        lat, depth = self.lat, self.depth
        peers = [
            (lat + 1, depth, lat < self.lats - 1),
            (lat - 1, depth, lat > 0),
            (lat, depth + 1, depth < self.depths - 1),
            (lat, depth - 1, depth > 0),
            (lat, self.depths - 1, self.top),
            (lat, 0, self.bottom),
            (lat - 1, self.depths - 1, self.top & (lat > 0)),
            (lat + 1, 0, self.bottom & (lat < self.lats - 1)),
        ]
        for peer_lat, peer_depth, present in peers:

            @pl.when(present)
            def _():
                pl.semaphore_signal(
                    barrier,
                    inc=1,
                    device_id={"lat": peer_lat, "depth": peer_depth},
                    device_id_type=MESH,
                )

        return barrier, sum(present.astype(jnp.int32) for _, _, present in peers)


class Exchange:
    def __init__(self, turn, place, fine, coarse, coupling, velocity, sems):
        self.place = place
        along_x = VELOCITY_X if velocity else STRESS_X
        along_z = VELOCITY_Z if velocity else STRESS_Z
        self.messages = {route: [] for route in place.routes}
        self.numbers = {route: number for number, route in enumerate(place.routes)}
        self.length = dict.fromkeys(place.routes, 0)
        self.send_sems, self.recv_sems, self.token = (sems[0].at[turn], sems[1].at[turn], sems[2])
        ref = coarse.velocity if velocity else coarse.stress
        block = coupling.block
        for slot, (part, (low, _)) in enumerate(along_z):
            for layer in range(2):
                for tile in range(coarse.tiles):
                    source = ref.at[part, tile, :, ROWS + layer, :]
                    lanes = pl.ds(tile * LANES, LANES)
                    begin = layer * block
                    self.add(
                        "head",
                        source.at[pl.ds(2, coarse.rows), :],
                        coupling.heads.at[turn, slot, pl.ds(begin, coarse.rows), lanes],
                    )
                    self.add(
                        "corner",
                        source.at[pl.ds(2, 1), :],
                        coupling.heads.at[turn, slot, pl.ds(begin + coarse.rows, 1), lanes],
                    )
            self.add(
                "lift",
                coupling.lifted.at[turn, slot, :, :, pl.ds(ROWS - low, low), :],
                coarse.around_z.at[turn, slot, :, :, pl.ds(ROWS - low, low), :],
            )
        for name, grid in (("fine", fine), ("coarse", coarse)):
            ref = grid.velocity if velocity else grid.stress
            inner = pl.ds(ROWS, grid.depth)
            for slot, (part, (low, high)) in enumerate(along_x):
                self.add(
                    f"next {name}",
                    ref.at[part, :, pl.ds(2 + grid.rows - low, low), inner, :],
                    grid.below_x.at[turn, slot, :, pl.ds(2 - low, low), :, :],
                )
                self.add(
                    f"previous {name}",
                    ref.at[part, :, pl.ds(2, high), inner, :],
                    grid.above_x.at[turn, slot, :, pl.ds(0, high), :, :],
                )
            for slot, (part, (low, high)) in enumerate(along_z):
                rows = pl.ds(2, grid.rows)
                self.add(
                    f"down {name}",
                    ref.at[part, :, rows, pl.ds(ROWS + grid.depth - low, low), :],
                    grid.around_z.at[turn, slot, :, :, pl.ds(ROWS - low, low), :],
                )
                self.add(
                    f"up {name}",
                    ref.at[part, :, rows, pl.ds(ROWS, high), :],
                    grid.around_z.at[turn, slot, :, :, pl.ds(2 * ROWS, high), :],
                )

    def add(self, route, source, target):
        number = self.numbers[route]
        copy = pltpu.make_async_remote_copy(
            src_ref=source,
            dst_ref=target,
            send_sem=self.send_sems.at[number],
            recv_sem=self.recv_sems.at[number],
            device_id=self.place.target(route),
            device_id_type=MESH,
        )
        self.messages[route].append(copy)
        self.length[route] += math.prod(target.shape) // LANES

    def settle(self, route, sem):
        whole = self.token.at[pl.ds(0, self.length[route]), :]
        pltpu.make_async_copy(whole, whole, sem).wait()

    def send(self, *routes):
        for route in routes:

            @pl.when(self.place.routes[route][2])
            def _():
                for copy in self.messages[route]:
                    copy.start()

    def receive(self, *routes):
        for route in routes:

            @pl.when(self.place.routes[route][3])
            def _():
                self.settle(route, self.recv_sems.at[self.numbers[route]])

    def sent(self):
        for route in self.messages:

            @pl.when(self.place.routes[route][2])
            def _():
                self.settle(route, self.send_sems.at[self.numbers[route]])


ROUTES = 11
EDGE = 2
KERNEL_BYTES = 32 * 1024 * 1024


def waves_kernel(*refs):
    refs = list(refs)

    def take(count):
        taken = refs[:count]
        del refs[:count]
        return taken

    table_ref, interp_ref, restrict_ref = take(3)
    inputs = [take(5), take(5)]
    states = [take(5), take(5)]
    fine = Field(1.0, states[0] + take(4))
    coarse = Field(3.0, states[1] + take(4))
    coupling = Coupling(fine, coarse, interp_ref, restrict_ref, take(6))
    filled, token = take(2)
    load_sems, send_sems, recv_sems = take(3)
    place = Place()
    grids = (fine, coarse)

    loads = {}
    for grid, arrays, sems in zip(grids, inputs, (load_sems.at[0], load_sems.at[1])):
        velocity, stress, memory, peak, zone = arrays
        rows, inner = pl.ds(2, grid.rows), pl.ds(ROWS, grid.depth)
        wholes = (zone, stress, velocity, memory, peak)
        for index, name in enumerate(("zone", "stress", "velocity", "memory", "peak")):
            copies = []
            for tile in range(grid.tiles):
                lanes = pl.ds(tile * LANES, LANES)
                source, target = {
                    "zone": (zone.at[:, :, lanes], grid.zone.at[tile]),
                    "stress": (stress.at[:, :, :, lanes], grid.stress.at[:, tile, rows, inner, :]),
                    "velocity": (
                        velocity.at[:, :, :, lanes],
                        grid.velocity.at[:, tile, rows, inner, :],
                    ),
                    "memory": (memory.at[:, :, :, lanes], grid.memory.at[:, tile]),
                    "peak": (peak.at[:, :, lanes], grid.peak.at[tile]),
                }[name]
                copies.append(pltpu.make_async_copy(source, target, sems.at[index]))
            whole = pltpu.make_async_copy(wholes[index], wholes[index], sems.at[index])
            loads.setdefault(name, []).append((copies, whole))

    def start(name):
        for copies, _ in loads[name]:
            for copy in copies:
                copy.start()

    def finish(name):
        for _, whole in loads[name]:
            whole.wait()

    start("stress")
    coupling.heads[...] = jnp.zeros(coupling.heads.shape, jnp.float32)
    barrier, peers = place.greet()
    for name in ("zone", "velocity", "memory", "peak"):
        start(name)

    turns = [
        Exchange(turn, place, fine, coarse, coupling, turn % 2 == 1, (send_sems, recv_sems, token))
        for turn in range(2 * STEPS)
    ]

    def restrict(turn):
        velocity = turn % 2 == 1

        @pl.when(place.bottom)
        def _():
            coupling.restrict(
                turn,
                fine.velocity if velocity else fine.stress,
                VELOCITY_Z if velocity else STRESS_Z,
            )

        turns[turn].send("lift")

    def open_coarse(turn):
        turns[turn].send(
            "head", "corner", "next coarse", "previous coarse", "down coarse", "up coarse"
        )

    def open_fine(turn):
        turns[turn].send("next fine", "previous fine", "down fine", "up fine")

    def outer_z(grid, turn):
        if turn % 2 == 1:
            grid.stress_outer_z(turn)
        else:
            grid.velocity_outer_z(turn)

    def outer_x(grid, turn):
        if turn % 2 == 1:
            grid.stress_outer_x(turn)
        else:
            grid.velocity_outer_x(turn)

    def close_turn(turn):
        last = turn == 2 * STEPS - 1
        turns[turn].receive("down coarse", "up coarse", "lift")
        outer_z(coarse, turn)
        turns[turn].receive("next coarse", "previous coarse")
        outer_x(coarse, turn)
        if last:
            coarse.each_row(coarse.raise_peak)
        else:
            open_coarse(turn + 1)
        turns[turn].receive("head", "corner")

        @pl.when(place.bottom)
        def _():
            coupling.interpolate(turn)

        turns[turn].receive("down fine", "up fine")
        outer_z(fine, turn)
        if last:
            fine.each_row(fine.raise_peak, EDGE, fine.rows - EDGE)
        turns[turn].receive("next fine", "previous fine")
        outer_x(fine, turn)
        if not last:
            open_fine(turn + 1)
            restrict(turn + 1)

    finish("stress")
    pl.semaphore_wait(barrier, peers)
    open_coarse(0)
    open_fine(0)

    @pl.when(place.bottom)
    def _():
        coupling.clear()

    restrict(0)

    for grid in grids:
        grid.clear()

    @pl.when(place.top)
    def _():
        fine.clear_z(0)

    @pl.when(place.bottom)
    def _():
        coarse.clear_z(1)

    for side, outside in ((0, place.lat == 0), (1, place.lat == place.lats - 1)):

        @pl.when(outside)
        def _():
            for grid in grids:
                grid.clear_x(side)

    finish("zone")
    for grid in grids:
        grid.fill_props(table_ref, filled)

    early = 2 * fine.rows // 3
    for step in range(STEPS):
        turn = 2 * step
        if step == 0:
            finish("velocity")
        else:
            turns[turn - 1].sent()
        for grid in grids:
            grid.each_pair(grid.velocity_inner)
        if step > 0:
            fine.each_row(fine.raise_peak, 0, early)
        close_turn(turn)
        if step == 0:
            finish("memory")
            finish("peak")
        else:
            fine.each_row(fine.raise_peak, early)
            coarse.each_row(coarse.raise_peak)
        turns[turn].sent()
        for grid in grids:
            grid.each_pair(grid.stress_inner)
        close_turn(turn + 1)
    turns[2 * STEPS - 1].sent()


def finish_kernel(*refs):
    states, outputs = [refs[0:5], refs[5:10]], [refs[10:14], refs[14:18]]
    raised_fine, sems = refs[18:20]
    wholes = []
    for grid, ((stress, velocity, memory, peak, _), arrays) in enumerate(zip(states, outputs)):
        new_velocity, new_stress, new_memory, _ = arrays
        tiles, rows, depth, _ = peak.shape
        inner_rows, inner = pl.ds(2, rows), pl.ds(ROWS, depth)
        for tile in range(tiles):
            lanes = pl.ds(tile * LANES, LANES)
            for index, (source, target) in enumerate(
                (
                    (velocity.at[:, tile, inner_rows, inner, :], new_velocity),
                    (stress.at[:, tile, inner_rows, inner, :], new_stress),
                    (memory.at[:, tile], new_memory),
                )
            ):
                place = target.at[:, :, :, lanes]
                pltpu.make_async_copy(source, place, sems.at[grid, index]).start()
        wholes += [(array, sems.at[grid, index]) for index, array in enumerate(arrays)]
    for grid, ((stress, _, _, peak, props), (_, _, _, new_peak), raised) in enumerate(
        zip(states, outputs, (raised_fine, None))
    ):
        tiles, rows, depth, _ = peak.shape

        def emit(source, begin, end, new_peak=new_peak, grid=grid, tiles=tiles):
            span = pl.ds(begin, end - begin)
            for tile in range(tiles):
                place = new_peak.at[span, :, pl.ds(tile * LANES, LANES)]
                pltpu.make_async_copy(source.at[tile, span], place, sems.at[grid, 3]).start()

        if raised is None:
            emit(peak, 0, rows)
            continue
        emit(peak, EDGE, rows - EDGE)

        def body(row, carry):
            for tile in range(tiles):
                strain = principal(
                    [stress[part, tile, row + 2, pl.ds(ROWS, depth), :] for part in range(6)],
                    props[VOLUMETRIC, tile, row],
                    props[SCALE, tile, row],
                )
                raised[tile, row] = jnp.maximum(peak[tile, row], strain)
            return carry

        for begin, end in ((0, EDGE), (rows - EDGE, rows)):
            lax.fori_loop(begin, end, body, 0)
            emit(raised, begin, end)
    for array, sem in wholes:
        pltpu.make_async_copy(array, array, sem).wait()


def sizes_of(peak):
    rows, depth, cells = peak.shape
    tiles = cells // LANES
    return tiles, (tiles, rows + 4, depth + 2 * ROWS, LANES), (tiles, rows, depth, LANES)


def state_of(peak):
    _, full, plain = sizes_of(peak)
    shapes = [(6, *full), (3, *full), (6, *plain), plain, (7, *plain)]
    return [pltpu.VMEM(shape, jnp.float32) for shape in shapes]


def scratch_of(peak):
    tiles, _, plain = sizes_of(peak)
    _, rows, depth, _ = plain
    side = pltpu.VMEM((2 * STEPS, 3, tiles, 2, depth, LANES), jnp.float32)
    around = pltpu.VMEM((2 * STEPS, 3, tiles, rows, 3 * ROWS, LANES), jnp.float32)
    return [pltpu.VMEM(plain, jnp.int32), side, side, around]


def on_device(
    velocity_fine,
    stress_fine,
    memory_fine,
    peak_fine,
    zone_fine,
    velocity_coarse,
    stress_coarse,
    memory_coarse,
    peak_coarse,
    zone_coarse,
    zone_table,
    interp_weight,
    restrict_weight,
):
    fine = (velocity_fine, stress_fine, memory_fine, peak_fine)
    coarse = (velocity_coarse, stress_coarse, memory_coarse, peak_coarse)
    fine_rows, _, fine_cells = peak_fine.shape
    coarse_rows, _, coarse_cells = peak_coarse.shape
    block = ROWS * ((coarse_rows + ROWS) // ROWS)
    turns = 2 * STEPS
    hbm = pl.BlockSpec(memory_space=pl.ANY)
    smem = pl.BlockSpec(memory_space=pltpu.SMEM)
    vmem = pl.BlockSpec(memory_space=pltpu.VMEM)
    token_rows = sum(
        5 * (peak.size // LANES) // min(peak.shape[:2]) for peak in (peak_fine, peak_coarse)
    )
    state = pl.pallas_call(
        waves_kernel,
        out_shape=state_of(peak_fine) + state_of(peak_coarse),
        in_specs=[smem] * 3 + [hbm] * 10,
        out_specs=[vmem] * 10,
        scratch_shapes=[
            *scratch_of(peak_fine),
            *scratch_of(peak_coarse),
            pltpu.VMEM((turns, 3, 2 * block, coarse_cells), jnp.float32),
            pltpu.VMEM((turns, 3, coarse_cells // LANES, coarse_rows, ROWS, LANES), jnp.float32),
            pltpu.VMEM((3 * coarse_rows * ROWS, fine_cells), jnp.float32),
            pltpu.VMEM((coarse_cells, fine_cells), jnp.bfloat16),
            pltpu.VMEM((fine_cells, coarse_cells), jnp.bfloat16),
            pltpu.VMEM((2 * fine_rows, 6 * block), jnp.bfloat16),
            pltpu.VMEM((7, zone_table.shape[0], ROWS, LANES), jnp.float32),
            pltpu.VMEM((token_rows, LANES), jnp.float32),
            pltpu.SemaphoreType.DMA((2, 5)),
            pltpu.SemaphoreType.DMA((turns, ROUTES)),
            pltpu.SemaphoreType.DMA((turns, ROUTES)),
        ],
        compiler_params=pltpu.CompilerParams(
            collective_id=0, has_side_effects=True, vmem_limit_bytes=KERNEL_BYTES
        ),
        name="waves",
    )(
        *(
            pltpu.with_memory_space_constraint(array, pltpu.HBM)
            for array in (
                zone_table,
                interp_weight,
                restrict_weight,
                *fine,
                zone_fine,
                *coarse,
                zone_coarse,
            )
        )
    )
    outputs = (*fine, *coarse)
    return tuple(
        pl.pallas_call(
            finish_kernel,
            out_shape=[jax.ShapeDtypeStruct(array.shape, array.dtype) for array in outputs],
            in_specs=[vmem] * 10,
            out_specs=[hbm] * 8,
            scratch_shapes=[
                pltpu.VMEM(sizes_of(peak_fine)[2], jnp.float32),
                pltpu.SemaphoreType.DMA((2, 4)),
            ],
            compiler_params=pltpu.CompilerParams(vmem_limit_bytes=KERNEL_BYTES),
            name="finish",
        )(*state)
    )


def solution(mesh):
    field, scalar, whole = P(None, "lat", "depth", None), P("lat", "depth", None), P()
    return jax.shard_map(
        on_device,
        mesh=mesh,
        in_specs=(field, field, field, scalar, scalar) * 2 + (whole,) * 3,
        out_specs=(field, field, field, scalar) * 2,
        check_vma=False,
    )
```
